16 devices in a mesh: hp: 4 (over z, y), cp: 4 (over x, core).
Axes of the slice: x: 2, y: 2, z: 2, core: 2. Of those that a mesh axis runs over, the one named last changes fastest.
Arguments:
- q: bfloat16 [6144, 8, 128], P('cp', 'hp'), parts along dimension 1
- k: bfloat16 [6144, 8, 128], P('cp', 'hp'), parts along dimension 1
- v: bfloat16 [6144, 8, 128], P('cp', 'hp'), parts along dimension 1
- u_bias: float32 [8, 128], P('hp'), parts along dimension 0
- v_bias: float32 [8, 128], P('hp'), parts along dimension 0
- rel_table: bfloat16 [6144, 1024], P('cp')
- w_rel: bfloat16 [1024, 8, 128], P(None, 'hp'), parts along dimension 1
- d_out: bfloat16 [6144, 8, 128], P('cp', 'hp'), parts along dimension 1
Outputs:
- output 1: bfloat16 [6144, 8, 128], P('cp', 'hp'), parts along dimension 1
- output 2: bfloat16 [6144, 8, 128], P('cp', 'hp'), parts along dimension 1
- output 3: bfloat16 [6144, 8, 128], P('cp', 'hp'), parts along dimension 1
- output 4: bfloat16 [6144, 8, 128], P('cp', 'hp'), parts along dimension 1
- output 5: float32 [8, 128], P('hp'), parts along dimension 0
- output 6: float32 [8, 128], P('hp'), parts along dimension 0
- output 7: float32 [1024, 8, 128], P(None, 'hp'), parts along dimension 1
There are 4 independent parts. The reference program is written for one: setup_inputs(seed, part) draws one part's arguments, and reference() takes and returns one part's arrays. A program takes and returns all parts, laid end to end along the dimension named above; an argument that names none is the same for every part.
All inputs are finite; a program needn't handle non-finite values.
Results may differ from the reference program's by a relative error of at most 0.0150476.
Values are sent between devices in bfloat16 or wider.
A program may use at most 1 GiB of HBM per device.

```python
import math
import jax
import jax.numpy as jnp
from jax import lax

SEQ_LEN = 6144
HEADS_PART = 2
HEAD_DIM = 128
MODEL_DIM = 1024
ROW_BLOCK = math.gcd(SEQ_LEN, 256)
INV_SQRT = HEAD_DIM ** -0.5


def setup_inputs(seed: int = 0, part: int = 0) -> dict:
    part_key = jax.random.fold_in(jax.random.key(seed), part)
    keys_part = jax.random.split(part_key, 7)
    table_keys = jax.random.split(jax.random.key(seed + 17), 2)
    seq_shape = (SEQ_LEN, HEADS_PART, HEAD_DIM)
    head_shape = (HEADS_PART, HEAD_DIM)
    q = jax.random.normal(keys_part[0], seq_shape, jnp.float32)
    k = 2.0 * jax.random.normal(keys_part[1], seq_shape, jnp.float32)
    v = jax.random.normal(keys_part[2], seq_shape, jnp.float32)
    u_bias = 0.5 * jax.random.normal(keys_part[3], head_shape, jnp.float32)
    v_bias = jax.random.normal(keys_part[4], head_shape, jnp.float32)
    w_rel = jax.random.normal(keys_part[5], (MODEL_DIM, HEADS_PART, HEAD_DIM), jnp.float32) * MODEL_DIM ** -0.5
    d_out = jax.random.normal(keys_part[6], seq_shape, jnp.float32)
    freq_cols = 10000.0 ** (-jax.random.uniform(table_keys[0], (MODEL_DIM,), jnp.float32))
    phases = 2.0 * math.pi * jax.random.uniform(table_keys[1], (MODEL_DIM,), jnp.float32)
    offsets = jnp.arange(SEQ_LEN, dtype=jnp.float32)
    rel_table = jnp.sin(offsets[:, None] * freq_cols[None, :] + phases[None, :])
    return {
        'q': q.astype(jnp.bfloat16),
        'k': k.astype(jnp.bfloat16),
        'v': v.astype(jnp.bfloat16),
        'u_bias': u_bias,
        'v_bias': v_bias,
        'rel_table': rel_table.astype(jnp.bfloat16),
        'w_rel': w_rel.astype(jnp.bfloat16),
        'd_out': d_out.astype(jnp.bfloat16),
    }


def attention(q_u, q_v, k, v, rel):
    key_pos = jnp.arange(SEQ_LEN)

    def one_head(head_args):
        qu_h, qv_h, k_h, v_h, rel_h = head_args

        def row_block(start):
            qu_rows = lax.dynamic_slice_in_dim(qu_h, start, ROW_BLOCK)
            qv_rows = lax.dynamic_slice_in_dim(qv_h, start, ROW_BLOCK)
            query_pos = start + jnp.arange(ROW_BLOCK)
            offset_ij = query_pos[:, None] - key_pos[None, :]
            content = jnp.dot(qu_rows, k_h.T)
            by_offset = jnp.dot(qv_rows, rel_h.T)
            position = jnp.take_along_axis(by_offset, jnp.clip(offset_ij, 0, SEQ_LEN - 1), axis=1)
            score_ij = jnp.where(offset_ij >= 0, (content + position) * INV_SQRT, -jnp.inf)
            return jnp.dot(jax.nn.softmax(score_ij, axis=-1), v_h)

        starts = jnp.arange(0, SEQ_LEN, ROW_BLOCK)
        return lax.map(jax.checkpoint(row_block), starts).reshape(SEQ_LEN, HEAD_DIM)

    per_head = lax.map(jax.checkpoint(one_head), tuple(stacked.transpose(1, 0, 2) for stacked in (q_u, q_v, k, v, rel)))
    return per_head.transpose(1, 0, 2)


def reference(q, k, v, u_bias, v_bias, rel_table, w_rel, d_out):
    rel = jnp.dot(rel_table, w_rel.reshape(MODEL_DIM, HEADS_PART * HEAD_DIM), preferred_element_type=jnp.float32)
    rel = rel.astype(jnp.bfloat16).reshape(SEQ_LEN, HEADS_PART, HEAD_DIM)
    q_wide = q.astype(jnp.float32)
    q_u = (q_wide + u_bias).astype(jnp.bfloat16).astype(jnp.float32)
    q_v = (q_wide + v_bias).astype(jnp.bfloat16).astype(jnp.float32)
    out_full, pullback = jax.vjp(attention, q_u, q_v, k.astype(jnp.float32), v.astype(jnp.float32), rel.astype(jnp.float32))
    g_qu, g_qv, g_k, g_v, g_rel = pullback(d_out.astype(jnp.float32))
    d_rel = g_rel.astype(jnp.bfloat16).reshape(SEQ_LEN, HEADS_PART * HEAD_DIM)
    d_w_rel = jnp.dot(rel_table.T, d_rel, preferred_element_type=jnp.float32).reshape(MODEL_DIM, HEADS_PART, HEAD_DIM)
    return (
        out_full.astype(jnp.bfloat16),
        (g_qu + g_qv).astype(jnp.bfloat16),
        g_k.astype(jnp.bfloat16),
        g_v.astype(jnp.bfloat16),
        g_qu.sum(axis=0),
        g_qv.sum(axis=0),
        d_w_rel,
    )
```

```python
import functools

import jax
import jax.numpy as jnp
from jax import lax
from jax.experimental import pallas as pl
from jax.experimental.pallas import tpu as pltpu
from jax.sharding import PartitionSpec as P

TILE = 512
SUB = 128
NSUB = TILE // SUB
LOG2E = 1.4426950408889634
F32 = jnp.float32
BF16 = jnp.bfloat16


def dot(lhs, rhs):
    return jnp.dot(lhs, rhs, preferred_element_type=F32)


def sub(idx):
    return slice(idx * SUB, (idx + 1) * SUB)


def roll_left(part, flip):
    groups = []
    for start in range(0, SUB, 8):
        rows = jnp.take_along_axis(part[start:start + 8], flip, axis=0)
        rows = pltpu.roll(rows, (SUB - 8 - start) % SUB, 1, stride=1, stride_axis=0)
        groups.append(jnp.take_along_axis(rows, flip, axis=0))
    return jnp.concatenate(groups, axis=0)


def attn_kernel(num_tiles, inv_sqrt, u_ref, v_ref, own_ref, own_p_ref, cross_ref, cross_p_ref,
                rows_ref, keep_ref, send_ref, bias_ref,
                full_ref, acc_ref, kt_ref, valt_ref, relt_ref, sc_ref, rot_ref, ds_ref, dw_ref, p_ref,
                qu_ref, qv_ref, qut_ref, qvt_ref, dot_ref, max_ref, sum_ref, gu_ref, gv_ref, row_ref, in_sems, out_sems):
    step = pl.program_id(0)
    steps = pl.num_programs(0)
    dev = lax.axis_index('cp')
    chip, core = lax.div(dev, 2), lax.rem(dev, 2)
    odd = lax.rem(step, 2)
    blk = 2 * step + odd + core - 2 * odd * core
    scale = inv_sqrt * LOG2E
    block_len = own_ref.shape[1]
    k_ref, val_ref, rel_ref = full_ref.at[0], full_ref.at[1], full_ref.at[2]
    q_ref, do_ref = full_ref.at[3], full_ref.at[4]
    dk_ref, dv_ref, drel_ref = acc_ref.at[0], acc_ref.at[1], acc_ref.at[2]

    def cols(tile):
        return pl.ds(pl.multiple_of(tile * TILE, TILE), TILE)

    @pl.when(step == 0)
    def _():
        my_core = [core, 1 - core]
        my_chip = [chip, 1 - chip]
        copies = []
        for piece, src in enumerate((own_ref, own_p_ref, cross_ref, cross_p_ref)):
            block = 2 * my_chip[piece // 2] + my_core[piece % 2]
            for arr in range(5):
                at = 3 - block if arr == 2 else block
                dst = full_ref.at[arr, pl.ds(pl.multiple_of(at * block_len, block_len), block_len)]
                copies.append(pltpu.make_async_copy(src.at[arr], dst, in_sems.at[piece, arr]))
        for copy in copies:
            copy.start()
        for copy in copies:
            copy.wait()

        def prep(tile, _):
            kt_ref[:, cols(tile)] = k_ref[cols(tile), :].T
            valt_ref[:, cols(tile)] = val_ref[cols(tile), :].T
            relt_ref[:, cols(tile)] = rel_ref[cols(tile), :].T
            acc_ref[:, :, cols(tile)] = jnp.zeros((3, SUB, TILE), F32)
            return 0
        lax.fori_loop(0, num_tiles, prep, 0)
        bias_ref[...] = jnp.zeros_like(bias_ref)

    rows_at = cols(blk)
    d_out = do_ref[rows_at, :]
    q_wide = q_ref[rows_at, :].astype(F32)
    q_u = (q_wide + u_ref[...]).astype(BF16)
    q_v = (q_wide + v_ref[...]).astype(BF16)
    qu_ref[...] = q_u
    qv_ref[...] = q_v
    qut_ref[...] = q_u.T
    qvt_ref[...] = q_v.T
    dot_ref[...] = d_out.T
    max_ref[...] = jnp.full_like(max_ref, -jnp.inf)
    sum_ref[...] = jnp.zeros_like(sum_ref)
    gu_ref[...] = jnp.zeros_like(gu_ref)
    gv_ref[...] = jnp.zeros_like(gv_ref)
    lane = lax.broadcasted_iota(jnp.int32, (SUB, SUB), 1)
    row = lax.broadcasted_iota(jnp.int32, (SUB, SUB), 0)
    upper = lane > row
    flip = 7 - lax.broadcasted_iota(jnp.int32, (8, SUB), 0)
    lower = lane + row < SUB - 1
    first_rel = num_tiles - 1 - blk

    def rotate_rel(tile, slot):
        for half in range(2):
            start = pl.multiple_of(tile * TILE + half * 256, 256)
            by_offset = dot(qv_ref[...], relt_ref[:, pl.ds(start, 256)])
            for a in range(NSUB):
                for c in range(2):
                    part = by_offset[sub(a), sub(c)]
                    rot_ref[slot, sub(a), sub(half * 2 + c)] = pltpu.roll(part, 1, 1, stride=1, stride_axis=0)

    rotate_rel(first_rel, 0)

    def score_tile(tile, diag):
        left = lax.rem(tile, 2)
        right = 1 - left
        if not diag:
            rotate_rel(first_rel + tile + 1, right)
        for half in range(2):
            start = pl.multiple_of(tile * TILE + half * 256, 256)
            content = dot(qu_ref[...], kt_ref[:, pl.ds(start, 256)])
            for a in range(NSUB):
                run_max = max_ref[sub(a), :]
                for c2 in range(2):
                    c = half * 2 + c2
                    hi, lo = c - a + NSUB, c - a + NSUB - 1
                    if diag and c > a:
                        score = jnp.full((SUB, SUB), -jnp.inf, F32)
                    else:
                        low_part = rot_ref[left if lo < NSUB else right, sub(a), sub(lo % NSUB)]
                        if diag and c == a:
                            score = jnp.where(upper, -jnp.inf, content[sub(a), sub(c2)] + low_part)
                        else:
                            high_part = rot_ref[left if hi < NSUB else right, sub(a), sub(hi % NSUB)]
                            score = content[sub(a), sub(c2)] + jnp.where(upper, high_part, low_part)
                    run_max = jnp.maximum(run_max, score)
                    sc_ref[sub(a), pl.ds(pl.multiple_of(tile * TILE + c * SUB, SUB), SUB)] = score
                max_ref[sub(a), :] = run_max

    def score_body(tile, _):
        score_tile(tile, False)
        return 0

    lax.fori_loop(0, blk, score_body, 0)
    score_tile(blk, True)
    row_ref[...] = jnp.broadcast_to(jnp.max(max_ref[...], axis=1, keepdims=True) * scale, (TILE, SUB))

    def prob_body(tile, _):
        for a in range(NSUB):
            run_sum = sum_ref[sub(a), :]
            row_max = row_ref[sub(a), :]
            for c in range(NSUB):
                where = pl.ds(pl.multiple_of(tile * TILE + c * SUB, SUB), SUB)
                prob = jnp.exp2(sc_ref[sub(a), where] * scale - row_max)
                sc_ref[sub(a), where] = prob
                p_ref[sub(a), sub(c)] = prob.astype(BF16)
                run_sum = run_sum + prob
            sum_ref[sub(a), :] = run_sum
        gu_ref[...] += dot(p_ref[...], val_ref[cols(tile), :])
        return 0

    lax.fori_loop(0, blk + 1, prob_body, 0)
    inv_sum = 1.0 / jnp.sum(sum_ref[...], axis=1, keepdims=True)
    out = gu_ref[...] * inv_sum
    rows_ref[0, 0] = out.astype(BF16)
    delta = jnp.sum(out * do_ref[rows_at, :].astype(F32), axis=1, keepdims=True)
    row_ref[...] = jnp.broadcast_to(delta, (TILE, SUB))
    sum_ref[...] = jnp.broadcast_to(inv_sum, (TILE, SUB))
    gu_ref[...] = jnp.zeros_like(gu_ref)
    ds_ref[1, :, :] = jnp.zeros((TILE, TILE), F32)

    def grad_body(tile, _):
        now = lax.rem(tile, 2)
        old = 1 - now
        for half in range(2):
            start = pl.multiple_of(tile * TILE + half * 256, 256)
            d_prob = dot(do_ref[rows_at, :], valt_ref[:, pl.ds(start, 256)])
            for a in range(NSUB):
                inv = sum_ref[sub(a), :]
                shift = row_ref[sub(a), :]
                for c2 in range(2):
                    c = half * 2 + c2
                    prob = sc_ref[sub(a), pl.ds(pl.multiple_of(tile * TILE + c * SUB, SUB), SUB)] * inv
                    p_ref[sub(a), sub(c)] = prob.astype(BF16)
                    d_score = prob * (d_prob[sub(a), sub(c2)] - shift)
                    dw_ref[sub(a), sub(c)] = d_score.astype(BF16)
                    ds_ref[now, sub(a), sub(c)] = roll_left(d_score, flip)
            win = pl.ds(start, 256)
            dv_ref[:, win] += dot(dot_ref[...], p_ref[:, half * 256:half * 256 + 256])
            dk_ref[:, win] += dot(qut_ref[...], dw_ref[:, half * 256:half * 256 + 256])
        gu_ref[...] += dot(dw_ref[...], k_ref[cols(tile), :])
        for a in range(NSUB):
            for y in range(NSUB):
                c_lo = y + a - NSUB
                c_hi = c_lo + 1
                lo_part = ds_ref[now if c_lo >= 0 else old, sub(a), sub(c_lo % NSUB)]
                hi_part = ds_ref[now if c_hi >= 0 else old, sub(a), sub(c_hi % NSUB)]
                p_ref[sub(a), sub(y)] = jnp.where(lower, lo_part, hi_part).astype(BF16)
        rel_tile = first_rel + tile
        gv_ref[...] += dot(p_ref[...], rel_ref[cols(rel_tile), :])
        for half in range(2):
            start = pl.multiple_of(rel_tile * TILE + half * 256, 256)
            drel_ref[:, pl.ds(start, 256)] += dot(qvt_ref[...], p_ref[:, half * 256:half * 256 + 256])
        return 0

    lax.fori_loop(0, blk + 1, grad_body, 0)
    grad_u = gu_ref[...] * inv_sqrt
    grad_v = gv_ref[...] * inv_sqrt
    rows_ref[0, 1] = (grad_u + grad_v).astype(BF16)
    bias_ref[0:1, :] += jnp.sum(grad_u, axis=0, keepdims=True)
    bias_ref[1:2, :] += jnp.sum(grad_v, axis=0, keepdims=True)

    @pl.when(step == steps - 1)
    def _():
        copies = []
        for half in range(2):
            for to, (dst, which) in enumerate(((keep_ref, core), (send_ref, 1 - core))):
                block = 2 * half + which
                for arr in range(3):
                    at = 3 - block if arr == 2 else block
                    src = acc_ref.at[arr, :, pl.ds(pl.multiple_of(at * block_len, block_len), block_len)]
                    copies.append(pltpu.make_async_copy(src, dst.at[arr, half], out_sems.at[half, to, arr]))
        for copy in copies:
            copy.start()
        for copy in copies:
            copy.wait()


def run_attn(u_bias, v_bias, own, own_p, cross, cross_p):
    _, block_len, head_dim = own.shape
    seq_len = 4 * block_len
    num_tiles = seq_len // TILE
    steps = num_tiles // 2
    vec = pl.BlockSpec(memory_space=pltpu.VMEM)
    hbm = pl.BlockSpec(memory_space=pl.ANY)
    part = jax.ShapeDtypeStruct((3, 2, head_dim, block_len), F32)
    return pl.pallas_call(
        functools.partial(attn_kernel, num_tiles, head_dim ** -0.5),
        grid=(steps,),
        in_specs=[vec, vec, hbm, hbm, hbm, hbm],
        out_specs=[pl.BlockSpec((1, 2, TILE, head_dim), lambda i: (i, 0, 0, 0)), hbm, hbm, vec],
        scratch_shapes=[
            pltpu.VMEM((5, seq_len, head_dim), BF16),
            pltpu.VMEM((3, head_dim, seq_len), F32),
            pltpu.VMEM((head_dim, seq_len), BF16),
            pltpu.VMEM((head_dim, seq_len), BF16),
            pltpu.VMEM((head_dim, seq_len), BF16),
            pltpu.VMEM((TILE, seq_len), F32),
            pltpu.VMEM((2, TILE, TILE), F32),
            pltpu.VMEM((2, TILE, TILE), F32),
            pltpu.VMEM((TILE, TILE), BF16),
            pltpu.VMEM((TILE, TILE), BF16),
            pltpu.VMEM((TILE, head_dim), BF16),
            pltpu.VMEM((TILE, head_dim), BF16),
            pltpu.VMEM((head_dim, TILE), BF16),
            pltpu.VMEM((head_dim, TILE), BF16),
            pltpu.VMEM((head_dim, TILE), BF16),
            pltpu.VMEM((TILE, SUB), F32),
            pltpu.VMEM((TILE, SUB), F32),
            pltpu.VMEM((TILE, head_dim), F32),
            pltpu.VMEM((TILE, head_dim), F32),
            pltpu.VMEM((TILE, SUB), F32),
            pltpu.SemaphoreType.DMA((4, 5)),
            pltpu.SemaphoreType.DMA((2, 2, 3)),
        ],
        out_shape=[jax.ShapeDtypeStruct((steps, 2, TILE, head_dim), BF16), part, part, jax.ShapeDtypeStruct((2, head_dim), F32)],
        compiler_params=pltpu.CompilerParams(dimension_semantics=("arbitrary",), vmem_limit_bytes=60 * 1024 * 1024),
        name="attn_rows",
    )(u_bias, v_bias, own, own_p, cross, cross_p)


def exchange_matrix():
    row = lax.broadcasted_iota(jnp.int32, (SUB, SUB), 0)
    col = lax.broadcasted_iota(jnp.int32, (SUB, SUB), 1)
    return jnp.where(row + col == SUB - 1, 1.0, 0.0).astype(BF16)


def pack_kernel(k_ref, v_ref, q_ref, do_ref, table_ref, w_ref, own_ref, send_ref):
    chip = lax.div(lax.axis_index('cp'), 2)
    flip = exchange_matrix()
    weights = jnp.swapaxes(w_ref[...], 0, 1)

    def put(arr, at, heads):
        first = chip == 0
        own_ref[arr, at] = jnp.where(first, heads[0], heads[1])
        send_ref[arr, at] = jnp.where(first, heads[1], heads[0])

    for arr, src in ((0, k_ref), (1, v_ref), (3, q_ref), (4, do_ref)):
        put(arr, slice(None), jnp.swapaxes(src[...], 0, 1))
    chunks = table_ref.shape[0] // SUB
    both = jnp.concatenate([weights[0], weights[1]], axis=1)
    for chunk in range(chunks):
        rel = dot(table_ref[sub(chunk), :], both).astype(BF16)
        rel = dot(flip, rel).astype(BF16)
        put(2, sub(chunks - 1 - chunk), (rel[:, :SUB], rel[:, SUB:]))


def merge_kernel(inv_sqrt, keep_ref, got_ref, rows_ref, rows_p_ref, own_ref, send_ref):
    dev = lax.axis_index('cp')
    chip, core = lax.div(dev, 2), lax.rem(dev, 2)
    flip = exchange_matrix()
    block_len = keep_ref.shape[3]
    tiles = block_len // TILE

    def fill(half, out_ref):
        for arr in range(2):
            for tile in range(tiles):
                part = slice(tile * TILE, (tile + 1) * TILE)
                total = keep_ref[arr, half, :, part] + got_ref[arr, half, :, part]
                if arr == 0:
                    total = total * inv_sqrt
                out_ref[2 + arr, part] = total.astype(BF16).T
        chunks = block_len // SUB
        for chunk in range(chunks):
            total = ((keep_ref[2, half, :, sub(chunk)] + got_ref[2, half, :, sub(chunk)]) * inv_sqrt).astype(BF16)
            back = lax.dot_general(flip, total, (((1,), (1,)), ((), ())), preferred_element_type=F32)
            out_ref[4, sub(chunks - 1 - chunk)] = back.astype(BF16)
        for tile in range(tiles):
            blk = (2 * half + core) * tiles + tile
            step = lax.div(blk, 2)
            mine = lax.rem(blk + step + core, 2) == 0
            part = slice(tile * TILE, (tile + 1) * TILE)
            for arr in range(2):
                out_ref[arr, part] = jnp.where(mine, rows_ref[step, arr], rows_p_ref[step, arr])

    for half in range(2):
        @pl.when(chip == half)
        def _():
            fill(half, own_ref)

        @pl.when(chip != half)
        def _():
            fill(half, send_ref)


def unpack_kernel(own_ref, got_ref, table_ref, o_ref, dq_ref, dk_ref, dv_ref, dw_ref):
    chip = lax.div(lax.axis_index('cp'), 2)

    def heads(arr):
        own, got = own_ref[arr], got_ref[arr]
        return jnp.where(chip == 0, own, got), jnp.where(chip == 0, got, own)

    for arr, dst in enumerate((o_ref, dq_ref, dk_ref, dv_ref)):
        dst[...] = jnp.stack(heads(arr), axis=1)
    d_rel = jnp.concatenate(heads(4), axis=1)
    for part in range(table_ref.shape[1] // 256):
        at = slice(part * 256, part * 256 + 256)
        d_w = lax.dot_general(table_ref[:, at], d_rel, (((0,), (0,)), ((), ())), preferred_element_type=F32)
        dw_ref[at] = jnp.stack([d_w[:, :SUB], d_w[:, SUB:]], axis=1)


def simple_call(body, out_shape, name):
    vmem = pl.BlockSpec(memory_space=pltpu.VMEM)
    return pl.pallas_call(
        body, out_shape=out_shape, out_specs=[vmem] * len(out_shape), name=name,
        compiler_params=pltpu.CompilerParams(vmem_limit_bytes=48 * 1024 * 1024))


def solution(mesh):
    seq_spec = P('cp', 'hp', None)
    head_spec = P('hp', None)
    weight_spec = P(None, 'hp', None)
    cross_pairs = [(0, 2), (2, 0), (1, 3), (3, 1)]
    core_pairs = [(0, 1), (1, 0), (2, 3), (3, 2)]

    def local_fn(q, k, v, u_bias, v_bias, rel_table, w_rel, d_out):
        block_len, num_heads, head_dim = q.shape
        chip = lax.axis_index('cp') // 2
        five = jax.ShapeDtypeStruct((5, block_len, head_dim), BF16)
        seq = jax.ShapeDtypeStruct(q.shape, BF16)
        d_weights = jax.ShapeDtypeStruct(w_rel.shape, F32)
        own, send = simple_call(pack_kernel, [five, five], "pack")(k, v, q, d_out, rel_table, w_rel)
        cross = lax.ppermute(send, 'cp', cross_pairs)
        own_p = lax.ppermute(own, 'cp', core_pairs)
        cross_p = lax.ppermute(cross, 'cp', core_pairs)
        u_mine = lax.dynamic_slice_in_dim(u_bias, chip, 1)
        v_mine = lax.dynamic_slice_in_dim(v_bias, chip, 1)
        rows, keep, away, bias_grad = run_attn(u_mine, v_mine, own, own_p, cross, cross_p)
        rows_p = lax.ppermute(rows, 'cp', core_pairs)
        away_p = lax.ppermute(away, 'cp', core_pairs)
        merge = functools.partial(merge_kernel, head_dim ** -0.5)
        out_own, out_send = simple_call(merge, [five, five], "merge")(keep, away_p, rows, rows_p)
        got = lax.ppermute(out_send, 'cp', cross_pairs)
        out, dq, dk, dv, d_w_rel = simple_call(unpack_kernel, [seq] * 4 + [d_weights], "unpack")(out_own, got, rel_table)
        head_mask = (jnp.arange(num_heads) == chip)[:, None, None]
        bias_grad = lax.psum(jnp.where(head_mask, bias_grad[None], 0.0), 'cp')
        return out, dq, dk, dv, bias_grad[:, 0], bias_grad[:, 1], lax.psum(d_w_rel, 'cp')

    return jax.shard_map(
        local_fn,
        mesh=mesh,
        in_specs=(seq_spec, seq_spec, seq_spec, head_spec, head_spec, P('cp', None), weight_spec, seq_spec),
        out_specs=(seq_spec, seq_spec, seq_spec, seq_spec, head_spec, head_spec, weight_spec),
        check_vma=False,
    )
```

```python
import functools

import jax
import jax.numpy as jnp
from jax import lax
from jax.experimental import pallas as pl
from jax.experimental.pallas import tpu as pltpu
from jax.sharding import PartitionSpec as P

TILE = 512
SUB = 128
NSUB = TILE // SUB
LOG2E = 1.4426950408889634
F32 = jnp.float32
BF16 = jnp.bfloat16


def dot(lhs, rhs):
    return jnp.dot(lhs, rhs, preferred_element_type=F32)


def sub(idx):
    return slice(idx * SUB, (idx + 1) * SUB)


def roll_left(part, flip):
    groups = []
    for start in range(0, SUB, 8):
        rows = jnp.take_along_axis(part[start:start + 8], flip, axis=0)
        rows = pltpu.roll(rows, (SUB - 8 - start) % SUB, 1, stride=1, stride_axis=0)
        groups.append(jnp.take_along_axis(rows, flip, axis=0))
    return jnp.concatenate(groups, axis=0)


def attn_kernel(num_tiles, inv_sqrt, u_ref, v_ref, own_ref, away_ref,
                res_own_ref, res_got_ref, bias_ref,
                full_ref, acc_ref, kt_ref, valt_ref, relt_ref, sc_ref, rot_ref, ds_ref, dw_ref, p_ref,
                qu_ref, qv_ref, qut_ref, qvt_ref, dot_ref, max_ref, sum_ref, gu_ref, gv_ref, row_ref,
                st_rows_ref, st_grad_ref, part_ref,
                local_sems, own_send, own_recv, cross_send, cross_recv, fwd_send, fwd_recv,
                part_send, part_recv, rows_send, grad_send, res_sems):
    step = pl.program_id(0)
    last = pl.num_programs(0) - 1
    dev = lax.axis_index('cp')
    chip, core = lax.div(dev, 2), lax.rem(dev, 2)
    core_peer, chip_peer = dev + 1 - 2 * core, dev + 2 - 4 * chip
    half_steps = num_tiles // 4
    pair = jnp.where(step < half_steps, step + half_steps * chip, (3 - chip) * half_steps - 1 - step)
    odd = lax.rem(pair, 2)
    blk = 2 * pair + odd + core - 2 * odd * core
    scale = inv_sqrt * LOG2E
    block_len = own_ref.shape[1]
    block_tiles = block_len // TILE
    k_ref, val_ref, rel_ref = full_ref.at[0], full_ref.at[1], full_ref.at[2]
    q_ref, do_ref = full_ref.at[3], full_ref.at[4]
    dk_ref, dv_ref, drel_ref = acc_ref.at[0], acc_ref.at[1], acc_ref.at[2]

    def cols(tile):
        return pl.ds(pl.multiple_of(tile * TILE, TILE), TILE)

    def place(arr, block):
        at = 3 - block if arr == 2 else block
        return full_ref.at[arr, pl.ds(pl.multiple_of(at * block_len, block_len), block_len)]

    def to_device(src, dst, send_sem, recv_sem, peer):
        return pltpu.make_async_remote_copy(
            src_ref=src, dst_ref=dst, send_sem=send_sem, recv_sem=recv_sem,
            device_id={'cp': peer}, device_id_type=pl.DeviceIdType.MESH)

    def own_copy(arr):
        return to_device(own_ref.at[arr], place(arr, dev), own_send.at[arr], own_recv.at[arr], core_peer)

    def cross_copy(arr):
        return to_device(away_ref.at[arr], place(arr, dev), cross_send.at[arr], cross_recv.at[arr], chip_peer)

    def fwd_copy(arr):
        return to_device(place(arr, chip_peer), place(arr, chip_peer), fwd_send.at[arr], fwd_recv.at[arr], core_peer)

    def transpose_half(arr, which):
        dst = (kt_ref, valt_ref, relt_ref)[arr]
        first = (1 - which if arr == 2 else which) * (num_tiles // 2)

        def body(idx, _):
            dst[:, cols(first + idx)] = full_ref[arr, cols(first + idx), :].T
            return 0
        lax.fori_loop(0, num_tiles // 2, body, 0)

    def arrive(arrays):
        for arr in arrays:
            cross_copy(arr).wait_recv()
            fwd_copy(arr).start()
        for arr in arrays:
            fwd_copy(arr).wait_recv()
            if arr < 3:
                transpose_half(arr, 1 - chip)

    def part_copy(slot, pair_idx, arr):
        tile = 2 * pair_idx + 1 - core
        at = num_tiles - 1 - tile if arr == 2 else tile
        return to_device(acc_ref.at[arr, :, cols(at)], part_ref.at[slot, arr],
                         part_send.at[slot, arr], part_recv.at[slot, arr], core_peer)

    def start_parts(slot, pair_idx):
        for arr in range(3):
            part_copy(slot, pair_idx, arr).start()

    def deliver(tile, stage, part, send_sem, start):
        owner = lax.div(tile, block_tiles)
        local = tile - owner * block_tiles
        where = pl.ds(0, 2) if part == 0 else pl.ds(2, 3)

        @pl.when(owner == dev)
        def _():
            if start:
                pltpu.make_async_copy(stage, res_own_ref.at[local, where], res_sems.at[0, part, local]).start()

        @pl.when(owner == core_peer)
        def _():
            copy = to_device(stage, res_own_ref.at[local, where], send_sem, res_sems.at[0, part, local], owner)
            copy.start() if start else copy.wait_send()

        @pl.when(lax.div(owner, 2) != chip)
        def _():
            copy = to_device(stage, res_got_ref.at[local, where], send_sem, res_sems.at[1, part, local], owner)
            copy.start() if start else copy.wait_send()

    def finish_parts(slot, pair_idx):
        tile = 2 * pair_idx + core
        for arr in range(3):
            part_copy(slot, pair_idx, arr).wait_recv()
        d_key = (acc_ref[0, :, cols(tile)] + part_ref[slot, 0]) * inv_sqrt
        st_grad_ref[slot, 0] = d_key.astype(BF16).T
        d_val = acc_ref[1, :, cols(tile)] + part_ref[slot, 1]
        st_grad_ref[slot, 1] = d_val.astype(BF16).T
        d_off = ((acc_ref[2, :, cols(num_tiles - 1 - tile)] + part_ref[slot, 2]) * inv_sqrt).astype(BF16)
        flip_rows = exchange_matrix()
        for chunk in range(NSUB):
            back = lax.dot_general(flip_rows, d_off[:, sub(chunk)], (((1,), (1,)), ((), ())), preferred_element_type=F32)
            st_grad_ref[slot, 2, sub(NSUB - 1 - chunk)] = back.astype(BF16)
        deliver(tile, st_grad_ref.at[slot], 1, grad_send.at[slot], True)

    def pair_of(idx):
        return jnp.where(idx < half_steps, (2 - chip) * half_steps - 1 - idx, idx - half_steps + half_steps * chip)

    @pl.when(step == 0)
    def _():
        barrier = pltpu.get_barrier_semaphore()
        for peer in (core_peer, chip_peer, 3 - dev):
            pl.semaphore_signal(barrier, inc=1, device_id={'cp': peer}, device_id_type=pl.DeviceIdType.MESH)
        pl.semaphore_wait(barrier, 3)
        local = [pltpu.make_async_copy(own_ref.at[arr], place(arr, dev), local_sems.at[arr]) for arr in range(5)]
        for arr in range(5):
            cross_copy(arr).start()
            own_copy(arr).start()
            local[arr].start()

        def clear(tile, _):
            acc_ref[:, :, cols(tile)] = jnp.zeros((3, SUB, TILE), F32)
            return 0
        lax.fori_loop(0, num_tiles, clear, 0)
        bias_ref[...] = jnp.zeros_like(bias_ref)
        for arr in range(5):
            local[arr].wait()
            own_copy(arr).wait_recv()
            if arr < 3:
                transpose_half(arr, chip)

    @pl.when(step == half_steps * (1 - chip))
    def _():
        arrive((0, 1, 2))

    @pl.when(step == half_steps)
    def _():
        arrive((3, 4))

    rows_at = cols(blk)
    d_out = do_ref[rows_at, :]
    q_wide = q_ref[rows_at, :].astype(F32)
    q_u = (q_wide + u_ref[...]).astype(BF16)
    q_v = (q_wide + v_ref[...]).astype(BF16)
    qu_ref[...] = q_u
    qv_ref[...] = q_v
    qut_ref[...] = q_u.T
    qvt_ref[...] = q_v.T
    dot_ref[...] = d_out.T
    max_ref[...] = jnp.full_like(max_ref, -jnp.inf)
    sum_ref[...] = jnp.zeros_like(sum_ref)
    gu_ref[...] = jnp.zeros_like(gu_ref)
    gv_ref[...] = jnp.zeros_like(gv_ref)
    lane = lax.broadcasted_iota(jnp.int32, (SUB, SUB), 1)
    row = lax.broadcasted_iota(jnp.int32, (SUB, SUB), 0)
    upper = lane > row
    flip = 7 - lax.broadcasted_iota(jnp.int32, (8, SUB), 0)
    lower = lane + row < SUB - 1
    first_rel = num_tiles - 1 - blk

    def rotate_rel(tile, slot):
        for half in range(2):
            start = pl.multiple_of(tile * TILE + half * 256, 256)
            by_offset = dot(qv_ref[...], relt_ref[:, pl.ds(start, 256)])
            for a in range(NSUB):
                for c in range(2):
                    part = by_offset[sub(a), sub(c)]
                    rot_ref[slot, sub(a), sub(half * 2 + c)] = pltpu.roll(part, 1, 1, stride=1, stride_axis=0)

    rotate_rel(first_rel, 0)

    def score_tile(tile, diag):
        left = lax.rem(tile, 2)
        right = 1 - left
        if not diag:
            rotate_rel(first_rel + tile + 1, right)
        for half in range(2):
            start = pl.multiple_of(tile * TILE + half * 256, 256)
            content = dot(qu_ref[...], kt_ref[:, pl.ds(start, 256)])
            for a in range(NSUB):
                run_max = max_ref[sub(a), :]
                for c2 in range(2):
                    c = half * 2 + c2
                    hi, lo = c - a + NSUB, c - a + NSUB - 1
                    if diag and c > a:
                        score = jnp.full((SUB, SUB), -jnp.inf, F32)
                    else:
                        low_part = rot_ref[left if lo < NSUB else right, sub(a), sub(lo % NSUB)]
                        if diag and c == a:
                            score = jnp.where(upper, -jnp.inf, content[sub(a), sub(c2)] + low_part)
                        else:
                            high_part = rot_ref[left if hi < NSUB else right, sub(a), sub(hi % NSUB)]
                            score = content[sub(a), sub(c2)] + jnp.where(upper, high_part, low_part)
                    run_max = jnp.maximum(run_max, score)
                    sc_ref[sub(a), pl.ds(pl.multiple_of(tile * TILE + c * SUB, SUB), SUB)] = score
                max_ref[sub(a), :] = run_max

    def score_body(tile, _):
        score_tile(tile, False)
        return 0

    lax.fori_loop(0, blk, score_body, 0)
    score_tile(blk, True)
    row_ref[...] = jnp.broadcast_to(jnp.max(max_ref[...], axis=1, keepdims=True) * scale, (TILE, SUB))

    def prob_body(tile, _):
        for a in range(NSUB):
            run_sum = sum_ref[sub(a), :]
            row_max = row_ref[sub(a), :]
            for c in range(NSUB):
                where = pl.ds(pl.multiple_of(tile * TILE + c * SUB, SUB), SUB)
                prob = jnp.exp2(sc_ref[sub(a), where] * scale - row_max)
                sc_ref[sub(a), where] = prob
                p_ref[sub(a), sub(c)] = prob.astype(BF16)
                run_sum = run_sum + prob
            sum_ref[sub(a), :] = run_sum
        gu_ref[...] += dot(p_ref[...], val_ref[cols(tile), :])
        return 0

    lax.fori_loop(0, blk + 1, prob_body, 0)
    inv_sum = 1.0 / jnp.sum(sum_ref[...], axis=1, keepdims=True)
    out = gu_ref[...] * inv_sum
    st_rows_ref[step, 0] = out.astype(BF16)
    delta = jnp.sum(out * do_ref[rows_at, :].astype(F32), axis=1, keepdims=True)
    row_ref[...] = jnp.broadcast_to(delta, (TILE, SUB))
    sum_ref[...] = jnp.broadcast_to(inv_sum, (TILE, SUB))
    gu_ref[...] = jnp.zeros_like(gu_ref)
    ds_ref[1, :, :] = jnp.zeros((TILE, TILE), F32)

    def grad_body(tile, _):
        now = lax.rem(tile, 2)
        old = 1 - now
        for half in range(2):
            start = pl.multiple_of(tile * TILE + half * 256, 256)
            d_prob = dot(do_ref[rows_at, :], valt_ref[:, pl.ds(start, 256)])
            for a in range(NSUB):
                inv = sum_ref[sub(a), :]
                shift = row_ref[sub(a), :]
                for c2 in range(2):
                    c = half * 2 + c2
                    prob = sc_ref[sub(a), pl.ds(pl.multiple_of(tile * TILE + c * SUB, SUB), SUB)] * inv
                    p_ref[sub(a), sub(c)] = prob.astype(BF16)
                    d_score = prob * (d_prob[sub(a), sub(c2)] - shift)
                    dw_ref[sub(a), sub(c)] = d_score.astype(BF16)
                    ds_ref[now, sub(a), sub(c)] = roll_left(d_score, flip)
            win = pl.ds(start, 256)
            dv_ref[:, win] += dot(dot_ref[...], p_ref[:, half * 256:half * 256 + 256])
            dk_ref[:, win] += dot(qut_ref[...], dw_ref[:, half * 256:half * 256 + 256])
        gu_ref[...] += dot(dw_ref[...], k_ref[cols(tile), :])
        for a in range(NSUB):
            for y in range(NSUB):
                c_lo = y + a - NSUB
                c_hi = c_lo + 1
                lo_part = ds_ref[now if c_lo >= 0 else old, sub(a), sub(c_lo % NSUB)]
                hi_part = ds_ref[now if c_hi >= 0 else old, sub(a), sub(c_hi % NSUB)]
                p_ref[sub(a), sub(y)] = jnp.where(lower, lo_part, hi_part).astype(BF16)
        rel_tile = first_rel + tile
        gv_ref[...] += dot(p_ref[...], rel_ref[cols(rel_tile), :])
        for half in range(2):
            start = pl.multiple_of(rel_tile * TILE + half * 256, 256)
            drel_ref[:, pl.ds(start, 256)] += dot(qvt_ref[...], p_ref[:, half * 256:half * 256 + 256])
        return 0

    @pl.when(step > half_steps)
    def _():
        finish_parts(step - half_steps - 1, pair_of(step - half_steps - 1))

    lax.fori_loop(0, blk + 1, grad_body, 0)
    grad_u = gu_ref[...] * inv_sqrt
    grad_v = gv_ref[...] * inv_sqrt
    st_rows_ref[step, 1] = (grad_u + grad_v).astype(BF16)
    bias_ref[0:1, :] += jnp.sum(grad_u, axis=0, keepdims=True)
    bias_ref[1:2, :] += jnp.sum(grad_v, axis=0, keepdims=True)
    deliver(blk, st_rows_ref.at[step], 0, rows_send.at[step], True)

    @pl.when(step >= half_steps)
    def _():
        start_parts(step - half_steps, pair)

    @pl.when(step == last)
    def _():
        def start_rest(idx, _):
            start_parts(idx, pair_of(idx))
            return 0

        def finish_rest(idx, _):
            finish_parts(idx, pair_of(idx))
            return 0

        def drain(idx, _):
            for arr in range(3):
                part_copy(idx, pair_of(idx), arr).wait_send()
            deliver(2 * pair_of(idx) + core, st_grad_ref.at[idx], 1, grad_send.at[idx], False)
            pair_idx = jnp.where(idx < half_steps, idx + half_steps * chip, (3 - chip) * half_steps - 1 - idx)
            odd_idx = lax.rem(pair_idx, 2)
            deliver(2 * pair_idx + odd_idx + core - 2 * odd_idx * core, st_rows_ref.at[idx], 0, rows_send.at[idx], False)
            return 0

        lax.fori_loop(half_steps, 2 * half_steps, start_rest, 0)
        lax.fori_loop(half_steps - 1, 2 * half_steps, finish_rest, 0)
        lax.fori_loop(0, 2 * half_steps, drain, 0)
        for arr in range(5):
            own_copy(arr).wait_send()
            cross_copy(arr).wait_send()
            fwd_copy(arr).wait_send()
        for which, res in enumerate((res_own_ref, res_got_ref)):
            for local in range(block_tiles):
                for part, where in enumerate((pl.ds(0, 2), pl.ds(2, 3))):
                    dst = res.at[local, where]
                    pltpu.make_async_copy(dst, dst, res_sems.at[which, part, local]).wait()


def run_attn(u_bias, v_bias, own, away):
    _, block_len, head_dim = own.shape
    seq_len = 4 * block_len
    num_tiles = seq_len // TILE
    steps = num_tiles // 2
    block_tiles = block_len // TILE
    vec = pl.BlockSpec(memory_space=pltpu.VMEM)
    hbm = pl.BlockSpec(memory_space=pl.ANY)
    result = jax.ShapeDtypeStruct((block_tiles, 5, TILE, head_dim), BF16)
    dma = pltpu.SemaphoreType.DMA
    return pl.pallas_call(
        functools.partial(attn_kernel, num_tiles, head_dim ** -0.5),
        grid=(steps,),
        in_specs=[vec, vec, hbm, hbm],
        out_specs=[hbm, hbm, vec],
        scratch_shapes=[
            pltpu.VMEM((5, seq_len, head_dim), BF16),
            pltpu.VMEM((3, head_dim, seq_len), F32),
            pltpu.VMEM((head_dim, seq_len), BF16),
            pltpu.VMEM((head_dim, seq_len), BF16),
            pltpu.VMEM((head_dim, seq_len), BF16),
            pltpu.VMEM((TILE, seq_len), F32),
            pltpu.VMEM((2, TILE, TILE), F32),
            pltpu.VMEM((2, TILE, TILE), F32),
            pltpu.VMEM((TILE, TILE), BF16),
            pltpu.VMEM((TILE, TILE), BF16),
            pltpu.VMEM((TILE, head_dim), BF16),
            pltpu.VMEM((TILE, head_dim), BF16),
            pltpu.VMEM((head_dim, TILE), BF16),
            pltpu.VMEM((head_dim, TILE), BF16),
            pltpu.VMEM((head_dim, TILE), BF16),
            pltpu.VMEM((TILE, SUB), F32),
            pltpu.VMEM((TILE, SUB), F32),
            pltpu.VMEM((TILE, head_dim), F32),
            pltpu.VMEM((TILE, head_dim), F32),
            pltpu.VMEM((TILE, SUB), F32),
            pltpu.VMEM((steps, 2, TILE, head_dim), BF16),
            pltpu.VMEM((steps, 3, TILE, head_dim), BF16),
            pltpu.VMEM((steps, 3, head_dim, TILE), F32),
            dma((5,)), dma((5,)), dma((5,)), dma((5,)), dma((5,)), dma((5,)), dma((5,)),
            dma((steps, 3)), dma((steps, 3)), dma((steps,)), dma((steps,)), dma((2, 2, block_tiles)),
        ],
        out_shape=[result, result, jax.ShapeDtypeStruct((2, head_dim), F32)],
        compiler_params=pltpu.CompilerParams(
            dimension_semantics=("arbitrary",), vmem_limit_bytes=62 * 1024 * 1024, collective_id=0, has_side_effects=True),
        name="attn_rows",
    )(u_bias, v_bias, own, away)


def exchange_matrix():
    row = lax.broadcasted_iota(jnp.int32, (SUB, SUB), 0)
    col = lax.broadcasted_iota(jnp.int32, (SUB, SUB), 1)
    return jnp.where(row + col == SUB - 1, 1.0, 0.0).astype(BF16)


def pack_kernel(k_ref, v_ref, q_ref, do_ref, table_ref, w_ref, own_ref, send_ref):
    chip = lax.div(lax.axis_index('cp'), 2)
    flip = exchange_matrix()
    weights = jnp.swapaxes(w_ref[...], 0, 1)

    def put(arr, at, heads):
        first = chip == 0
        own_ref[arr, at] = jnp.where(first, heads[0], heads[1])
        send_ref[arr, at] = jnp.where(first, heads[1], heads[0])

    for arr, src in ((0, k_ref), (1, v_ref), (3, q_ref), (4, do_ref)):
        put(arr, slice(None), jnp.swapaxes(src[...], 0, 1))
    chunks = table_ref.shape[0] // SUB
    both = jnp.concatenate([weights[0], weights[1]], axis=1)
    for chunk in range(chunks):
        rel = dot(table_ref[sub(chunk), :], both).astype(BF16)
        rel = dot(flip, rel).astype(BF16)
        put(2, sub(chunks - 1 - chunk), (rel[:, :SUB], rel[:, SUB:]))


def unpack_kernel(own_ref, got_ref, o_ref, dq_ref, dk_ref, dv_ref):
    chip = lax.div(lax.axis_index('cp'), 2)
    for tile in range(own_ref.shape[0]):
        rows = slice(tile * TILE, (tile + 1) * TILE)
        for arr, dst in enumerate((o_ref, dq_ref, dk_ref, dv_ref)):
            own, got = own_ref[tile, arr], got_ref[tile, arr]
            dst[rows] = jnp.stack([jnp.where(chip == 0, own, got), jnp.where(chip == 0, got, own)], axis=1)


def weight_kernel(own_ref, got_ref, table_ref, bias_ref, dw_ref, du_ref, dvb_ref,
                  part_ref, core_ref, chip_ref, sum_ref, final_ref, send_sems, recv_sems):
    dev = lax.axis_index('cp')
    chip, core = lax.div(dev, 2), lax.rem(dev, 2)
    core_peer, chip_peer = dev + 1 - 2 * core, dev + 2 - 4 * chip
    barrier = pltpu.get_barrier_semaphore()
    for peer in (core_peer, chip_peer):
        pl.semaphore_signal(barrier, inc=1, device_id={'cp': peer}, device_id_type=pl.DeviceIdType.MESH)
    pl.semaphore_wait(barrier, 2)
    own = jnp.concatenate([own_ref[tile, 4] for tile in range(own_ref.shape[0])], axis=0)
    got = jnp.concatenate([got_ref[tile, 4] for tile in range(got_ref.shape[0])], axis=0)
    d_rel = jnp.concatenate([jnp.where(chip == 0, own, got), jnp.where(chip == 0, got, own)], axis=1)
    model_dim = table_ref.shape[1]
    half_rows = part_ref.shape[1]
    flat = part_ref.shape[0] * half_rows
    for start in range(0, flat, 256):
        size = min(256, model_dim - start) if start < model_dim else 0
        rows = []
        if size > 0:
            rows.append(lax.dot_general(table_ref[:, start:start + size], d_rel, (((0,), (0,)), ((), ())), preferred_element_type=F32))
        else:
            bias = bias_ref[...]
            zero = jnp.zeros_like(bias)
            both = jnp.concatenate([jnp.where(chip == 0, bias, zero), jnp.where(chip == 0, zero, bias)], axis=1)
            rows.append(jnp.concatenate([both, jnp.zeros((flat - start - bias.shape[0], both.shape[1]), F32)], axis=0))
        block = rows[0]
        for at in range(0, block.shape[0], 8):
            pos = start + at
            part_ref[pos // half_rows, pos % half_rows:pos % half_rows + 8] = block[at:at + 8]

    def swap(idx, src, dst, peer):
        copy = pltpu.make_async_remote_copy(
            src_ref=src, dst_ref=dst, send_sem=send_sems.at[idx], recv_sem=recv_sems.at[idx],
            device_id={'cp': peer}, device_id_type=pl.DeviceIdType.MESH)
        copy.start()
        return copy

    first = swap(0, part_ref.at[1 - core], core_ref, core_peer)
    first.wait()
    sum_ref[...] = part_ref[core] + core_ref[...]
    second = swap(1, sum_ref, chip_ref, chip_peer)
    second.wait()
    final_ref[core] = sum_ref[...] + chip_ref[...]
    third = swap(2, final_ref.at[core], final_ref.at[core], core_peer)
    third.wait()
    total = jnp.concatenate([final_ref[0], final_ref[1]], axis=0)
    dw_ref[...] = jnp.stack([total[:model_dim, :SUB], total[:model_dim, SUB:]], axis=1)
    du_ref[...] = jnp.concatenate([total[model_dim:model_dim + 1, :SUB], total[model_dim:model_dim + 1, SUB:]], axis=0)
    dvb_ref[...] = jnp.concatenate([total[model_dim + 1:model_dim + 2, :SUB], total[model_dim + 1:model_dim + 2, SUB:]], axis=0)


def weight_grad(own, got, rel_table, bias_grad, w_shape):
    model_dim = w_shape[0]
    half_rows = model_dim // 2 + 8
    wide = 2 * SUB
    vmem = pl.BlockSpec(memory_space=pltpu.VMEM)
    bias = jax.ShapeDtypeStruct((2, SUB), F32)
    return pl.pallas_call(
        weight_kernel,
        in_specs=[vmem] * 4,
        out_specs=[vmem] * 3,
        out_shape=[jax.ShapeDtypeStruct(w_shape, F32), bias, bias],
        scratch_shapes=[
            pltpu.VMEM((2, half_rows, wide), F32),
            pltpu.VMEM((half_rows, wide), F32),
            pltpu.VMEM((half_rows, wide), F32),
            pltpu.VMEM((half_rows, wide), F32),
            pltpu.VMEM((2, half_rows, wide), F32),
            pltpu.SemaphoreType.DMA((3,)),
            pltpu.SemaphoreType.DMA((3,)),
        ],
        compiler_params=pltpu.CompilerParams(vmem_limit_bytes=48 * 1024 * 1024, collective_id=1, has_side_effects=True),
        name="weight_grad",
    )(own, got, rel_table, bias_grad)


def simple_call(body, out_shape, name):
    vmem = pl.BlockSpec(memory_space=pltpu.VMEM)
    return pl.pallas_call(
        body, out_shape=out_shape, out_specs=[vmem] * len(out_shape), name=name,
        compiler_params=pltpu.CompilerParams(vmem_limit_bytes=48 * 1024 * 1024))


def solution(mesh):
    seq_spec = P('cp', 'hp', None)
    head_spec = P('hp', None)
    weight_spec = P(None, 'hp', None)

    def local_fn(q, k, v, u_bias, v_bias, rel_table, w_rel, d_out):
        block_len, _, head_dim = q.shape
        chip = lax.axis_index('cp') // 2
        five = jax.ShapeDtypeStruct((5, block_len, head_dim), BF16)
        seq = jax.ShapeDtypeStruct(q.shape, BF16)
        own, away = simple_call(pack_kernel, [five, five], "pack")(k, v, q, d_out, rel_table, w_rel)
        u_mine = lax.dynamic_slice_in_dim(u_bias, chip, 1)
        v_mine = lax.dynamic_slice_in_dim(v_bias, chip, 1)
        res_own, res_got, bias_grad = run_attn(u_mine, v_mine, own, away)
        d_w_rel, d_u, d_v = weight_grad(res_own, res_got, rel_table, bias_grad, w_rel.shape)
        out, dq, dk, dv = simple_call(unpack_kernel, [seq] * 4, "unpack")(res_own, res_got)
        return out, dq, dk, dv, d_u, d_v, d_w_rel

    return jax.shard_map(
        local_fn,
        mesh=mesh,
        in_specs=(seq_spec, seq_spec, seq_spec, head_spec, head_spec, P('cp', None), weight_spec, seq_spec),
        out_specs=(seq_spec, seq_spec, seq_spec, seq_spec, head_spec, head_spec, weight_spec),
        check_vma=False,
    )
```

```python
import functools

import jax
import jax.numpy as jnp
from jax import lax
from jax.experimental import pallas as pl
from jax.experimental.pallas import tpu as pltpu
from jax.sharding import PartitionSpec as P

TILE = 512
SUB = 128
NSUB = TILE // SUB
MROWS = 2
LOG2E = 1.4426950408889634
F32 = jnp.float32
BF16 = jnp.bfloat16


def dot(lhs, rhs):
    return jnp.dot(lhs, rhs, preferred_element_type=F32)


def sub(idx):
    return slice(idx * SUB, (idx + 1) * SUB)


def roll_left(part, flip):
    groups = []
    for start in range(0, SUB, 8):
        rows = jnp.take_along_axis(part[start:start + 8], flip, axis=0)
        rows = pltpu.roll(rows, (SUB - 8 - start) % SUB, 1, stride=1, stride_axis=0)
        groups.append(jnp.take_along_axis(rows, flip, axis=0))
    return jnp.concatenate(groups, axis=0)


def attn_kernel(num_tiles, inv_sqrt, u_ref, v_ref, kin_ref, vin_ref, qin_ref, doin_ref, table_in_ref, w_in_ref,
                res_own_ref, res_got_ref, bias_ref,
                full_ref, acc_ref, kt_ref, valt_ref, relt_ref, sc_ref, rot_ref, ds_ref, dw_ref, p_ref,
                qu_ref, qv_ref, qut_ref, qvt_ref, dot_ref, max_ref, sum_ref, gu_ref, gv_ref, row_ref,
                st_rows_ref, st_grad_ref, part_ref, away_ref, raw_ref, table_ref, w_ref, wide_ref,
                local_sems, own_send, own_recv, cross_send, cross_recv, fwd_send, fwd_recv,
                part_send, part_recv, rows_send, grad_send, res_sems):
    step = pl.program_id(0)
    last = pl.num_programs(0) - 1
    dev = lax.axis_index('cp')
    chip, core = lax.div(dev, 2), lax.rem(dev, 2)
    core_peer, chip_peer = dev + 1 - 2 * core, dev + 2 - 4 * chip
    half_steps = num_tiles // 4
    pair = jnp.where(step < half_steps, step + half_steps * chip, (3 - chip) * half_steps - 1 - step)
    odd = lax.rem(pair, 2)
    blk = 2 * pair + odd + core - 2 * odd * core
    scale = inv_sqrt * LOG2E
    block_len = away_ref.shape[1]
    block_tiles = block_len // TILE
    k_ref, val_ref, rel_ref = full_ref.at[0], full_ref.at[1], full_ref.at[2]
    q_ref, do_ref = full_ref.at[3], full_ref.at[4]
    dk_ref, dv_ref, drel_ref = acc_ref.at[0], acc_ref.at[1], acc_ref.at[2]

    def cols(tile):
        return pl.ds(pl.multiple_of(tile * TILE, TILE), TILE)

    def place(arr, block):
        at = 3 - block if arr == 2 else block
        return full_ref.at[arr, pl.ds(pl.multiple_of(at * block_len, block_len), block_len)]

    def to_device(src, dst, send_sem, recv_sem, peer):
        return pltpu.make_async_remote_copy(
            src_ref=src, dst_ref=dst, send_sem=send_sem, recv_sem=recv_sem,
            device_id={'cp': peer}, device_id_type=pl.DeviceIdType.MESH)

    def own_copy(arr):
        return to_device(place(arr, dev), place(arr, dev), own_send.at[arr], own_recv.at[arr], core_peer)

    def cross_copy(arr):
        return to_device(away_ref.at[arr], place(arr, dev), cross_send.at[arr], cross_recv.at[arr], chip_peer)

    def fwd_copy(arr):
        return to_device(place(arr, chip_peer), place(arr, chip_peer), fwd_send.at[arr], fwd_recv.at[arr], core_peer)

    def transpose_half(arr, which):
        dst = (kt_ref, valt_ref, relt_ref)[arr]
        first = (1 - which if arr == 2 else which) * (num_tiles // 2)

        def body(idx, _):
            dst[:, cols(first + idx)] = full_ref[arr, cols(first + idx), :].T
            return 0
        lax.fori_loop(0, num_tiles // 2, body, 0)

    def arrive(arrays):
        for arr in arrays:
            cross_copy(arr).wait_recv()
            fwd_copy(arr).start()
        for arr in arrays:
            fwd_copy(arr).wait_recv()
            if arr < 3:
                transpose_half(arr, 1 - chip)

    def part_copy(slot, pair_idx, arr):
        tile = 2 * pair_idx + 1 - core
        at = num_tiles - 1 - tile if arr == 2 else tile
        return to_device(acc_ref.at[arr, :, cols(at)], part_ref.at[slot, arr],
                         part_send.at[slot, arr], part_recv.at[slot, arr], core_peer)

    def start_parts(slot, pair_idx):
        for arr in range(3):
            part_copy(slot, pair_idx, arr).start()

    def deliver(tile, stage, part, send_sem, start):
        owner = lax.div(tile, block_tiles)
        local = tile - owner * block_tiles
        where = pl.ds(0, 2) if part == 0 else pl.ds(2, 3)

        @pl.when(owner == dev)
        def _():
            if start:
                pltpu.make_async_copy(stage, res_own_ref.at[local, where], res_sems.at[0, part, local]).start()

        @pl.when(owner == core_peer)
        def _():
            copy = to_device(stage, res_own_ref.at[local, where], send_sem, res_sems.at[0, part, local], owner)
            copy.start() if start else copy.wait_send()

        @pl.when(lax.div(owner, 2) != chip)
        def _():
            copy = to_device(stage, res_got_ref.at[local, where], send_sem, res_sems.at[1, part, local], owner)
            copy.start() if start else copy.wait_send()

    def finish_parts(slot, pair_idx):
        tile = 2 * pair_idx + core
        for arr in range(3):
            part_copy(slot, pair_idx, arr).wait_recv()
        d_key = (acc_ref[0, :, cols(tile)] + part_ref[slot, 0]) * inv_sqrt
        st_grad_ref[slot, 0] = d_key.astype(BF16).T
        d_val = acc_ref[1, :, cols(tile)] + part_ref[slot, 1]
        st_grad_ref[slot, 1] = d_val.astype(BF16).T
        d_off = ((acc_ref[2, :, cols(num_tiles - 1 - tile)] + part_ref[slot, 2]) * inv_sqrt).astype(BF16)
        flip_rows = exchange_matrix()
        for chunk in range(NSUB):
            back = lax.dot_general(flip_rows, d_off[:, sub(chunk)], (((1,), (1,)), ((), ())), preferred_element_type=F32)
            st_grad_ref[slot, 2, sub(NSUB - 1 - chunk)] = back.astype(BF16)
        deliver(tile, st_grad_ref.at[slot], 1, grad_send.at[slot], True)

    def pair_of(idx):
        return jnp.where(idx < half_steps, (2 - chip) * half_steps - 1 - idx, idx - half_steps + half_steps * chip)

    def put_heads(arr, start, size, first, second):
        at = 3 - dev if arr == 2 else dev
        own_at = pl.ds(pl.multiple_of(at * block_len + start, SUB), size)
        away_at = pl.ds(pl.multiple_of(start, SUB), size)
        full_ref[arr, own_at] = jnp.where(chip == 0, first, second)
        away_ref[arr, away_at] = jnp.where(chip == 0, second, first)

    def pack_seq(arr, src):
        def body(idx, _):
            heads = jnp.swapaxes(raw_ref[src, cols(idx)], 0, 1)
            put_heads(arr, idx * TILE, TILE, heads[0], heads[1])
            return 0
        lax.fori_loop(0, block_tiles, body, 0)

    def pack_rel():
        weights = jnp.swapaxes(w_ref[...], 0, 1)
        wide_ref[:, :SUB] = weights[0]
        wide_ref[:, SUB:] = weights[1]

        def body(idx, _):
            rel = dot(table_ref[cols(idx), :], wide_ref[...]).astype(BF16)
            flip_rows = exchange_matrix()
            for chunk in range(NSUB):
                back = dot(flip_rows, rel[sub(NSUB - 1 - chunk)]).astype(BF16)
                put_heads(2, (block_tiles - 1 - idx) * TILE + chunk * SUB, SUB, back[:, :SUB], back[:, SUB:])
            return 0
        lax.fori_loop(0, block_tiles, body, 0)

    @pl.when(step == 0)
    def _():
        barrier = pltpu.get_barrier_semaphore()
        for peer in (core_peer, chip_peer, 3 - dev):
            pl.semaphore_signal(barrier, inc=1, device_id={'cp': peer}, device_id_type=pl.DeviceIdType.MESH)
        loads = [pltpu.make_async_copy(src, dst, local_sems.at[idx]) for idx, (src, dst) in enumerate((
            (kin_ref, raw_ref.at[0]), (w_in_ref, w_ref), (table_in_ref, table_ref),
            (vin_ref, raw_ref.at[1]), (qin_ref, raw_ref.at[2]), (doin_ref, raw_ref.at[3])))]
        for load in loads:
            load.start()

        def clear(tile, _):
            acc_ref[:, :, cols(tile)] = jnp.zeros((3, SUB, TILE), F32)
            return 0

        def ship(arr):
            cross_copy(arr).start()
            own_copy(arr).start()

        loads[0].wait()
        pack_seq(0, 0)
        pl.semaphore_wait(barrier, 3)
        ship(0)
        loads[1].wait()
        loads[2].wait()
        pack_rel()
        ship(2)
        for idx, arr in enumerate((1, 3, 4)):
            loads[3 + idx].wait()
            pack_seq(arr, idx + 1)
            ship(arr)
        lax.fori_loop(0, num_tiles, clear, 0)
        bias_ref[...] = jnp.zeros_like(bias_ref)
        for arr in (0, 2, 1, 3, 4):
            own_copy(arr).wait_recv()
            if arr < 3:
                transpose_half(arr, chip)

    @pl.when(step == half_steps * (1 - chip))
    def _():
        arrive((0, 2))

    @pl.when(step == half_steps)
    def _():
        arrive((3, 4))

    rows_at = cols(blk)
    d_out = do_ref[rows_at, :]
    q_wide = q_ref[rows_at, :].astype(F32)
    q_u = (q_wide + u_ref[...]).astype(BF16)
    q_v = (q_wide + v_ref[...]).astype(BF16)
    qu_ref[...] = q_u
    qv_ref[...] = q_v
    qut_ref[...] = q_u.T
    qvt_ref[...] = q_v.T
    dot_ref[...] = d_out.T
    max_ref[...] = jnp.full_like(max_ref, -jnp.inf)
    sum_ref[...] = jnp.zeros_like(sum_ref)
    gu_ref[...] = jnp.zeros_like(gu_ref)
    gv_ref[...] = jnp.zeros_like(gv_ref)
    lane = lax.broadcasted_iota(jnp.int32, (SUB, SUB), 1)
    row = lax.broadcasted_iota(jnp.int32, (SUB, SUB), 0)
    upper = lane > row
    flip = 7 - lax.broadcasted_iota(jnp.int32, (8, SUB), 0)
    lower = lane + row < SUB - 1
    first_rel = num_tiles - 1 - blk

    def rotate_rel(tile, slot):
        for half in range(2):
            start = pl.multiple_of(tile * TILE + half * 256, 256)
            for a in range(NSUB):
                if a % MROWS == 0:
                    by_offset = dot(qv_ref[a * SUB:(a + MROWS) * SUB, :], relt_ref[:, pl.ds(start, 256)])
                for c in range(2):
                    part = by_offset[sub(a % MROWS), sub(c)]
                    rot_ref[slot, sub(a), sub(half * 2 + c)] = pltpu.roll(part, 1, 1, stride=1, stride_axis=0)

    rotate_rel(first_rel, 0)

    @pl.when(blk > 0)
    def _():
        rotate_rel(first_rel + 1, 1)

    def score_tile(tile, diag):
        left = lax.rem(tile, 3)
        right = lax.rem(tile + 1, 3)
        for half in range(2):
            start = pl.multiple_of(tile * TILE + half * 256, 256)
            for a in range(NSUB):
                if a % MROWS == 0:
                    content = dot(qu_ref[a * SUB:(a + MROWS) * SUB, :], kt_ref[:, pl.ds(start, 256)])
                run_max = max_ref[sub(a), :]
                for c2 in range(2):
                    c = half * 2 + c2
                    hi, lo = c - a + NSUB, c - a + NSUB - 1
                    if diag and c > a:
                        score = jnp.full((SUB, SUB), -jnp.inf, F32)
                    else:
                        low_part = rot_ref[left if lo < NSUB else right, sub(a), sub(lo % NSUB)]
                        if diag and c == a:
                            score = jnp.where(upper, -jnp.inf, (content[sub(a % MROWS), sub(c2)] + low_part) * scale)
                        else:
                            high_part = rot_ref[left if hi < NSUB else right, sub(a), sub(hi % NSUB)]
                            score = (content[sub(a % MROWS), sub(c2)] + jnp.where(upper, high_part, low_part)) * scale
                    run_max = jnp.maximum(run_max, score)
                    sc_ref[sub(a), pl.ds(pl.multiple_of(tile * TILE + c * SUB, SUB), SUB)] = score
                max_ref[sub(a), :] = run_max
        if not diag:
            rotate_rel(jnp.minimum(first_rel + tile + 2, num_tiles - 1), lax.rem(tile + 2, 3))

    def score_body(tile, _):
        score_tile(tile, False)
        return 0

    lax.fori_loop(0, blk, score_body, 0)
    score_tile(blk, True)
    max_ref[...] = jnp.broadcast_to(jnp.max(max_ref[...], axis=1, keepdims=True), (TILE, SUB))

    @pl.when(step == half_steps * (1 - chip))
    def _():
        arrive((1,))

    def prob_body(tile, _):
        for a in range(NSUB):
            run_sum = sum_ref[sub(a), :]
            row_max = max_ref[sub(a), :]
            for c in range(NSUB):
                where = pl.ds(pl.multiple_of(tile * TILE + c * SUB, SUB), SUB)
                prob = jnp.exp2(sc_ref[sub(a), where] - row_max)
                p_ref[sub(a), sub(c)] = prob.astype(BF16)
                run_sum = run_sum + prob
            sum_ref[sub(a), :] = run_sum
        gu_ref[...] += dot(p_ref[...], val_ref[cols(tile), :])
        return 0

    lax.fori_loop(0, blk + 1, prob_body, 0)
    total = jnp.sum(sum_ref[...], axis=1, keepdims=True)
    inv_sum = 1.0 / total
    out = gu_ref[...] * inv_sum
    st_rows_ref[step, 0] = out.astype(BF16)
    delta = jnp.sum(out * do_ref[rows_at, :].astype(F32), axis=1, keepdims=True)
    row_ref[...] = jnp.broadcast_to(delta, (TILE, SUB))
    sum_ref[...] = max_ref[...] + jnp.log2(total)
    gu_ref[...] = jnp.zeros_like(gu_ref)
    ds_ref[1, :, :] = jnp.zeros((TILE, TILE), F32)

    def grad_body(tile, _):
        now = lax.rem(tile, 2)
        old = 1 - now
        for half in range(2):
            start = pl.multiple_of(tile * TILE + half * 256, 256)
            for a in range(NSUB):
                if a % MROWS == 0:
                    do_rows = pl.ds(pl.multiple_of(blk * TILE + a * SUB, SUB), MROWS * SUB)
                    d_prob = dot(do_ref[do_rows, :], valt_ref[:, pl.ds(start, 256)])
                log_norm = sum_ref[sub(a), :]
                shift = row_ref[sub(a), :]
                for c2 in range(2):
                    c = half * 2 + c2
                    prob = jnp.exp2(sc_ref[sub(a), pl.ds(pl.multiple_of(tile * TILE + c * SUB, SUB), SUB)] - log_norm)
                    p_ref[sub(a), sub(c)] = prob.astype(BF16)
                    d_score = prob * (d_prob[sub(a % MROWS), sub(c2)] - shift)
                    dw_ref[sub(a), sub(c)] = d_score.astype(BF16)
                    ds_ref[now, sub(a), sub(c)] = roll_left(d_score, flip)
            win = pl.ds(start, 256)
            dv_ref[:, win] += dot(dot_ref[...], p_ref[:, half * 256:half * 256 + 256])
            dk_ref[:, win] += dot(qut_ref[...], dw_ref[:, half * 256:half * 256 + 256])
        gu_ref[...] += dot(dw_ref[...], k_ref[cols(tile), :])
        for a in range(NSUB):
            for y in range(NSUB):
                c_lo = y + a - NSUB
                c_hi = c_lo + 1
                lo_part = ds_ref[now if c_lo >= 0 else old, sub(a), sub(c_lo % NSUB)]
                hi_part = ds_ref[now if c_hi >= 0 else old, sub(a), sub(c_hi % NSUB)]
                p_ref[sub(a), sub(y)] = jnp.where(lower, lo_part, hi_part).astype(BF16)
        rel_tile = first_rel + tile
        gv_ref[...] += dot(p_ref[...], rel_ref[cols(rel_tile), :])
        for half in range(2):
            start = pl.multiple_of(rel_tile * TILE + half * 256, 256)
            drel_ref[:, pl.ds(start, 256)] += dot(qvt_ref[...], p_ref[:, half * 256:half * 256 + 256])
        return 0

    @pl.when(step > half_steps)
    def _():
        finish_parts(step - half_steps - 1, pair_of(step - half_steps - 1))

    lax.fori_loop(0, blk + 1, grad_body, 0)
    grad_u = gu_ref[...] * inv_sqrt
    grad_v = gv_ref[...] * inv_sqrt
    st_rows_ref[step, 1] = (grad_u + grad_v).astype(BF16)
    bias_ref[0:1, :] += jnp.sum(grad_u, axis=0, keepdims=True)
    bias_ref[1:2, :] += jnp.sum(grad_v, axis=0, keepdims=True)
    deliver(blk, st_rows_ref.at[step], 0, rows_send.at[step], True)

    @pl.when(step >= half_steps)
    def _():
        start_parts(step - half_steps, pair)

    @pl.when(step == last)
    def _():
        def start_rest(idx, _):
            start_parts(idx, pair_of(idx))
            return 0

        def finish_rest(idx, _):
            finish_parts(idx, pair_of(idx))
            return 0

        def drain(idx, _):
            for arr in range(3):
                part_copy(idx, pair_of(idx), arr).wait_send()
            deliver(2 * pair_of(idx) + core, st_grad_ref.at[idx], 1, grad_send.at[idx], False)
            pair_idx = jnp.where(idx < half_steps, idx + half_steps * chip, (3 - chip) * half_steps - 1 - idx)
            odd_idx = lax.rem(pair_idx, 2)
            deliver(2 * pair_idx + odd_idx + core - 2 * odd_idx * core, st_rows_ref.at[idx], 0, rows_send.at[idx], False)
            return 0

        lax.fori_loop(half_steps, 2 * half_steps, start_rest, 0)
        lax.fori_loop(half_steps - 1, 2 * half_steps, finish_rest, 0)
        lax.fori_loop(0, 2 * half_steps, drain, 0)
        for arr in range(5):
            own_copy(arr).wait_send()
            cross_copy(arr).wait_send()
            fwd_copy(arr).wait_send()
        for which, res in enumerate((res_own_ref, res_got_ref)):
            for local in range(block_tiles):
                for part, where in enumerate((pl.ds(0, 2), pl.ds(2, 3))):
                    dst = res.at[local, where]
                    pltpu.make_async_copy(dst, dst, res_sems.at[which, part, local]).wait()


def run_attn(u_bias, v_bias, k, v, q, d_out, rel_table, w_rel):
    block_len, _, head_dim = k.shape
    seq_len = 4 * block_len
    num_tiles = seq_len // TILE
    steps = num_tiles // 2
    block_tiles = block_len // TILE
    vec = pl.BlockSpec(memory_space=pltpu.VMEM)
    hbm = pl.BlockSpec(memory_space=pl.ANY)
    result = jax.ShapeDtypeStruct((block_tiles, 5, TILE, head_dim), BF16)
    dma = pltpu.SemaphoreType.DMA
    return pl.pallas_call(
        functools.partial(attn_kernel, num_tiles, head_dim ** -0.5),
        grid=(steps,),
        in_specs=[vec, vec] + [hbm] * 6,
        out_specs=[hbm, hbm, vec],
        scratch_shapes=[
            pltpu.VMEM((5, seq_len, head_dim), BF16),
            pltpu.VMEM((3, head_dim, seq_len), F32),
            pltpu.VMEM((head_dim, seq_len), BF16),
            pltpu.VMEM((head_dim, seq_len), BF16),
            pltpu.VMEM((head_dim, seq_len), BF16),
            pltpu.VMEM((TILE, seq_len), F32),
            pltpu.VMEM((3, TILE, TILE), F32),
            pltpu.VMEM((2, TILE, TILE), F32),
            pltpu.VMEM((TILE, TILE), BF16),
            pltpu.VMEM((TILE, TILE), BF16),
            pltpu.VMEM((TILE, head_dim), BF16),
            pltpu.VMEM((TILE, head_dim), BF16),
            pltpu.VMEM((head_dim, TILE), BF16),
            pltpu.VMEM((head_dim, TILE), BF16),
            pltpu.VMEM((head_dim, TILE), BF16),
            pltpu.VMEM((TILE, SUB), F32),
            pltpu.VMEM((TILE, SUB), F32),
            pltpu.VMEM((TILE, head_dim), F32),
            pltpu.VMEM((TILE, head_dim), F32),
            pltpu.VMEM((TILE, SUB), F32),
            pltpu.VMEM((steps, 2, TILE, head_dim), BF16),
            pltpu.VMEM((steps, 3, TILE, head_dim), BF16),
            pltpu.VMEM((steps, 3, head_dim, TILE), F32),
            pltpu.VMEM((5, block_len, head_dim), BF16),
            pltpu.VMEM((4,) + k.shape, BF16),
            pltpu.VMEM(rel_table.shape, BF16),
            pltpu.VMEM(w_rel.shape, BF16),
            pltpu.VMEM((w_rel.shape[0], 2 * head_dim), BF16),
            dma((6,)), dma((5,)), dma((5,)), dma((5,)), dma((5,)), dma((5,)), dma((5,)),
            dma((steps, 3)), dma((steps, 3)), dma((steps,)), dma((steps,)), dma((2, 2, block_tiles)),
        ],
        out_shape=[result, result, jax.ShapeDtypeStruct((2, head_dim), F32)],
        compiler_params=pltpu.CompilerParams(
            dimension_semantics=("arbitrary",), vmem_limit_bytes=67043328, collective_id=0, has_side_effects=True),
        name="attn_rows",
    )(u_bias, v_bias, k, v, q, d_out, rel_table, w_rel)


def exchange_matrix():
    row = lax.broadcasted_iota(jnp.int32, (SUB, SUB), 0)
    col = lax.broadcasted_iota(jnp.int32, (SUB, SUB), 1)
    return jnp.where(row + col == SUB - 1, 1.0, 0.0).astype(BF16)


def finish_kernel(own_ref, got_ref, table_ref, bias_ref, o_ref, dq_ref, dk_ref, dv_ref, dw_ref, du_ref, dvb_ref,
                  rel_ref, part_ref, core_ref, sum_ref, chip_ref, final_ref, send_sems, recv_sems):
    dev = lax.axis_index('cp')
    chip, core = lax.div(dev, 2), lax.rem(dev, 2)
    core_peer, chip_peer = dev + 1 - 2 * core, dev + 2 - 4 * chip
    barrier = pltpu.get_barrier_semaphore()
    for peer in (core_peer, chip_peer):
        pl.semaphore_signal(barrier, inc=1, device_id={'cp': peer}, device_id_type=pl.DeviceIdType.MESH)
    tiles = own_ref.shape[0]
    half = table_ref.shape[1] // 2

    def heads(arr, tile):
        own, got = own_ref[tile, arr], got_ref[tile, arr]
        return jnp.where(chip == 0, own, got), jnp.where(chip == 0, got, own)

    for tile in range(tiles):
        rows = slice(tile * TILE, (tile + 1) * TILE)
        rel_ref[rows, :SUB], rel_ref[rows, SUB:] = heads(4, tile)

    def partial(which):
        for start in range(0, half, 256):
            at = pl.ds(pl.multiple_of(which * half + start, 256), 256)
            part_ref[which, start:start + 256] = lax.dot_general(
                table_ref[:, at], rel_ref[...], (((0,), (0,)), ((), ())), preferred_element_type=F32)
        bias = bias_ref[...]
        zero = jnp.zeros_like(bias)
        both = jnp.concatenate([jnp.where(chip == 0, bias, zero), jnp.where(chip == 0, zero, bias)], axis=1)
        part_ref[which, half:] = jnp.concatenate([both, jnp.zeros((6, both.shape[1]), F32)], axis=0)

    def swap(idx, src, dst, peer):
        copy = pltpu.make_async_remote_copy(
            src_ref=src, dst_ref=dst, send_sem=send_sems.at[idx], recv_sem=recv_sems.at[idx],
            device_id={'cp': peer}, device_id_type=pl.DeviceIdType.MESH)
        copy.start()
        return copy

    partial(1 - core)
    pl.semaphore_wait(barrier, 2)
    first = swap(0, part_ref.at[1 - core], core_ref, core_peer)
    partial(core)
    first.wait()
    sum_ref[...] = part_ref[core] + core_ref[...]
    second = swap(1, sum_ref, chip_ref, chip_peer)
    for tile in range(tiles):
        rows = slice(tile * TILE, (tile + 1) * TILE)
        for arr, dst in enumerate((o_ref, dq_ref, dk_ref, dv_ref)):
            dst[rows] = jnp.stack(heads(arr, tile), axis=1)
    second.wait()
    final_ref[core] = sum_ref[...] + chip_ref[...]
    third = swap(2, final_ref.at[core], final_ref.at[core], core_peer)
    third.wait()
    for which in range(2):
        dw_ref[which * half:(which + 1) * half] = jnp.stack(
            [final_ref[which, :half, :SUB], final_ref[which, :half, SUB:]], axis=1)
    tail = final_ref[0, half:]
    du_ref[...] = jnp.concatenate([tail[0:1, :SUB], tail[0:1, SUB:]], axis=0)
    dvb_ref[...] = jnp.concatenate([tail[1:2, :SUB], tail[1:2, SUB:]], axis=0)


def finish(own, got, rel_table, bias_grad, seq_shape, w_shape):
    half_rows = w_shape[0] // 2 + 8
    wide = 2 * SUB
    vmem = pl.BlockSpec(memory_space=pltpu.VMEM)
    bias = jax.ShapeDtypeStruct((2, SUB), F32)
    seq = jax.ShapeDtypeStruct(seq_shape, BF16)
    return pl.pallas_call(
        finish_kernel,
        in_specs=[vmem] * 4,
        out_specs=[vmem] * 7,
        out_shape=[seq, seq, seq, seq, jax.ShapeDtypeStruct(w_shape, F32), bias, bias],
        scratch_shapes=[
            pltpu.VMEM((rel_table.shape[0], wide), BF16),
            pltpu.VMEM((2, half_rows, wide), F32),
            pltpu.VMEM((half_rows, wide), F32),
            pltpu.VMEM((half_rows, wide), F32),
            pltpu.VMEM((half_rows, wide), F32),
            pltpu.VMEM((2, half_rows, wide), F32),
            pltpu.SemaphoreType.DMA((3,)),
            pltpu.SemaphoreType.DMA((3,)),
        ],
        compiler_params=pltpu.CompilerParams(vmem_limit_bytes=48 * 1024 * 1024, collective_id=1, has_side_effects=True),
        name="finish",
    )(own, got, rel_table, bias_grad)


def solution(mesh):
    seq_spec = P('cp', 'hp', None)
    head_spec = P('hp', None)
    weight_spec = P(None, 'hp', None)

    def local_fn(q, k, v, u_bias, v_bias, rel_table, w_rel, d_out):
        chip = lax.axis_index('cp') // 2
        u_mine = lax.dynamic_slice_in_dim(u_bias, chip, 1)
        v_mine = lax.dynamic_slice_in_dim(v_bias, chip, 1)
        res_own, res_got, bias_grad = run_attn(u_mine, v_mine, k, v, q, d_out, rel_table, w_rel)
        out, dq, dk, dv, d_w_rel, d_u, d_v = finish(res_own, res_got, rel_table, bias_grad, q.shape, w_rel.shape)
        return out, dq, dk, dv, d_u, d_v, d_w_rel

    return jax.shard_map(
        local_fn,
        mesh=mesh,
        in_specs=(seq_spec, seq_spec, seq_spec, head_spec, head_spec, P('cp', None), weight_spec, seq_spec),
        out_specs=(seq_spec, seq_spec, seq_spec, seq_spec, head_spec, head_spec, weight_spec),
        check_vma=False,
    )
```

```python
import functools

import jax
import jax.numpy as jnp
from jax import lax
from jax.experimental import pallas as pl
from jax.experimental.pallas import tpu as pltpu
from jax.sharding import PartitionSpec as P

TILE = 512
SUB = 128
NSUB = TILE // SUB
MROWS = 2
PARTS = (pl.ds(0, 2), pl.ds(2, 2), pl.ds(4, 1))
LOG2E = 1.4426950408889634
F32 = jnp.float32
BF16 = jnp.bfloat16


def dot(lhs, rhs):
    return jnp.dot(lhs, rhs, preferred_element_type=F32)


def sub(idx):
    return slice(idx * SUB, (idx + 1) * SUB)


def roll_left(part, flip):
    groups = []
    for start in range(0, SUB, 8):
        rows = jnp.take_along_axis(part[start:start + 8], flip, axis=0)
        rows = pltpu.roll(rows, (SUB - 8 - start) % SUB, 1, stride=1, stride_axis=0)
        groups.append(jnp.take_along_axis(rows, flip, axis=0))
    return jnp.concatenate(groups, axis=0)


def attn_kernel(num_tiles, inv_sqrt, u_ref, v_ref, kin_ref, vin_ref, qin_ref, doin_ref, table_in_ref, w_in_ref,
                res_own_ref, res_got_ref, bias_ref,
                full_ref, acc_ref, kt_ref, valt_ref, relt_ref, sc_ref, rot_ref, ds_ref, dw_ref, p_ref,
                qu_ref, qv_ref, qut_ref, qvt_ref, dot_ref, max_ref, sum_ref, gu_ref, gv_ref, row_ref,
                st_rows_ref, st_grad_ref, part_ref, away_ref, raw_ref, table_ref, w_ref, wide_ref,
                local_sems, own_send, own_recv, cross_send, cross_recv, fwd_send, fwd_recv,
                part_send, part_recv, rows_send, grad_send, res_sems):
    step = pl.program_id(0)
    last = pl.num_programs(0) - 1
    dev = lax.axis_index('cp')
    chip, core = lax.div(dev, 2), lax.rem(dev, 2)
    core_peer, chip_peer = dev + 1 - 2 * core, dev + 2 - 4 * chip
    half_steps = num_tiles // 4

    def pair_at(idx):
        first = jnp.where(idx < half_steps, idx, 3 * half_steps - 1 - idx)
        second = jnp.where(idx < half_steps - 1, idx + half_steps, 2 * half_steps - 2 - idx)
        second = jnp.where(idx == last, last, second)
        return jnp.where(chip == 0, first, second)

    def block_at(idx):
        odd = lax.rem(pair_at(idx), 2)
        return 2 * pair_at(idx) + odd + core - 2 * odd * core

    blk = block_at(step)
    scale = inv_sqrt * LOG2E
    block_len = away_ref.shape[1]
    block_tiles = block_len // TILE
    k_ref, val_ref, rel_ref = full_ref.at[0], full_ref.at[1], full_ref.at[2]
    q_ref, do_ref = full_ref.at[3], full_ref.at[4]
    dk_ref, dv_ref, drel_ref = acc_ref.at[0], acc_ref.at[1], acc_ref.at[2]

    def cols(tile):
        return pl.ds(pl.multiple_of(tile * TILE, TILE), TILE)

    def place(arr, block):
        at = 3 - block if arr == 2 else block
        return full_ref.at[arr, pl.ds(pl.multiple_of(at * block_len, block_len), block_len)]

    def to_device(src, dst, send_sem, recv_sem, peer):
        return pltpu.make_async_remote_copy(
            src_ref=src, dst_ref=dst, send_sem=send_sem, recv_sem=recv_sem,
            device_id={'cp': peer}, device_id_type=pl.DeviceIdType.MESH)

    def own_copy(arr):
        return to_device(place(arr, dev), place(arr, dev), own_send.at[arr], own_recv.at[arr], core_peer)

    def cross_copy(arr):
        return to_device(away_ref.at[arr], place(arr, dev), cross_send.at[arr], cross_recv.at[arr], chip_peer)

    def fwd_copy(arr):
        return to_device(place(arr, chip_peer), place(arr, chip_peer), fwd_send.at[arr], fwd_recv.at[arr], core_peer)

    def transpose_half(arr, which):
        dst = (kt_ref, valt_ref, relt_ref)[arr]
        first = (1 - which if arr == 2 else which) * (num_tiles // 2)

        def body(idx, _):
            dst[:, cols(first + idx)] = full_ref[arr, cols(first + idx), :].T
            return 0
        lax.fori_loop(0, num_tiles // 2, body, 0)

    def arrive(arrays):
        for arr in arrays:
            cross_copy(arr).wait_recv()
            fwd_copy(arr).start()
        for arr in arrays:
            fwd_copy(arr).wait_recv()
            if arr < 3:
                transpose_half(arr, 1 - chip)

    def part_copy(slot, pair_idx, arr):
        tile = 2 * pair_idx + 1 - core
        at = num_tiles - 1 - tile if arr == 2 else tile
        return to_device(acc_ref.at[arr, :, cols(at)], part_ref.at[slot, arr],
                         part_send.at[slot, arr], part_recv.at[slot, arr], core_peer)

    def start_parts(slot, arrays):
        for arr in arrays:
            part_copy(slot, pair_of(slot), arr).start()

    def deliver(tile, stage, part, send_sem, start):
        owner = lax.div(tile, block_tiles)
        local = tile - owner * block_tiles
        where = PARTS[part]

        @pl.when(owner == dev)
        def _():
            if start:
                pltpu.make_async_copy(stage, res_own_ref.at[local, where], res_sems.at[0, part, local]).start()

        @pl.when(owner == core_peer)
        def _():
            copy = to_device(stage, res_own_ref.at[local, where], send_sem, res_sems.at[0, part, local], owner)
            copy.start() if start else copy.wait_send()

        @pl.when(lax.div(owner, 2) != chip)
        def _():
            copy = to_device(stage, res_got_ref.at[local, where], send_sem, res_sems.at[1, part, local], owner)
            copy.start() if start else copy.wait_send()

    def finish_keys(slot):
        tile = 2 * pair_of(slot) + core
        for arr in range(2):
            part_copy(slot, pair_of(slot), arr).wait_recv()
        d_key = (acc_ref[0, :, cols(tile)] + part_ref[slot, 0]) * inv_sqrt
        st_grad_ref[slot, 0] = d_key.astype(BF16).T
        d_val = acc_ref[1, :, cols(tile)] + part_ref[slot, 1]
        st_grad_ref[slot, 1] = d_val.astype(BF16).T
        deliver(tile, st_grad_ref.at[slot, pl.ds(0, 2)], 1, grad_send.at[slot, 0], True)

    def finish_offsets(slot):
        tile = 2 * pair_of(slot) + core
        part_copy(slot, pair_of(slot), 2).wait_recv()
        d_off = ((acc_ref[2, :, cols(num_tiles - 1 - tile)] + part_ref[slot, 2]) * inv_sqrt).astype(BF16)
        flip_rows = exchange_matrix()
        for chunk in range(NSUB):
            back = lax.dot_general(flip_rows, d_off[:, sub(chunk)], (((1,), (1,)), ((), ())), preferred_element_type=F32)
            st_grad_ref[slot, 2, sub(NSUB - 1 - chunk)] = back.astype(BF16)
        deliver(tile, st_grad_ref.at[slot, pl.ds(2, 1)], 2, grad_send.at[slot, 1], True)

    def pair_of(idx):
        return jnp.where(idx < half_steps, (2 - chip) * half_steps - 1 - idx, idx - half_steps + half_steps * chip)

    def put_heads(arr, start, size, first, second):
        at = 3 - dev if arr == 2 else dev
        own_at = pl.ds(pl.multiple_of(at * block_len + start, SUB), size)
        away_at = pl.ds(pl.multiple_of(start, SUB), size)
        full_ref[arr, own_at] = jnp.where(chip == 0, first, second)
        away_ref[arr, away_at] = jnp.where(chip == 0, second, first)

    def pack_seq(arr, src):
        def body(idx, _):
            heads = jnp.swapaxes(raw_ref[src, cols(idx)], 0, 1)
            put_heads(arr, idx * TILE, TILE, heads[0], heads[1])
            return 0
        lax.fori_loop(0, block_tiles, body, 0)

    def pack_rel():
        weights = jnp.swapaxes(w_ref[...], 0, 1)
        wide_ref[:, :SUB] = weights[0]
        wide_ref[:, SUB:] = weights[1]

        def body(idx, _):
            rel = dot(table_ref[cols(idx), :], wide_ref[...]).astype(BF16)
            flip_rows = exchange_matrix()
            for chunk in range(NSUB):
                back = dot(flip_rows, rel[sub(NSUB - 1 - chunk)]).astype(BF16)
                put_heads(2, (block_tiles - 1 - idx) * TILE + chunk * SUB, SUB, back[:, :SUB], back[:, SUB:])
            return 0
        lax.fori_loop(0, block_tiles, body, 0)

    @pl.when(step == 0)
    def _():
        barrier = pltpu.get_barrier_semaphore()
        for peer in (core_peer, chip_peer, 3 - dev):
            pl.semaphore_signal(barrier, inc=1, device_id={'cp': peer}, device_id_type=pl.DeviceIdType.MESH)
        loads = [pltpu.make_async_copy(src, dst, local_sems.at[idx]) for idx, (src, dst) in enumerate((
            (kin_ref, raw_ref.at[0]), (w_in_ref, w_ref), (table_in_ref, table_ref),
            (vin_ref, raw_ref.at[1]), (qin_ref, raw_ref.at[2]), (doin_ref, raw_ref.at[3])))]
        for load in loads:
            load.start()

        def clear(tile, _):
            acc_ref[:, :, cols(tile)] = jnp.zeros((3, SUB, TILE), F32)
            return 0

        def ship(arr):
            cross_copy(arr).start()
            own_copy(arr).start()

        loads[0].wait()
        pack_seq(0, 0)
        pl.semaphore_wait(barrier, 3)
        ship(0)
        loads[1].wait()
        loads[2].wait()
        pack_rel()
        ship(2)
        for idx, arr in enumerate((1, 3, 4)):
            loads[3 + idx].wait()
            pack_seq(arr, idx + 1)
            ship(arr)
        lax.fori_loop(0, num_tiles, clear, 0)
        bias_ref[...] = jnp.zeros_like(bias_ref)
        for arr in (0, 2, 1, 3, 4):
            own_copy(arr).wait_recv()
            if arr < 3:
                transpose_half(arr, chip)

    @pl.when(step == half_steps * (1 - chip))
    def _():
        arrive((0, 2))

    @pl.when(step == half_steps - chip)
    def _():
        arrive((3, 4))

    rows_at = cols(blk)
    d_out = do_ref[rows_at, :]
    q_wide = q_ref[rows_at, :].astype(F32)
    q_u = (q_wide + u_ref[...]).astype(BF16)
    q_v = (q_wide + v_ref[...]).astype(BF16)
    qu_ref[...] = q_u
    qv_ref[...] = q_v
    qut_ref[...] = q_u.T
    qvt_ref[...] = q_v.T
    dot_ref[...] = d_out.T
    max_ref[...] = jnp.full_like(max_ref, -jnp.inf)
    sum_ref[...] = jnp.zeros_like(sum_ref)
    gu_ref[...] = jnp.zeros_like(gu_ref)
    gv_ref[...] = jnp.zeros_like(gv_ref)
    lane = lax.broadcasted_iota(jnp.int32, (SUB, SUB), 1)
    row = lax.broadcasted_iota(jnp.int32, (SUB, SUB), 0)
    upper = lane > row
    flip = 7 - lax.broadcasted_iota(jnp.int32, (8, SUB), 0)
    lower = lane + row < SUB - 1
    first_rel = num_tiles - 1 - blk

    def rotate_rel(tile, slot):
        for half in range(2):
            start = pl.multiple_of(tile * TILE + half * 256, 256)
            for a in range(NSUB):
                if a % MROWS == 0:
                    by_offset = dot(qv_ref[a * SUB:(a + MROWS) * SUB, :], relt_ref[:, pl.ds(start, 256)])
                for c in range(2):
                    part = by_offset[sub(a % MROWS), sub(c)]
                    rot_ref[slot, sub(a), sub(half * 2 + c)] = pltpu.roll(part, 1, 1, stride=1, stride_axis=0)

    rotate_rel(first_rel, 0)

    @pl.when(blk > 0)
    def _():
        rotate_rel(first_rel + 1, 1)

    def score_tile(tile, diag):
        left = lax.rem(tile, 3)
        right = lax.rem(tile + 1, 3)
        for half in range(2):
            start = pl.multiple_of(tile * TILE + half * 256, 256)
            for a in range(NSUB):
                if a % MROWS == 0:
                    content = dot(qu_ref[a * SUB:(a + MROWS) * SUB, :], kt_ref[:, pl.ds(start, 256)])
                run_max = max_ref[sub(a), :]
                for c2 in range(2):
                    c = half * 2 + c2
                    hi, lo = c - a + NSUB, c - a + NSUB - 1
                    if diag and c > a:
                        score = jnp.full((SUB, SUB), -jnp.inf, F32)
                    else:
                        low_part = rot_ref[left if lo < NSUB else right, sub(a), sub(lo % NSUB)]
                        if diag and c == a:
                            score = jnp.where(upper, -jnp.inf, (content[sub(a % MROWS), sub(c2)] + low_part) * scale)
                        else:
                            high_part = rot_ref[left if hi < NSUB else right, sub(a), sub(hi % NSUB)]
                            score = (content[sub(a % MROWS), sub(c2)] + jnp.where(upper, high_part, low_part)) * scale
                    run_max = jnp.maximum(run_max, score)
                    sc_ref[sub(a), pl.ds(pl.multiple_of(tile * TILE + c * SUB, SUB), SUB)] = score
                max_ref[sub(a), :] = run_max
        if not diag:
            rotate_rel(jnp.minimum(first_rel + tile + 2, num_tiles - 1), lax.rem(tile + 2, 3))

    def score_body(tile, _):
        score_tile(tile, False)
        return 0

    lax.fori_loop(0, blk, score_body, 0)
    score_tile(blk, True)
    max_ref[...] = jnp.broadcast_to(jnp.max(max_ref[...], axis=1, keepdims=True), (TILE, SUB))

    @pl.when(step == half_steps * (1 - chip))
    def _():
        arrive((1,))

    def prob_body(tile, _):
        for a in range(NSUB):
            run_sum = sum_ref[sub(a), :]
            row_max = max_ref[sub(a), :]
            for c in range(NSUB):
                where = pl.ds(pl.multiple_of(tile * TILE + c * SUB, SUB), SUB)
                prob = jnp.exp2(sc_ref[sub(a), where] - row_max)
                p_ref[sub(a), sub(c)] = prob.astype(BF16)
                run_sum = run_sum + prob
            sum_ref[sub(a), :] = run_sum
        gu_ref[...] += dot(p_ref[...], val_ref[cols(tile), :])
        return 0

    lax.fori_loop(0, blk + 1, prob_body, 0)
    total = jnp.sum(sum_ref[...], axis=1, keepdims=True)
    inv_sum = 1.0 / total
    out = gu_ref[...] * inv_sum
    st_rows_ref[step, 0] = out.astype(BF16)
    delta = jnp.sum(out * do_ref[rows_at, :].astype(F32), axis=1, keepdims=True)
    row_ref[...] = jnp.broadcast_to(delta, (TILE, SUB))
    sum_ref[...] = max_ref[...] + jnp.log2(total)
    gu_ref[...] = jnp.zeros_like(gu_ref)
    ds_ref[1, :, :] = jnp.zeros((TILE, TILE), F32)

    def grad_body(tile, _):
        now = lax.rem(tile, 2)
        old = 1 - now
        for half in range(2):
            start = pl.multiple_of(tile * TILE + half * 256, 256)
            for a in range(NSUB):
                if a % MROWS == 0:
                    do_rows = pl.ds(pl.multiple_of(blk * TILE + a * SUB, SUB), MROWS * SUB)
                    d_prob = dot(do_ref[do_rows, :], valt_ref[:, pl.ds(start, 256)])
                log_norm = sum_ref[sub(a), :]
                shift = row_ref[sub(a), :]
                for c2 in range(2):
                    c = half * 2 + c2
                    prob = jnp.exp2(sc_ref[sub(a), pl.ds(pl.multiple_of(tile * TILE + c * SUB, SUB), SUB)] - log_norm)
                    p_ref[sub(a), sub(c)] = prob.astype(BF16)
                    d_score = prob * (d_prob[sub(a % MROWS), sub(c2)] - shift)
                    dw_ref[sub(a), sub(c)] = d_score.astype(BF16)
                    ds_ref[now, sub(a), sub(c)] = roll_left(d_score, flip)
            win = pl.ds(start, 256)
            dv_ref[:, win] += dot(dot_ref[...], p_ref[:, half * 256:half * 256 + 256])
            dk_ref[:, win] += dot(qut_ref[...], dw_ref[:, half * 256:half * 256 + 256])
        gu_ref[...] += dot(dw_ref[...], k_ref[cols(tile), :])
        for a in range(NSUB):
            for y in range(NSUB):
                c_lo = y + a - NSUB
                c_hi = c_lo + 1
                lo_part = ds_ref[now if c_lo >= 0 else old, sub(a), sub(c_lo % NSUB)]
                hi_part = ds_ref[now if c_hi >= 0 else old, sub(a), sub(c_hi % NSUB)]
                p_ref[sub(a), sub(y)] = jnp.where(lower, lo_part, hi_part).astype(BF16)
        rel_tile = first_rel + tile
        gv_ref[...] += dot(p_ref[...], rel_ref[cols(rel_tile), :])
        for half in range(2):
            start = pl.multiple_of(rel_tile * TILE + half * 256, 256)
            drel_ref[:, pl.ds(start, 256)] += dot(qvt_ref[...], p_ref[:, half * 256:half * 256 + 256])

        @pl.when((step == last) & (chip == 1) & (lax.rem(tile, 2) == 1) & (tile < 2 * half_steps + 2))
        def _():
            now_pair = lax.div(tile, 2)

            @pl.when(now_pair < half_steps)
            def _():
                start_parts(half_steps - 1 - now_pair, (0, 1))

            @pl.when(now_pair > 0)
            def _():
                finish_keys(half_steps - now_pair)
        return 0

    @pl.when((step > half_steps) & (chip == 0))
    def _():
        finish_offsets(step - half_steps - 1)
        finish_keys(step - half_steps - 1)

    lax.fori_loop(0, blk + 1, grad_body, 0)
    grad_u = gu_ref[...] * inv_sqrt
    grad_v = gv_ref[...] * inv_sqrt
    st_rows_ref[step, 1] = (grad_u + grad_v).astype(BF16)
    bias_ref[0:1, :] += jnp.sum(grad_u, axis=0, keepdims=True)
    bias_ref[1:2, :] += jnp.sum(grad_v, axis=0, keepdims=True)
    deliver(blk, st_rows_ref.at[step], 0, rows_send.at[step], True)

    @pl.when((step >= half_steps) & (chip == 0))
    def _():
        start_parts(step - half_steps, (2, 0, 1))

    @pl.when(step == last)
    def _():
        def start_far(idx, _):
            start_parts(idx, (2,))
            return 0

        def start_near(idx, _):
            start_parts(idx, (0, 1, 2))
            return 0

        def finish_far(idx, _):
            finish_offsets(idx)
            return 0

        def finish_near(idx, _):
            finish_offsets(idx)
            finish_keys(idx)
            return 0

        def drain(idx, _):
            for arr in range(3):
                part_copy(idx, pair_of(idx), arr).wait_send()
            tile = 2 * pair_of(idx) + core
            deliver(tile, st_grad_ref.at[idx, pl.ds(0, 2)], 1, grad_send.at[idx, 0], False)
            deliver(tile, st_grad_ref.at[idx, pl.ds(2, 1)], 2, grad_send.at[idx, 1], False)
            deliver(block_at(idx), st_rows_ref.at[idx], 0, rows_send.at[idx], False)
            return 0

        @pl.when(chip == 1)
        def _():
            lax.fori_loop(0, half_steps, start_far, 0)
        lax.fori_loop(half_steps, 2 * half_steps, start_near, 0)

        @pl.when(chip == 1)
        def _():
            lax.fori_loop(0, half_steps, finish_far, 0)

        @pl.when(chip == 0)
        def _():
            finish_near(half_steps - 1, 0)
        lax.fori_loop(half_steps, 2 * half_steps, finish_near, 0)
        lax.fori_loop(0, 2 * half_steps, drain, 0)
        for arr in range(5):
            own_copy(arr).wait_send()
            cross_copy(arr).wait_send()
            fwd_copy(arr).wait_send()
        for which, res in enumerate((res_own_ref, res_got_ref)):
            for local in range(block_tiles):
                for part, where in enumerate(PARTS):
                    dst = res.at[local, where]
                    pltpu.make_async_copy(dst, dst, res_sems.at[which, part, local]).wait()


def run_attn(u_bias, v_bias, k, v, q, d_out, rel_table, w_rel):
    block_len, _, head_dim = k.shape
    seq_len = 4 * block_len
    num_tiles = seq_len // TILE
    steps = num_tiles // 2
    block_tiles = block_len // TILE
    vec = pl.BlockSpec(memory_space=pltpu.VMEM)
    hbm = pl.BlockSpec(memory_space=pl.ANY)
    result = jax.ShapeDtypeStruct((block_tiles, 5, TILE, head_dim), BF16)
    dma = pltpu.SemaphoreType.DMA
    return pl.pallas_call(
        functools.partial(attn_kernel, num_tiles, head_dim ** -0.5),
        grid=(steps,),
        in_specs=[vec, vec] + [hbm] * 6,
        out_specs=[hbm, hbm, vec],
        scratch_shapes=[
            pltpu.VMEM((5, seq_len, head_dim), BF16),
            pltpu.VMEM((3, head_dim, seq_len), F32),
            pltpu.VMEM((head_dim, seq_len), BF16),
            pltpu.VMEM((head_dim, seq_len), BF16),
            pltpu.VMEM((head_dim, seq_len), BF16),
            pltpu.VMEM((TILE, seq_len), F32),
            pltpu.VMEM((3, TILE, TILE), F32),
            pltpu.VMEM((2, TILE, TILE), F32),
            pltpu.VMEM((TILE, TILE), BF16),
            pltpu.VMEM((TILE, TILE), BF16),
            pltpu.VMEM((TILE, head_dim), BF16),
            pltpu.VMEM((TILE, head_dim), BF16),
            pltpu.VMEM((head_dim, TILE), BF16),
            pltpu.VMEM((head_dim, TILE), BF16),
            pltpu.VMEM((head_dim, TILE), BF16),
            pltpu.VMEM((TILE, SUB), F32),
            pltpu.VMEM((TILE, SUB), F32),
            pltpu.VMEM((TILE, head_dim), F32),
            pltpu.VMEM((TILE, head_dim), F32),
            pltpu.VMEM((TILE, SUB), F32),
            pltpu.VMEM((steps, 2, TILE, head_dim), BF16),
            pltpu.VMEM((steps, 3, TILE, head_dim), BF16),
            pltpu.VMEM((steps, 3, head_dim, TILE), F32),
            pltpu.VMEM((5, block_len, head_dim), BF16),
            pltpu.VMEM((4,) + k.shape, BF16),
            pltpu.VMEM(rel_table.shape, BF16),
            pltpu.VMEM(w_rel.shape, BF16),
            pltpu.VMEM((w_rel.shape[0], 2 * head_dim), BF16),
            dma((6,)), dma((5,)), dma((5,)), dma((5,)), dma((5,)), dma((5,)), dma((5,)),
            dma((steps, 3)), dma((steps, 3)), dma((steps,)), dma((steps, 2)), dma((2, 3, block_tiles)),
        ],
        out_shape=[result, result, jax.ShapeDtypeStruct((2, head_dim), F32)],
        compiler_params=pltpu.CompilerParams(
            dimension_semantics=("arbitrary",), vmem_limit_bytes=67043328, collective_id=0, has_side_effects=True),
        name="attn_rows",
    )(u_bias, v_bias, k, v, q, d_out, rel_table, w_rel)


def exchange_matrix():
    row = lax.broadcasted_iota(jnp.int32, (SUB, SUB), 0)
    col = lax.broadcasted_iota(jnp.int32, (SUB, SUB), 1)
    return jnp.where(row + col == SUB - 1, 1.0, 0.0).astype(BF16)


def finish_kernel(own_ref, got_ref, table_ref, bias_ref, o_ref, dq_ref, dk_ref, dv_ref, dw_ref, du_ref, dvb_ref,
                  rel_ref, part_ref, core_ref, sum_ref, chip_ref, final_ref, send_sems, recv_sems):
    dev = lax.axis_index('cp')
    chip, core = lax.div(dev, 2), lax.rem(dev, 2)
    core_peer, chip_peer = dev + 1 - 2 * core, dev + 2 - 4 * chip
    barrier = pltpu.get_barrier_semaphore()
    for peer in (core_peer, chip_peer):
        pl.semaphore_signal(barrier, inc=1, device_id={'cp': peer}, device_id_type=pl.DeviceIdType.MESH)
    tiles = own_ref.shape[0]
    half = table_ref.shape[1] // 2

    def heads(arr, tile):
        own, got = own_ref[tile, arr], got_ref[tile, arr]
        return jnp.where(chip == 0, own, got), jnp.where(chip == 0, got, own)

    for tile in range(tiles):
        rows = slice(tile * TILE, (tile + 1) * TILE)
        rel_ref[rows, :SUB], rel_ref[rows, SUB:] = heads(4, tile)

    def partial(which):
        for start in range(0, half, 256):
            at = pl.ds(pl.multiple_of(which * half + start, 256), 256)
            part_ref[which, start:start + 256] = lax.dot_general(
                table_ref[:, at], rel_ref[...], (((0,), (0,)), ((), ())), preferred_element_type=F32)
        bias = bias_ref[...]
        zero = jnp.zeros_like(bias)
        both = jnp.concatenate([jnp.where(chip == 0, bias, zero), jnp.where(chip == 0, zero, bias)], axis=1)
        part_ref[which, half:] = jnp.concatenate([both, jnp.zeros((6, both.shape[1]), F32)], axis=0)

    def swap(idx, src, dst, peer):
        copy = pltpu.make_async_remote_copy(
            src_ref=src, dst_ref=dst, send_sem=send_sems.at[idx], recv_sem=recv_sems.at[idx],
            device_id={'cp': peer}, device_id_type=pl.DeviceIdType.MESH)
        copy.start()
        return copy

    partial(1 - core)
    pl.semaphore_wait(barrier, 2)
    first = swap(0, part_ref.at[1 - core], core_ref, core_peer)
    partial(core)
    first.wait()
    sum_ref[...] = part_ref[core] + core_ref[...]
    second = swap(1, sum_ref, chip_ref, chip_peer)
    for tile in range(tiles):
        rows = slice(tile * TILE, (tile + 1) * TILE)
        for arr, dst in enumerate((o_ref, dq_ref, dk_ref, dv_ref)):
            dst[rows] = jnp.stack(heads(arr, tile), axis=1)
    second.wait()
    final_ref[core] = sum_ref[...] + chip_ref[...]
    third = swap(2, final_ref.at[core], final_ref.at[core], core_peer)
    third.wait()
    for which in range(2):
        dw_ref[which * half:(which + 1) * half] = jnp.stack(
            [final_ref[which, :half, :SUB], final_ref[which, :half, SUB:]], axis=1)
    tail = final_ref[0, half:]
    du_ref[...] = jnp.concatenate([tail[0:1, :SUB], tail[0:1, SUB:]], axis=0)
    dvb_ref[...] = jnp.concatenate([tail[1:2, :SUB], tail[1:2, SUB:]], axis=0)


def finish(own, got, rel_table, bias_grad, seq_shape, w_shape):
    half_rows = w_shape[0] // 2 + 8
    wide = 2 * SUB
    vmem = pl.BlockSpec(memory_space=pltpu.VMEM)
    bias = jax.ShapeDtypeStruct((2, SUB), F32)
    seq = jax.ShapeDtypeStruct(seq_shape, BF16)
    return pl.pallas_call(
        finish_kernel,
        in_specs=[vmem] * 4,
        out_specs=[vmem] * 7,
        out_shape=[seq, seq, seq, seq, jax.ShapeDtypeStruct(w_shape, F32), bias, bias],
        scratch_shapes=[
            pltpu.VMEM((rel_table.shape[0], wide), BF16),
            pltpu.VMEM((2, half_rows, wide), F32),
            pltpu.VMEM((half_rows, wide), F32),
            pltpu.VMEM((half_rows, wide), F32),
            pltpu.VMEM((half_rows, wide), F32),
            pltpu.VMEM((2, half_rows, wide), F32),
            pltpu.SemaphoreType.DMA((3,)),
            pltpu.SemaphoreType.DMA((3,)),
        ],
        compiler_params=pltpu.CompilerParams(vmem_limit_bytes=48 * 1024 * 1024, collective_id=1, has_side_effects=True),
        name="finish",
    )(own, got, rel_table, bias_grad)


def solution(mesh):
    seq_spec = P('cp', 'hp', None)
    head_spec = P('hp', None)
    weight_spec = P(None, 'hp', None)

    def local_fn(q, k, v, u_bias, v_bias, rel_table, w_rel, d_out):
        chip = lax.axis_index('cp') // 2
        u_mine = lax.dynamic_slice_in_dim(u_bias, chip, 1)
        v_mine = lax.dynamic_slice_in_dim(v_bias, chip, 1)
        res_own, res_got, bias_grad = run_attn(u_mine, v_mine, k, v, q, d_out, rel_table, w_rel)
        out, dq, dk, dv, d_w_rel, d_u, d_v = finish(res_own, res_got, rel_table, bias_grad, q.shape, w_rel.shape)
        return out, dq, dk, dv, d_u, d_v, d_w_rel

    return jax.shard_map(
        local_fn,
        mesh=mesh,
        in_specs=(seq_spec, seq_spec, seq_spec, head_spec, head_spec, P('cp', None), weight_spec, seq_spec),
        out_specs=(seq_spec, seq_spec, seq_spec, seq_spec, head_spec, head_spec, weight_spec),
        check_vma=False,
    )
```

```python
import functools

import jax
import jax.numpy as jnp
from jax import lax
from jax.experimental import pallas as pl
from jax.experimental.pallas import tpu as pltpu
from jax.sharding import PartitionSpec as P

TILE = 512
SUB = 128
NSUB = TILE // SUB
MROWS = 2
PARTS = (pl.ds(0, 2), pl.ds(2, 2), pl.ds(4, 1))
LOG2E = 1.4426950408889634
F32 = jnp.float32
BF16 = jnp.bfloat16


def dot(lhs, rhs):
    return jnp.dot(lhs, rhs, preferred_element_type=F32)


def sub(idx):
    return slice(idx * SUB, (idx + 1) * SUB)


def roll_left(part, flip):
    groups = []
    for start in range(0, SUB, 8):
        rows = jnp.take_along_axis(part[start:start + 8], flip, axis=0)
        rows = pltpu.roll(rows, (SUB - 8 - start) % SUB, 1, stride=1, stride_axis=0)
        groups.append(jnp.take_along_axis(rows, flip, axis=0))
    return jnp.concatenate(groups, axis=0)


def attn_kernel(num_tiles, inv_sqrt, u_ref, v_ref, kin_ref, vin_ref, qin_ref, doin_ref, table_in_ref, w_in_ref,
                res_own_ref, res_got_ref, bias_ref,
                full_ref, acc_ref, kt_ref, valt_ref, relt_ref, sc_ref, rot_ref, ds_ref, dw_ref, p_ref,
                qu_ref, qv_ref, qut_ref, qvt_ref, dot_ref, max_ref, sum_ref, gu_ref, gv_ref, row_ref,
                st_rows_ref, st_grad_ref, part_ref, away_ref, raw_ref, table_ref, w_ref, wide_ref,
                local_sems, own_send, own_recv, cross_send, cross_recv, fwd_send, fwd_recv,
                part_send, part_recv, rows_send, grad_send, res_sems):
    step = pl.program_id(0)
    last = pl.num_programs(0) - 1
    dev = lax.axis_index('cp')
    chip, core = lax.div(dev, 2), lax.rem(dev, 2)
    core_peer, chip_peer = dev + 1 - 2 * core, dev + 2 - 4 * chip
    half_steps = num_tiles // 4

    def pair_at(idx):
        first = jnp.where(idx < half_steps, idx, 3 * half_steps - 1 - idx)
        second = jnp.where(idx < half_steps - 1, idx + half_steps, 2 * half_steps - 2 - idx)
        second = jnp.where(idx == last, last, second)
        return jnp.where(chip == 0, first, second)

    def block_at(idx):
        odd = lax.rem(pair_at(idx), 2)
        return 2 * pair_at(idx) + odd + core - 2 * odd * core

    blk = block_at(step)
    scale = inv_sqrt * LOG2E
    block_len = away_ref.shape[1]
    block_tiles = block_len // TILE
    k_ref, val_ref, rel_ref = full_ref.at[0], full_ref.at[1], full_ref.at[2]
    q_ref, do_ref = full_ref.at[3], full_ref.at[4]
    dk_ref, dv_ref, drel_ref = acc_ref.at[0], acc_ref.at[1], acc_ref.at[2]

    def cols(tile):
        return pl.ds(pl.multiple_of(tile * TILE, TILE), TILE)

    def place(arr, block):
        at = 3 - block if arr == 2 else block
        return full_ref.at[arr, pl.ds(pl.multiple_of(at * block_len, block_len), block_len)]

    def to_device(src, dst, send_sem, recv_sem, peer):
        return pltpu.make_async_remote_copy(
            src_ref=src, dst_ref=dst, send_sem=send_sem, recv_sem=recv_sem,
            device_id={'cp': peer}, device_id_type=pl.DeviceIdType.MESH)

    def own_copy(arr):
        return to_device(place(arr, dev), place(arr, dev), own_send.at[arr], own_recv.at[arr], core_peer)

    def cross_copy(arr):
        return to_device(away_ref.at[arr], place(arr, dev), cross_send.at[arr], cross_recv.at[arr], chip_peer)

    def fwd_copy(arr):
        return to_device(place(arr, chip_peer), place(arr, chip_peer), fwd_send.at[arr], fwd_recv.at[arr], core_peer)

    def transpose_half(arr, which):
        dst = (kt_ref, valt_ref, relt_ref)[arr]
        first = (1 - which if arr == 2 else which) * (num_tiles // 2)

        def body(idx, _):
            dst[:, cols(first + idx)] = full_ref[arr, cols(first + idx), :].T
            return 0
        lax.fori_loop(0, num_tiles // 2, body, 0)

    def arrive(arrays):
        for arr in arrays:
            cross_copy(arr).wait_recv()
            fwd_copy(arr).start()
        for arr in arrays:
            fwd_copy(arr).wait_recv()
            if arr < 3:
                transpose_half(arr, 1 - chip)

    def part_copy(slot, arr):
        tile = 2 * slot + 1 - core
        at = num_tiles - 1 - tile if arr == 2 else tile
        return to_device(acc_ref.at[arr, :, cols(at)], part_ref.at[slot, arr],
                         part_send.at[slot, arr], part_recv.at[slot, arr], core_peer)

    def start_parts(slot, arrays):
        for arr in arrays:
            part_copy(slot, arr).start()

    def deliver(tile, stage, part, send_sem, start):
        owner = lax.div(tile, block_tiles)
        local = tile - owner * block_tiles
        where = PARTS[part]

        @pl.when(owner == dev)
        def _():
            if start:
                pltpu.make_async_copy(stage, res_own_ref.at[local, where], res_sems.at[0, part, local]).start()

        @pl.when(owner == core_peer)
        def _():
            copy = to_device(stage, res_own_ref.at[local, where], send_sem, res_sems.at[0, part, local], owner)
            copy.start() if start else copy.wait_send()

        @pl.when(lax.div(owner, 2) != chip)
        def _():
            copy = to_device(stage, res_got_ref.at[local, where], send_sem, res_sems.at[1, part, local], owner)
            copy.start() if start else copy.wait_send()

    def finish_keys(slot):
        tile = 2 * slot + core
        for arr in range(2):
            part_copy(slot, arr).wait_recv()
        d_key = (acc_ref[0, :, cols(tile)] + part_ref[slot, 0]) * inv_sqrt
        st_grad_ref[slot, 0] = d_key.astype(BF16).T
        d_val = acc_ref[1, :, cols(tile)] + part_ref[slot, 1]
        st_grad_ref[slot, 1] = d_val.astype(BF16).T
        deliver(tile, st_grad_ref.at[slot, pl.ds(0, 2)], 1, grad_send.at[slot, 0], True)

    def finish_offsets(slot):
        tile = 2 * slot + core
        part_copy(slot, 2).wait_recv()
        d_off = ((acc_ref[2, :, cols(num_tiles - 1 - tile)] + part_ref[slot, 2]) * inv_sqrt).astype(BF16)
        flip_rows = exchange_matrix()
        for chunk in range(NSUB):
            back = lax.dot_general(flip_rows, d_off[:, sub(chunk)], (((1,), (1,)), ((), ())), preferred_element_type=F32)
            st_grad_ref[slot, 2, sub(NSUB - 1 - chunk)] = back.astype(BF16)
        deliver(tile, st_grad_ref.at[slot, pl.ds(2, 1)], 2, grad_send.at[slot, 1], True)

    top_tile = 2 * pair_at(last) + 1
    top_pair = pair_at(last)

    def put_heads(arr, start, size, first, second):
        at = 3 - dev if arr == 2 else dev
        own_at = pl.ds(pl.multiple_of(at * block_len + start, SUB), size)
        away_at = pl.ds(pl.multiple_of(start, SUB), size)
        full_ref[arr, own_at] = jnp.where(chip == 0, first, second)
        away_ref[arr, away_at] = jnp.where(chip == 0, second, first)

    def pack_seq(arr, src):
        def body(idx, _):
            heads = jnp.swapaxes(raw_ref[src, cols(idx)], 0, 1)
            put_heads(arr, idx * TILE, TILE, heads[0], heads[1])
            return 0
        lax.fori_loop(0, block_tiles, body, 0)

    def pack_rel():
        weights = jnp.swapaxes(w_ref[...], 0, 1)
        wide_ref[:, :SUB] = weights[0]
        wide_ref[:, SUB:] = weights[1]

        def body(idx, _):
            rel = dot(table_ref[cols(idx), :], wide_ref[...]).astype(BF16)
            flip_rows = exchange_matrix()
            for chunk in range(NSUB):
                back = dot(flip_rows, rel[sub(NSUB - 1 - chunk)]).astype(BF16)
                put_heads(2, (block_tiles - 1 - idx) * TILE + chunk * SUB, SUB, back[:, :SUB], back[:, SUB:])
            return 0
        lax.fori_loop(0, block_tiles, body, 0)

    @pl.when(step == 0)
    def _():
        barrier = pltpu.get_barrier_semaphore()
        for peer in (core_peer, chip_peer, 3 - dev):
            pl.semaphore_signal(barrier, inc=1, device_id={'cp': peer}, device_id_type=pl.DeviceIdType.MESH)
        loads = [pltpu.make_async_copy(src, dst, local_sems.at[idx]) for idx, (src, dst) in enumerate((
            (kin_ref, raw_ref.at[0]), (w_in_ref, w_ref), (table_in_ref, table_ref),
            (vin_ref, raw_ref.at[1]), (qin_ref, raw_ref.at[2]), (doin_ref, raw_ref.at[3])))]
        for load in loads:
            load.start()

        def clear(tile, _):
            acc_ref[:, :, cols(tile)] = jnp.zeros((3, SUB, TILE), F32)
            return 0

        def ship(arr):
            cross_copy(arr).start()
            own_copy(arr).start()

        loads[0].wait()
        pack_seq(0, 0)
        pl.semaphore_wait(barrier, 3)
        ship(0)
        loads[1].wait()
        loads[2].wait()
        pack_rel()
        ship(2)
        for idx, arr in enumerate((1, 3, 4)):
            loads[3 + idx].wait()
            pack_seq(arr, idx + 1)
            ship(arr)
        lax.fori_loop(0, num_tiles, clear, 0)
        bias_ref[...] = jnp.zeros_like(bias_ref)
        for arr in (0, 2, 1, 3, 4):
            own_copy(arr).wait_recv()
            if arr < 3:
                transpose_half(arr, chip)

    @pl.when(step == half_steps * (1 - chip))
    def _():
        arrive((0, 2))

    @pl.when(step == half_steps - chip)
    def _():
        arrive((3, 4))

    rows_at = cols(blk)
    d_out = do_ref[rows_at, :]
    q_wide = q_ref[rows_at, :].astype(F32)
    q_u = (q_wide + u_ref[pl.ds(chip, 1), :]).astype(BF16)
    q_v = (q_wide + v_ref[pl.ds(chip, 1), :]).astype(BF16)
    qu_ref[...] = q_u
    qv_ref[...] = q_v
    qut_ref[...] = q_u.T
    qvt_ref[...] = q_v.T
    dot_ref[...] = d_out.T
    max_ref[...] = jnp.full_like(max_ref, -jnp.inf)
    sum_ref[...] = jnp.zeros_like(sum_ref)
    gu_ref[...] = jnp.zeros_like(gu_ref)
    gv_ref[...] = jnp.zeros_like(gv_ref)
    lane = lax.broadcasted_iota(jnp.int32, (SUB, SUB), 1)
    row = lax.broadcasted_iota(jnp.int32, (SUB, SUB), 0)
    upper = lane > row
    flip = 7 - lax.broadcasted_iota(jnp.int32, (8, SUB), 0)
    lower = lane + row < SUB - 1
    first_rel = num_tiles - 1 - blk

    def rotate_rel(tile, slot):
        for half in range(2):
            start = pl.multiple_of(tile * TILE + half * 256, 256)
            for a in range(NSUB):
                if a % MROWS == 0:
                    by_offset = dot(qv_ref[a * SUB:(a + MROWS) * SUB, :], relt_ref[:, pl.ds(start, 256)])
                for c in range(2):
                    part = by_offset[sub(a % MROWS), sub(c)]
                    rot_ref[slot, sub(a), sub(half * 2 + c)] = pltpu.roll(part, 1, 1, stride=1, stride_axis=0)

    rotate_rel(first_rel, 0)
    rotate_rel(jnp.minimum(first_rel + 1, num_tiles - 1), 1)

    def score_tile(tile, diag):
        left = lax.rem(tile, 3)
        right = lax.rem(tile + 1, 3)
        for half in range(2):
            start = pl.multiple_of(tile * TILE + half * 256, 256)
            for a in range(NSUB):
                if a % MROWS == 0:
                    content = dot(qu_ref[a * SUB:(a + MROWS) * SUB, :], kt_ref[:, pl.ds(start, 256)])
                run_max = max_ref[sub(a), :]
                for c2 in range(2):
                    c = half * 2 + c2
                    hi, lo = c - a + NSUB, c - a + NSUB - 1
                    if diag and c > a:
                        score = jnp.full((SUB, SUB), -jnp.inf, F32)
                    else:
                        low_part = rot_ref[left if lo < NSUB else right, sub(a), sub(lo % NSUB)]
                        if diag and c == a:
                            score = jnp.where(upper, -jnp.inf, (content[sub(a % MROWS), sub(c2)] + low_part) * scale)
                        else:
                            high_part = rot_ref[left if hi < NSUB else right, sub(a), sub(hi % NSUB)]
                            score = (content[sub(a % MROWS), sub(c2)] + jnp.where(upper, high_part, low_part)) * scale
                    run_max = jnp.maximum(run_max, score)
                    sc_ref[sub(a), pl.ds(pl.multiple_of(tile * TILE + c * SUB, SUB), SUB)] = score
                max_ref[sub(a), :] = run_max
        if not diag:
            rotate_rel(jnp.minimum(first_rel + tile + 2, num_tiles - 1), lax.rem(tile + 2, 3))

    def score_body(tile, _):
        score_tile(tile, False)
        return 0

    lax.fori_loop(0, blk, score_body, 0)
    score_tile(blk, True)
    max_ref[...] = jnp.broadcast_to(jnp.max(max_ref[...], axis=1, keepdims=True), (TILE, SUB))

    @pl.when(step == half_steps * (1 - chip))
    def _():
        arrive((1,))

    def prob_body(tile, _):
        for top in range(0, NSUB, 2):
            rows = slice(top * SUB, (top + 2) * SUB)
            prob_rows = []
            for a in range(top, top + 2):
                run_sum = sum_ref[sub(a), :]
                row_max = max_ref[sub(a), :]
                prob_cols = []
                for c in range(NSUB):
                    where = pl.ds(pl.multiple_of(tile * TILE + c * SUB, SUB), SUB)
                    prob = jnp.exp2(sc_ref[sub(a), where] - row_max)
                    prob_cols.append(prob.astype(BF16))
                    run_sum = run_sum + prob
                sum_ref[sub(a), :] = run_sum
                prob_rows.append(jnp.concatenate(prob_cols, axis=1))
            gu_ref[rows, :] += dot(jnp.concatenate(prob_rows, axis=0), val_ref[cols(tile), :])
        return 0

    lax.fori_loop(0, blk + 1, prob_body, 0)
    total = jnp.sum(sum_ref[...], axis=1, keepdims=True)
    inv_sum = 1.0 / total
    out = gu_ref[...] * inv_sum
    st_rows_ref[step, 0] = out.astype(BF16)
    delta = jnp.sum(out * do_ref[rows_at, :].astype(F32), axis=1, keepdims=True)
    row_ref[...] = jnp.broadcast_to(delta, (TILE, SUB))
    sum_ref[...] = max_ref[...] + jnp.log2(total)
    gu_ref[...] = jnp.zeros_like(gu_ref)
    ds_ref[1, :, :] = jnp.zeros((TILE, TILE), F32)

    def grad_body(tile, _):
        now = lax.rem(tile, 2)
        old = 1 - now
        for half in range(2):
            start = pl.multiple_of(tile * TILE + half * 256, 256)
            win = pl.ds(start, 256)
            d_val = d_key = None
            for top in range(0, NSUB, 2):
                rows = slice(top * SUB, (top + 2) * SUB)
                do_rows = pl.ds(pl.multiple_of(blk * TILE + top * SUB, SUB), 2 * SUB)
                d_prob = dot(do_ref[do_rows, :], valt_ref[:, win])
                prob_rows, score_rows = [], []
                for a in range(top, top + 2):
                    log_norm = sum_ref[sub(a), :]
                    shift = row_ref[sub(a), :]
                    prob_cols, score_cols = [], []
                    for c2 in range(2):
                        c = half * 2 + c2
                        prob = jnp.exp2(sc_ref[sub(a), pl.ds(pl.multiple_of(tile * TILE + c * SUB, SUB), SUB)] - log_norm)
                        d_score = prob * (d_prob[sub(a - top), sub(c2)] - shift)
                        ds_ref[now, sub(a), sub(c)] = roll_left(d_score, flip)
                        prob_cols.append(prob.astype(BF16))
                        score_cols.append(d_score.astype(BF16))
                    prob_rows.append(jnp.concatenate(prob_cols, axis=1))
                    score_rows.append(jnp.concatenate(score_cols, axis=1))
                probs = jnp.concatenate(prob_rows, axis=0)
                scores = jnp.concatenate(score_rows, axis=0)
                more_val, more_key = dot(dot_ref[:, rows], probs), dot(qut_ref[:, rows], scores)
                d_val = more_val if d_val is None else d_val + more_val
                d_key = more_key if d_key is None else d_key + more_key
                gu_ref[rows, :] += dot(scores, k_ref[win, :])
            dv_ref[:, win] += d_val
            dk_ref[:, win] += d_key
        rel_tile = first_rel + tile
        d_off = [None, None]
        for top in range(0, NSUB, 2):
            rows = slice(top * SUB, (top + 2) * SUB)
            wide_rows = []
            for a in range(top, top + 2):
                wide_cols = []
                for y in range(NSUB):
                    c_lo = y + a - NSUB
                    c_hi = c_lo + 1
                    lo_part = ds_ref[now if c_lo >= 0 else old, sub(a), sub(c_lo % NSUB)]
                    hi_part = ds_ref[now if c_hi >= 0 else old, sub(a), sub(c_hi % NSUB)]
                    wide_cols.append(jnp.where(lower, lo_part, hi_part).astype(BF16))
                wide_rows.append(jnp.concatenate(wide_cols, axis=1))
            by_off = jnp.concatenate(wide_rows, axis=0)
            gv_ref[rows, :] += dot(by_off, rel_ref[cols(rel_tile), :])
            for half in range(2):
                more = dot(qvt_ref[:, rows], by_off[:, half * 256:half * 256 + 256])
                d_off[half] = more if d_off[half] is None else d_off[half] + more
        for half in range(2):
            start = pl.multiple_of(rel_tile * TILE + half * 256, 256)
            drel_ref[:, pl.ds(start, 256)] += d_off[half]

        @pl.when((step == last) & (lax.rem(tile, 2) == 1) & (tile < top_tile))
        def _():
            key_pair = lax.div(tile, 2)
            off_pair = lax.div(top_tile - tile, 2)
            start_parts(off_pair, (2,))
            start_parts(key_pair, (0, 1))

            @pl.when(key_pair > 0)
            def _():
                finish_offsets(off_pair + 1)
                finish_keys(key_pair - 1)
        return 0

    @pl.when((step > half_steps) & (chip == 0))
    def _():
        finish_offsets(pair_at(step - 1))
        finish_keys(pair_at(step - 1))

    lax.fori_loop(0, blk + 1, grad_body, 0)
    grad_u = gu_ref[...] * inv_sqrt
    grad_v = gv_ref[...] * inv_sqrt
    st_rows_ref[step, 1] = (grad_u + grad_v).astype(BF16)
    bias_ref[0:1, :] += jnp.sum(grad_u, axis=0, keepdims=True)
    bias_ref[1:2, :] += jnp.sum(grad_v, axis=0, keepdims=True)
    deliver(blk, st_rows_ref.at[step], 0, rows_send.at[step], True)

    @pl.when((step >= half_steps) & (step < last) & (chip == 0))
    def _():
        start_parts(pair_at(step), (2, 0, 1))

    @pl.when(step == last)
    def _():
        start_parts(0, (2,))
        start_parts(top_pair, (0, 1))

        def finish_rest(idx, _):
            finish_offsets(1 - idx)
            finish_keys(top_pair - 1 + idx)
            return 0

        def drain(idx, _):
            for arr in range(3):
                part_copy(idx, arr).wait_send()
            tile = 2 * idx + core
            deliver(tile, st_grad_ref.at[idx, pl.ds(0, 2)], 1, grad_send.at[idx, 0], False)
            deliver(tile, st_grad_ref.at[idx, pl.ds(2, 1)], 2, grad_send.at[idx, 1], False)
            deliver(block_at(idx), st_rows_ref.at[idx], 0, rows_send.at[idx], False)
            return 0

        lax.fori_loop(0, 2, finish_rest, 0)
        lax.fori_loop(0, 2 * half_steps, drain, 0)
        for arr in range(5):
            own_copy(arr).wait_send()
            cross_copy(arr).wait_send()
            fwd_copy(arr).wait_send()
        for which, res in enumerate((res_own_ref, res_got_ref)):
            for local in range(block_tiles):
                for part, where in enumerate(PARTS):
                    dst = res.at[local, where]
                    pltpu.make_async_copy(dst, dst, res_sems.at[which, part, local]).wait()


def run_attn(u_bias, v_bias, k, v, q, d_out, rel_table, w_rel):
    block_len, _, head_dim = k.shape
    seq_len = 4 * block_len
    num_tiles = seq_len // TILE
    steps = num_tiles // 2
    block_tiles = block_len // TILE
    vec = pl.BlockSpec(memory_space=pltpu.VMEM)
    hbm = pl.BlockSpec(memory_space=pl.ANY)
    result = jax.ShapeDtypeStruct((block_tiles, 5, TILE, head_dim), BF16)
    dma = pltpu.SemaphoreType.DMA
    return pl.pallas_call(
        functools.partial(attn_kernel, num_tiles, head_dim ** -0.5),
        grid=(steps,),
        in_specs=[vec, vec] + [hbm] * 6,
        out_specs=[hbm, hbm, vec],
        scratch_shapes=[
            pltpu.VMEM((5, seq_len, head_dim), BF16),
            pltpu.VMEM((3, head_dim, seq_len), F32),
            pltpu.VMEM((head_dim, seq_len), BF16),
            pltpu.VMEM((head_dim, seq_len), BF16),
            pltpu.VMEM((head_dim, seq_len), BF16),
            pltpu.VMEM((TILE, seq_len), F32),
            pltpu.VMEM((3, TILE, TILE), F32),
            pltpu.VMEM((2, TILE, TILE), F32),
            pltpu.VMEM((TILE, TILE), BF16),
            pltpu.VMEM((TILE, TILE), BF16),
            pltpu.VMEM((TILE, head_dim), BF16),
            pltpu.VMEM((TILE, head_dim), BF16),
            pltpu.VMEM((head_dim, TILE), BF16),
            pltpu.VMEM((head_dim, TILE), BF16),
            pltpu.VMEM((head_dim, TILE), BF16),
            pltpu.VMEM((TILE, SUB), F32),
            pltpu.VMEM((TILE, SUB), F32),
            pltpu.VMEM((TILE, head_dim), F32),
            pltpu.VMEM((TILE, head_dim), F32),
            pltpu.VMEM((TILE, SUB), F32),
            pltpu.VMEM((steps, 2, TILE, head_dim), BF16),
            pltpu.VMEM((steps, 3, TILE, head_dim), BF16),
            pltpu.VMEM((steps, 3, head_dim, TILE), F32),
            pltpu.VMEM((5, block_len, head_dim), BF16),
            pltpu.VMEM((4,) + k.shape, BF16),
            pltpu.VMEM(rel_table.shape, BF16),
            pltpu.VMEM(w_rel.shape, BF16),
            pltpu.VMEM((w_rel.shape[0], 2 * head_dim), BF16),
            dma((6,)), dma((5,)), dma((5,)), dma((5,)), dma((5,)), dma((5,)), dma((5,)),
            dma((steps, 3)), dma((steps, 3)), dma((steps,)), dma((steps, 2)), dma((2, 3, block_tiles)),
        ],
        out_shape=[result, result, jax.ShapeDtypeStruct((2, head_dim), F32)],
        compiler_params=pltpu.CompilerParams(
            dimension_semantics=("arbitrary",), vmem_limit_bytes=67043328, collective_id=0, has_side_effects=True),
        name="attn_rows",
    )(u_bias, v_bias, k, v, q, d_out, rel_table, w_rel)


def exchange_matrix():
    row = lax.broadcasted_iota(jnp.int32, (SUB, SUB), 0)
    col = lax.broadcasted_iota(jnp.int32, (SUB, SUB), 1)
    return jnp.where(row + col == SUB - 1, 1.0, 0.0).astype(BF16)


def finish_kernel(own_in, got_in, table_in, bias_ref, o_ref, dq_ref, dk_ref, dv_ref, dw_ref, du_ref, dvb_ref,
                  own_ref, got_ref, table_ref, rel_ref, part_ref, core_ref, sum_ref, chip_ref, final_ref,
                  send_sems, recv_sems, load_sems):
    dev = lax.axis_index('cp')
    chip, core = lax.div(dev, 2), lax.rem(dev, 2)
    core_peer, chip_peer = dev + 1 - 2 * core, dev + 2 - 4 * chip
    barrier = pltpu.get_barrier_semaphore()
    for peer in (core_peer, chip_peer):
        pl.semaphore_signal(barrier, inc=1, device_id={'cp': peer}, device_id_type=pl.DeviceIdType.MESH)
    tiles = own_ref.shape[0]
    half = table_ref.shape[1] // 2
    loads = [pltpu.make_async_copy(src.at[:, where], dst.at[:, where], load_sems.at[idx]) for idx, (src, dst, where) in enumerate((
        (own_in, own_ref, pl.ds(4, 1)), (got_in, got_ref, pl.ds(4, 1)),
        (own_in, own_ref, pl.ds(0, 4)), (got_in, got_ref, pl.ds(0, 4))))]
    table_load = pltpu.make_async_copy(table_in, table_ref, load_sems.at[4])
    loads[0].start()
    loads[1].start()
    table_load.start()
    loads[2].start()
    loads[3].start()
    loads[0].wait()
    loads[1].wait()

    def heads(arr, tile):
        own, got = own_ref[tile, arr], got_ref[tile, arr]
        return jnp.where(chip == 0, own, got), jnp.where(chip == 0, got, own)

    for tile in range(tiles):
        rows = slice(tile * TILE, (tile + 1) * TILE)
        rel_ref[rows, :SUB], rel_ref[rows, SUB:] = heads(4, tile)

    def partial(which):
        for start in range(0, half, 256):
            at = pl.ds(pl.multiple_of(which * half + start, 256), 256)
            part_ref[which, start:start + 256] = lax.dot_general(
                table_ref[:, at], rel_ref[...], (((0,), (0,)), ((), ())), preferred_element_type=F32)
        bias = bias_ref[...]
        zero = jnp.zeros_like(bias)
        both = jnp.concatenate([jnp.where(chip == 0, bias, zero), jnp.where(chip == 0, zero, bias)], axis=1)
        part_ref[which, half:] = jnp.concatenate([both, jnp.zeros((6, both.shape[1]), F32)], axis=0)

    def swap(idx, src, dst, peer):
        copy = pltpu.make_async_remote_copy(
            src_ref=src, dst_ref=dst, send_sem=send_sems.at[idx], recv_sem=recv_sems.at[idx],
            device_id={'cp': peer}, device_id_type=pl.DeviceIdType.MESH)
        copy.start()
        return copy

    table_load.wait()
    partial(1 - core)
    pl.semaphore_wait(barrier, 2)
    first = swap(0, part_ref.at[1 - core], core_ref, core_peer)
    partial(core)
    first.wait()
    sum_ref[...] = part_ref[core] + core_ref[...]
    second = swap(1, sum_ref, chip_ref, chip_peer)
    loads[2].wait()
    loads[3].wait()
    for tile in range(tiles):
        rows = slice(tile * TILE, (tile + 1) * TILE)
        for arr, dst in enumerate((o_ref, dq_ref, dk_ref, dv_ref)):
            dst[rows] = jnp.stack(heads(arr, tile), axis=1)
    second.wait()
    final_ref[core] = sum_ref[...] + chip_ref[...]
    third = swap(2, final_ref.at[core], final_ref.at[core], core_peer)
    third.wait()
    for which in range(2):
        dw_ref[which * half:(which + 1) * half] = jnp.stack(
            [final_ref[which, :half, :SUB], final_ref[which, :half, SUB:]], axis=1)
    tail = final_ref[0, half:]
    du_ref[...] = jnp.concatenate([tail[0:1, :SUB], tail[0:1, SUB:]], axis=0)
    dvb_ref[...] = jnp.concatenate([tail[1:2, :SUB], tail[1:2, SUB:]], axis=0)


def finish(own, got, rel_table, bias_grad, seq_shape, w_shape):
    half_rows = w_shape[0] // 2 + 8
    wide = 2 * SUB
    vmem = pl.BlockSpec(memory_space=pltpu.VMEM)
    bias = jax.ShapeDtypeStruct((2, SUB), F32)
    seq = jax.ShapeDtypeStruct(seq_shape, BF16)
    return pl.pallas_call(
        finish_kernel,
        in_specs=[pl.BlockSpec(memory_space=pl.ANY)] * 3 + [vmem],
        out_specs=[vmem] * 7,
        out_shape=[seq, seq, seq, seq, jax.ShapeDtypeStruct(w_shape, F32), bias, bias],
        scratch_shapes=[
            pltpu.VMEM(own.shape, BF16),
            pltpu.VMEM(got.shape, BF16),
            pltpu.VMEM(rel_table.shape, BF16),
            pltpu.VMEM((rel_table.shape[0], wide), BF16),
            pltpu.VMEM((2, half_rows, wide), F32),
            pltpu.VMEM((half_rows, wide), F32),
            pltpu.VMEM((half_rows, wide), F32),
            pltpu.VMEM((half_rows, wide), F32),
            pltpu.VMEM((2, half_rows, wide), F32),
            pltpu.SemaphoreType.DMA((3,)),
            pltpu.SemaphoreType.DMA((3,)),
            pltpu.SemaphoreType.DMA((5,)),
        ],
        compiler_params=pltpu.CompilerParams(vmem_limit_bytes=48 * 1024 * 1024, collective_id=1, has_side_effects=True),
        name="finish",
    )(own, got, rel_table, bias_grad)


def solution(mesh):
    seq_spec = P('cp', 'hp', None)
    head_spec = P('hp', None)
    weight_spec = P(None, 'hp', None)

    def local_fn(q, k, v, u_bias, v_bias, rel_table, w_rel, d_out):
        res_own, res_got, bias_grad = run_attn(u_bias, v_bias, k, v, q, d_out, rel_table, w_rel)
        out, dq, dk, dv, d_w_rel, d_u, d_v = finish(res_own, res_got, rel_table, bias_grad, q.shape, w_rel.shape)
        return out, dq, dk, dv, d_u, d_v, d_w_rel

    return jax.shard_map(
        local_fn,
        mesh=mesh,
        in_specs=(seq_spec, seq_spec, seq_spec, head_spec, head_spec, P('cp', None), weight_spec, seq_spec),
        out_specs=(seq_spec, seq_spec, seq_spec, seq_spec, head_spec, head_spec, weight_spec),
        check_vma=False,
    )
```

```python
import functools

import jax
import jax.numpy as jnp
from jax import lax
from jax.experimental import pallas as pl
from jax.experimental.pallas import tpu as pltpu
from jax.sharding import PartitionSpec as P

TILE = 512
SUB = 128
NSUB = TILE // SUB
MROWS = 2
PARTS = (pl.ds(0, 2), pl.ds(2, 2), pl.ds(4, 1))
LOG2E = 1.4426950408889634
F32 = jnp.float32
BF16 = jnp.bfloat16


def dot(lhs, rhs):
    return jnp.dot(lhs, rhs, preferred_element_type=F32)


def sub(idx):
    return slice(idx * SUB, (idx + 1) * SUB)


def roll_left(part, flip):
    groups = []
    for start in range(0, SUB, 8):
        rows = jnp.take_along_axis(part[start:start + 8], flip, axis=0)
        rows = pltpu.roll(rows, (SUB - 8 - start) % SUB, 1, stride=1, stride_axis=0)
        groups.append(jnp.take_along_axis(rows, flip, axis=0))
    return jnp.concatenate(groups, axis=0)


def attn_kernel(num_tiles, inv_sqrt, u_ref, v_ref, kin_ref, vin_ref, qin_ref, doin_ref, table_in_ref, w_in_ref,
                o_ref, dq_ref, dk_out_ref, dv_out_ref, dw_out_ref, du_ref, dvb_ref, res_own_ref, res_got_ref,
                full_ref, acc_ref, kt_ref, valt_ref, relt_ref, sc_ref, rot_ref, ds_ref, dw_ref, p_ref,
                qu_ref, qv_ref, qut_ref, qvt_ref, dot_ref, max_ref, sum_ref, gu_ref, gv_ref, row_ref,
                st_rows_ref, st_grad_ref, part_ref, away_ref, raw_ref, table_ref, w_ref, wide_ref, bias_ref, res_rel_ref,
                core_ref, chip_ref, final_ref, sum_send, sum_recv,
                local_sems, own_send, own_recv, cross_send, cross_recv, fwd_send, fwd_recv,
                part_send, part_recv, rows_send, grad_send, res_sems, load_sems, out_sems):
    step = pl.program_id(0)
    last = pl.num_programs(0) - 1
    dev = lax.axis_index('cp')
    chip, core = lax.div(dev, 2), lax.rem(dev, 2)
    core_peer, chip_peer = dev + 1 - 2 * core, dev + 2 - 4 * chip
    half_steps = num_tiles // 4

    def pair_at(idx):
        first = jnp.where(idx < half_steps, idx, 3 * half_steps - 1 - idx)
        second = jnp.where(idx < half_steps - 1, idx + half_steps, 2 * half_steps - 2 - idx)
        second = jnp.where(idx == last, last, second)
        return jnp.where(chip == 0, first, second)

    def block_at(idx):
        odd = lax.rem(pair_at(idx), 2)
        return 2 * pair_at(idx) + odd + core - 2 * odd * core

    blk = block_at(step)
    scale = inv_sqrt * LOG2E
    block_len = away_ref.shape[1]
    block_tiles = block_len // TILE
    k_ref, val_ref, rel_ref = full_ref.at[0], full_ref.at[1], full_ref.at[2]
    q_ref, do_ref = full_ref.at[3], full_ref.at[4]
    dk_ref, dv_ref, drel_ref = acc_ref.at[0], acc_ref.at[1], acc_ref.at[2]

    def cols(tile):
        return pl.ds(pl.multiple_of(tile * TILE, TILE), TILE)

    def place(arr, block):
        at = 3 - block if arr == 2 else block
        return full_ref.at[arr, pl.ds(pl.multiple_of(at * block_len, block_len), block_len)]

    def to_device(src, dst, send_sem, recv_sem, peer):
        return pltpu.make_async_remote_copy(
            src_ref=src, dst_ref=dst, send_sem=send_sem, recv_sem=recv_sem,
            device_id={'cp': peer}, device_id_type=pl.DeviceIdType.MESH)

    def own_copy(arr):
        return to_device(place(arr, dev), place(arr, dev), own_send.at[arr], own_recv.at[arr], core_peer)

    def cross_copy(arr):
        return to_device(away_ref.at[arr], place(arr, dev), cross_send.at[arr], cross_recv.at[arr], chip_peer)

    def fwd_copy(arr):
        return to_device(place(arr, chip_peer), place(arr, chip_peer), fwd_send.at[arr], fwd_recv.at[arr], core_peer)

    def transpose_half(arr, which):
        dst = (kt_ref, valt_ref, relt_ref)[arr]
        first = (1 - which if arr == 2 else which) * (num_tiles // 2)

        def body(idx, _):
            dst[:, cols(first + idx)] = full_ref[arr, cols(first + idx), :].T
            return 0
        lax.fori_loop(0, num_tiles // 2, body, 0)

    def arrive(arrays):
        for arr in arrays:
            cross_copy(arr).wait_recv()
            fwd_copy(arr).start()
        for arr in arrays:
            fwd_copy(arr).wait_recv()
            if arr < 3:
                transpose_half(arr, 1 - chip)

    def part_copy(slot, arr):
        tile = 2 * slot + 1 - core
        at = num_tiles - 1 - tile if arr == 2 else tile
        return to_device(acc_ref.at[arr, :, cols(at)], part_ref.at[slot, arr],
                         part_send.at[slot, arr], part_recv.at[slot, arr], core_peer)

    def start_parts(slot, arrays):
        for arr in arrays:
            part_copy(slot, arr).start()

    def deliver(tile, stage, part, send_sem, start):
        owner = lax.div(tile, block_tiles)
        local = tile - owner * block_tiles
        if part == 2:
            own_dst, got_dst = res_rel_ref.at[0, pl.ds(local, 1)], res_rel_ref.at[1, pl.ds(local, 1)]
        else:
            own_dst, got_dst = res_own_ref.at[local, PARTS[part]], res_got_ref.at[local, PARTS[part]]

        @pl.when(owner == dev)
        def _():
            if start:
                pltpu.make_async_copy(stage, own_dst, res_sems.at[0, part, local]).start()

        @pl.when(owner == core_peer)
        def _():
            copy = to_device(stage, own_dst, send_sem, res_sems.at[0, part, local], owner)
            copy.start() if start else copy.wait_send()

        @pl.when(lax.div(owner, 2) != chip)
        def _():
            copy = to_device(stage, got_dst, send_sem, res_sems.at[1, part, local], owner)
            copy.start() if start else copy.wait_send()

    def finish_keys(slot):
        tile = 2 * slot + core
        for arr in range(2):
            part_copy(slot, arr).wait_recv()
        d_key = (acc_ref[0, :, cols(tile)] + part_ref[slot, 0]) * inv_sqrt
        st_grad_ref[slot, 0] = d_key.astype(BF16).T
        d_val = acc_ref[1, :, cols(tile)] + part_ref[slot, 1]
        st_grad_ref[slot, 1] = d_val.astype(BF16).T
        deliver(tile, st_grad_ref.at[slot, pl.ds(0, 2)], 1, grad_send.at[slot, 0], True)

    def finish_offsets(slot):
        tile = 2 * slot + core
        part_copy(slot, 2).wait_recv()
        d_off = ((acc_ref[2, :, cols(num_tiles - 1 - tile)] + part_ref[slot, 2]) * inv_sqrt).astype(BF16)
        flip_rows = exchange_matrix()
        for chunk in range(NSUB):
            back = lax.dot_general(flip_rows, d_off[:, sub(chunk)], (((1,), (1,)), ((), ())), preferred_element_type=F32)
            st_grad_ref[slot, 2, sub(NSUB - 1 - chunk)] = back.astype(BF16)
        deliver(tile, st_grad_ref.at[slot, pl.ds(2, 1)], 2, grad_send.at[slot, 1], True)

    top_tile = 2 * pair_at(last) + 1
    top_pair = pair_at(last)

    def finish_all():
        model_dim = table_ref.shape[1]
        half = model_dim // 2
        quarter = half // 2
        size = quarter + 8

        def piece(which, chunk):
            return rot_ref.at[which, pl.ds(0, size), pl.ds(chunk * 256, 256)]

        def total_piece(chunk):
            return rot_ref.at[2, pl.ds(0, size), pl.ds(chunk * 256, 256)]

        def wait_res(which, part):
            for local in range(block_tiles):
                if part == 2:
                    dst = res_rel_ref.at[which, pl.ds(local, 1)]
                else:
                    dst = (res_own_ref, res_got_ref)[which].at[local, PARTS[part]]
                pltpu.make_async_copy(dst, dst, res_sems.at[which, part, local]).wait()

        def partial(which, chunk, src):
            head = chip if src == 0 else 1 - chip
            lanes = pl.ds(pl.multiple_of(head * SUB, SUB), SUB)
            at = pl.ds(pl.multiple_of(which * half + chunk * quarter, 256), quarter)
            d_rel = jnp.concatenate([res_rel_ref[src, tile] for tile in range(block_tiles)], axis=0)
            piece(which, chunk)[pl.ds(0, quarter), lanes] = lax.dot_general(
                table_ref[:, at], d_rel, (((0,), (0,)), ((), ())), preferred_element_type=F32)
            bias = bias_ref[...] if src == 0 else jnp.zeros_like(bias_ref)
            piece(which, chunk)[pl.ds(quarter, 8), lanes] = jnp.concatenate([bias, jnp.zeros((6, SUB), F32)], axis=0)

        def swap(idx, src, dst, peer):
            copy = to_device(src, dst, sum_send.at[idx], sum_recv.at[idx], peer)
            copy.start()
            return copy

        order = ((1 - core, 0), (core, 0), (1 - core, 1), (core, 1))
        wait_res(0, 2)
        for which, chunk in order:
            partial(which, chunk, 0)
        wait_res(1, 2)
        first, second, third = [], [], []
        for chunk in range(2):
            partial(1 - core, chunk, 1)
            first.append(swap(chunk, piece(1 - core, chunk), core_ref.at[chunk], core_peer))
            partial(core, chunk, 1)
            first[chunk].wait()
            total_piece(chunk)[...] = piece(core, chunk)[...] + core_ref[chunk]
            second.append(swap(2 + chunk, total_piece(chunk), chip_ref.at[chunk], chip_peer))
        for part in range(2):
            wait_res(0, part)
            wait_res(1, part)
        loads = []
        for tile in range(block_tiles):
            for which, res in enumerate((res_own_ref, res_got_ref)):
                dst = full_ref.at[pl.ds(0, 4), pl.ds((which * block_tiles + tile) * TILE, TILE)]
                loads.append(pltpu.make_async_copy(res.at[tile], dst, load_sems.at[tile, which]))
        for load in loads:
            load.start()
        for tile in range(block_tiles):
            loads[2 * tile].wait()
            loads[2 * tile + 1].wait()
            rows = slice(tile * TILE, (tile + 1) * TILE)
            for arr in range(4):
                own = full_ref[arr, rows]
                got = full_ref[arr, (block_tiles + tile) * TILE:(block_tiles + tile + 1) * TILE]
                raw_ref[arr, rows] = jnp.stack([jnp.where(chip == 0, own, got), jnp.where(chip == 0, got, own)], axis=1)
        stores = [pltpu.make_async_copy(raw_ref.at[arr], dst, local_sems.at[arr])
                  for arr, dst in enumerate((o_ref, dq_ref, dk_out_ref, dv_out_ref))]
        for store in stores:
            store.start()

        def put(which, chunk):
            base = pl.multiple_of(which * half + chunk * quarter, 256)
            for head in range(2):
                store = pltpu.make_async_copy(
                    final_ref.at[which, chunk, pl.ds(0, quarter), pl.ds(head * SUB, SUB)],
                    dw_out_ref.at[head, pl.ds(base, quarter)], out_sems.at[len(stores) - 4])
                store.start()
                stores.append(store)

        for chunk in range(2):
            second[chunk].wait()
            final_ref[core, chunk] = total_piece(chunk)[...] + chip_ref[chunk]
            third.append(swap(4 + chunk, final_ref.at[core, chunk], final_ref.at[core, chunk], core_peer))
            put(core, chunk)
        for chunk in range(2):
            third[chunk].wait()
            put(1 - core, chunk)
        sums = final_ref[0, 0, quarter:]
        du_ref[...] = jnp.concatenate([sums[0:1, :SUB], sums[0:1, SUB:]], axis=0)
        dvb_ref[...] = jnp.concatenate([sums[1:2, :SUB], sums[1:2, SUB:]], axis=0)
        for store in stores:
            store.wait()

    def put_heads(arr, start, size, first, second):
        at = 3 - dev if arr == 2 else dev
        own_at = pl.ds(pl.multiple_of(at * block_len + start, SUB), size)
        away_at = pl.ds(pl.multiple_of(start, SUB), size)
        full_ref[arr, own_at] = jnp.where(chip == 0, first, second)
        away_ref[arr, away_at] = jnp.where(chip == 0, second, first)

    def pack_seq(arr, src):
        def body(idx, _):
            heads = jnp.swapaxes(raw_ref[src, cols(idx)], 0, 1)
            put_heads(arr, idx * TILE, TILE, heads[0], heads[1])
            return 0
        lax.fori_loop(0, block_tiles, body, 0)

    def pack_rel():
        weights = jnp.swapaxes(w_ref[...], 0, 1)
        wide_ref[:, :SUB] = weights[0]
        wide_ref[:, SUB:] = weights[1]

        def body(idx, _):
            rel = dot(table_ref[cols(idx), :], wide_ref[...]).astype(BF16)
            flip_rows = exchange_matrix()
            for chunk in range(NSUB):
                back = dot(flip_rows, rel[sub(NSUB - 1 - chunk)]).astype(BF16)
                put_heads(2, (block_tiles - 1 - idx) * TILE + chunk * SUB, SUB, back[:, :SUB], back[:, SUB:])
            return 0
        lax.fori_loop(0, block_tiles, body, 0)

    @pl.when(step == 0)
    def _():
        barrier = pltpu.get_barrier_semaphore()
        for peer in (core_peer, chip_peer, 3 - dev):
            pl.semaphore_signal(barrier, inc=1, device_id={'cp': peer}, device_id_type=pl.DeviceIdType.MESH)
        loads = [pltpu.make_async_copy(src, dst, local_sems.at[idx]) for idx, (src, dst) in enumerate((
            (kin_ref, raw_ref.at[0]), (w_in_ref, w_ref), (table_in_ref, table_ref),
            (vin_ref, raw_ref.at[1]), (qin_ref, raw_ref.at[2]), (doin_ref, raw_ref.at[3])))]
        loads[0].start()

        def clear(tile, _):
            acc_ref[:, :, cols(tile)] = jnp.zeros((3, SUB, TILE), F32)
            return 0

        def ship(arr):
            cross_copy(arr).start()
            own_copy(arr).start()

        loads[0].wait()
        for load in loads[1:]:
            load.start()
        pack_seq(0, 0)
        pl.semaphore_wait(barrier, 3)
        ship(0)
        loads[1].wait()
        loads[2].wait()
        pack_rel()
        ship(2)
        def load_and_ship(arr):
            idx = (1, 3, 4).index(arr)
            loads[3 + idx].wait()
            pack_seq(arr, idx + 1)
            ship(arr)

        @pl.when(chip == 0)
        def _():
            load_and_ship(1)
        load_and_ship(3)

        @pl.when(chip == 1)
        def _():
            load_and_ship(1)
        load_and_ship(4)
        lax.fori_loop(0, num_tiles, clear, 0)
        bias_ref[...] = jnp.zeros_like(bias_ref)
        for arr in (0, 2, 1, 3, 4):
            own_copy(arr).wait_recv()
            if arr < 3:
                transpose_half(arr, chip)

    @pl.when(step == half_steps * (1 - chip))
    def _():
        arrive((0, 2))

    @pl.when(step == half_steps - chip)
    def _():
        arrive((3,))

    rows_at = cols(blk)
    q_wide = q_ref[rows_at, :].astype(F32)
    q_u = (q_wide + u_ref[pl.ds(chip, 1), :]).astype(BF16)
    q_v = (q_wide + v_ref[pl.ds(chip, 1), :]).astype(BF16)
    qu_ref[...] = q_u
    qv_ref[...] = q_v
    qut_ref[...] = q_u.T
    qvt_ref[...] = q_v.T
    max_ref[...] = jnp.full_like(max_ref, -jnp.inf)
    sum_ref[...] = jnp.zeros_like(sum_ref)
    gu_ref[...] = jnp.zeros_like(gu_ref)
    gv_ref[...] = jnp.zeros_like(gv_ref)
    lane = lax.broadcasted_iota(jnp.int32, (SUB, SUB), 1)
    row = lax.broadcasted_iota(jnp.int32, (SUB, SUB), 0)
    upper = lane > row
    flip = 7 - lax.broadcasted_iota(jnp.int32, (8, SUB), 0)
    lower = lane + row < SUB - 1
    first_rel = num_tiles - 1 - blk

    def rotate_rel(tile, slot):
        for half in range(2):
            start = pl.multiple_of(tile * TILE + half * 256, 256)
            for a in range(NSUB):
                if a % MROWS == 0:
                    by_offset = dot(qv_ref[a * SUB:(a + MROWS) * SUB, :], relt_ref[:, pl.ds(start, 256)])
                for c in range(2):
                    part = by_offset[sub(a % MROWS), sub(c)]
                    rot_ref[slot, sub(a), sub(half * 2 + c)] = pltpu.roll(part, 1, 1, stride=1, stride_axis=0)

    rotate_rel(first_rel, 0)
    rotate_rel(jnp.minimum(first_rel + 1, num_tiles - 1), 1)

    def score_tile(tile, diag):
        left = lax.rem(tile, 3)
        right = lax.rem(tile + 1, 3)
        for half in range(2):
            start = pl.multiple_of(tile * TILE + half * 256, 256)
            for a in range(NSUB):
                if a % MROWS == 0:
                    content = dot(qu_ref[a * SUB:(a + MROWS) * SUB, :], kt_ref[:, pl.ds(start, 256)])
                run_max = max_ref[sub(a), :]
                for c2 in range(2):
                    c = half * 2 + c2
                    hi, lo = c - a + NSUB, c - a + NSUB - 1
                    if diag and c > a:
                        score = jnp.full((SUB, SUB), -jnp.inf, F32)
                    else:
                        low_part = rot_ref[left if lo < NSUB else right, sub(a), sub(lo % NSUB)]
                        if diag and c == a:
                            score = jnp.where(upper, -jnp.inf, (content[sub(a % MROWS), sub(c2)] + low_part) * scale)
                        else:
                            high_part = rot_ref[left if hi < NSUB else right, sub(a), sub(hi % NSUB)]
                            score = (content[sub(a % MROWS), sub(c2)] + jnp.where(upper, high_part, low_part)) * scale
                    run_max = jnp.maximum(run_max, score)
                    sc_ref[sub(a), pl.ds(pl.multiple_of(tile * TILE + c * SUB, SUB), SUB)] = score
                max_ref[sub(a), :] = run_max
        if not diag:
            rotate_rel(jnp.minimum(first_rel + tile + 2, num_tiles - 1), lax.rem(tile + 2, 3))

    def score_body(tile, _):
        score_tile(tile, False)
        return 0

    lax.fori_loop(0, blk, score_body, 0)
    score_tile(blk, True)
    max_ref[...] = jnp.broadcast_to(jnp.max(max_ref[...], axis=1, keepdims=True), (TILE, SUB))

    @pl.when(step == half_steps * (1 - chip))
    def _():
        arrive((1,))

    def prob_body(tile, _):
        for top in range(0, NSUB, 2):
            rows = slice(top * SUB, (top + 2) * SUB)
            prob_rows = []
            for a in range(top, top + 2):
                run_sum = sum_ref[sub(a), :]
                row_max = max_ref[sub(a), :]
                prob_cols = []
                for c in range(NSUB):
                    where = pl.ds(pl.multiple_of(tile * TILE + c * SUB, SUB), SUB)
                    prob = jnp.exp2(sc_ref[sub(a), where] - row_max)
                    prob_cols.append(prob.astype(BF16))
                    run_sum = run_sum + prob
                sum_ref[sub(a), :] = run_sum
                prob_rows.append(jnp.concatenate(prob_cols, axis=1))
            gu_ref[rows, :] += dot(jnp.concatenate(prob_rows, axis=0), val_ref[cols(tile), :])
        return 0

    lax.fori_loop(0, blk + 1, prob_body, 0)
    @pl.when(step == half_steps - chip)
    def _():
        arrive((4,))

    dot_ref[...] = do_ref[rows_at, :].T
    total = jnp.sum(sum_ref[...], axis=1, keepdims=True)
    inv_sum = 1.0 / total
    out = gu_ref[...] * inv_sum
    st_rows_ref[step, 0] = out.astype(BF16)
    delta = jnp.sum(out * do_ref[rows_at, :].astype(F32), axis=1, keepdims=True)
    row_ref[...] = jnp.broadcast_to(delta, (TILE, SUB))
    sum_ref[...] = max_ref[...] + jnp.log2(total)
    gu_ref[...] = jnp.zeros_like(gu_ref)
    ds_ref[1, :, :] = jnp.zeros((TILE, TILE), F32)

    def grad_body(tile, _):
        now = lax.rem(tile, 2)
        old = 1 - now
        for half in range(2):
            start = pl.multiple_of(tile * TILE + half * 256, 256)
            win = pl.ds(start, 256)
            d_val = d_key = None
            for top in range(0, NSUB, 2):
                rows = slice(top * SUB, (top + 2) * SUB)
                do_rows = pl.ds(pl.multiple_of(blk * TILE + top * SUB, SUB), 2 * SUB)
                d_prob = dot(do_ref[do_rows, :], valt_ref[:, win])
                prob_rows, score_rows = [], []
                for a in range(top, top + 2):
                    log_norm = sum_ref[sub(a), :]
                    shift = row_ref[sub(a), :]
                    prob_cols, score_cols = [], []
                    for c2 in range(2):
                        c = half * 2 + c2
                        prob = jnp.exp2(sc_ref[sub(a), pl.ds(pl.multiple_of(tile * TILE + c * SUB, SUB), SUB)] - log_norm)
                        d_score = prob * (d_prob[sub(a - top), sub(c2)] - shift)
                        ds_ref[now, sub(a), sub(c)] = roll_left(d_score, flip)
                        prob_cols.append(prob.astype(BF16))
                        score_cols.append(d_score.astype(BF16))
                    prob_rows.append(jnp.concatenate(prob_cols, axis=1))
                    score_rows.append(jnp.concatenate(score_cols, axis=1))
                probs = jnp.concatenate(prob_rows, axis=0)
                scores = jnp.concatenate(score_rows, axis=0)
                more_val, more_key = dot(dot_ref[:, rows], probs), dot(qut_ref[:, rows], scores)
                d_val = more_val if d_val is None else d_val + more_val
                d_key = more_key if d_key is None else d_key + more_key
                gu_ref[rows, :] += dot(scores, k_ref[win, :])
            dv_ref[:, win] += d_val
            dk_ref[:, win] += d_key
        rel_tile = first_rel + tile
        d_off = [None, None]
        for top in range(0, NSUB, 2):
            rows = slice(top * SUB, (top + 2) * SUB)
            wide_rows = []
            for a in range(top, top + 2):
                wide_cols = []
                for y in range(NSUB):
                    c_lo = y + a - NSUB
                    c_hi = c_lo + 1
                    lo_part = ds_ref[now if c_lo >= 0 else old, sub(a), sub(c_lo % NSUB)]
                    hi_part = ds_ref[now if c_hi >= 0 else old, sub(a), sub(c_hi % NSUB)]
                    wide_cols.append(jnp.where(lower, lo_part, hi_part).astype(BF16))
                wide_rows.append(jnp.concatenate(wide_cols, axis=1))
            by_off = jnp.concatenate(wide_rows, axis=0)
            gv_ref[rows, :] += dot(by_off, rel_ref[cols(rel_tile), :])
            for half in range(2):
                more = dot(qvt_ref[:, rows], by_off[:, half * 256:half * 256 + 256])
                d_off[half] = more if d_off[half] is None else d_off[half] + more
        for half in range(2):
            start = pl.multiple_of(rel_tile * TILE + half * 256, 256)
            drel_ref[:, pl.ds(start, 256)] += d_off[half]

        @pl.when((step == last) & (lax.rem(tile, 2) == 1) & (tile < top_tile))
        def _():
            key_pair = lax.div(tile, 2)
            off_pair = lax.div(top_tile - tile, 2)
            start_parts(off_pair, (2,))
            start_parts(key_pair, (0, 1))

            @pl.when(key_pair > 0)
            def _():
                finish_offsets(off_pair + 1)
                finish_keys(key_pair - 1)
        return 0

    @pl.when((step > half_steps) & (chip == 0))
    def _():
        finish_offsets(pair_at(step - 1))
        finish_keys(pair_at(step - 1))

    lax.fori_loop(0, blk + 1, grad_body, 0)
    grad_u = gu_ref[...] * inv_sqrt
    grad_v = gv_ref[...] * inv_sqrt
    st_rows_ref[step, 1] = (grad_u + grad_v).astype(BF16)
    bias_ref[0:1, :] += jnp.sum(grad_u, axis=0, keepdims=True)
    bias_ref[1:2, :] += jnp.sum(grad_v, axis=0, keepdims=True)
    deliver(blk, st_rows_ref.at[step], 0, rows_send.at[step], True)

    @pl.when((step >= half_steps) & (step < last) & (chip == 0))
    def _():
        start_parts(pair_at(step), (2, 0, 1))

    @pl.when(step == last)
    def _():
        start_parts(0, (2,))
        start_parts(top_pair, (0, 1))

        def finish_rest(idx, _):
            finish_offsets(1 - idx)
            finish_keys(top_pair - 1 + idx)
            return 0

        def drain(idx, _):
            for arr in range(3):
                part_copy(idx, arr).wait_send()
            tile = 2 * idx + core
            deliver(tile, st_grad_ref.at[idx, pl.ds(0, 2)], 1, grad_send.at[idx, 0], False)
            deliver(tile, st_grad_ref.at[idx, pl.ds(2, 1)], 2, grad_send.at[idx, 1], False)
            deliver(block_at(idx), st_rows_ref.at[idx], 0, rows_send.at[idx], False)
            return 0

        lax.fori_loop(0, 2, finish_rest, 0)
        for arr in range(5):
            own_copy(arr).wait_send()
            cross_copy(arr).wait_send()
            fwd_copy(arr).wait_send()
        finish_all()
        lax.fori_loop(0, 2 * half_steps, drain, 0)


def run_attn(u_bias, v_bias, k, v, q, d_out, rel_table, w_rel):
    block_len, _, head_dim = k.shape
    seq_len = 4 * block_len
    num_tiles = seq_len // TILE
    steps = num_tiles // 2
    block_tiles = block_len // TILE
    vec = pl.BlockSpec(memory_space=pltpu.VMEM)
    hbm = pl.BlockSpec(memory_space=pl.ANY)
    result = jax.ShapeDtypeStruct((block_tiles, 4, TILE, head_dim), BF16)
    seq = jax.ShapeDtypeStruct(k.shape, BF16)
    bias = jax.ShapeDtypeStruct((2, head_dim), F32)
    d_weights = jax.ShapeDtypeStruct((2, w_rel.shape[0], head_dim), F32)
    size = w_rel.shape[0] // 4 + 8
    dma = pltpu.SemaphoreType.DMA
    return pl.pallas_call(
        functools.partial(attn_kernel, num_tiles, head_dim ** -0.5),
        grid=(steps,),
        in_specs=[vec, vec] + [hbm] * 6,
        out_specs=[hbm] * 5 + [vec, vec, hbm, hbm],
        scratch_shapes=[
            pltpu.VMEM((5, seq_len, head_dim), BF16),
            pltpu.VMEM((3, head_dim, seq_len), F32),
            pltpu.VMEM((head_dim, seq_len), BF16),
            pltpu.VMEM((head_dim, seq_len), BF16),
            pltpu.VMEM((head_dim, seq_len), BF16),
            pltpu.VMEM((TILE, seq_len), F32),
            pltpu.VMEM((3, TILE, TILE), F32),
            pltpu.VMEM((2, TILE, TILE), F32),
            pltpu.VMEM((TILE, TILE), BF16),
            pltpu.VMEM((TILE, TILE), BF16),
            pltpu.VMEM((TILE, head_dim), BF16),
            pltpu.VMEM((TILE, head_dim), BF16),
            pltpu.VMEM((head_dim, TILE), BF16),
            pltpu.VMEM((head_dim, TILE), BF16),
            pltpu.VMEM((head_dim, TILE), BF16),
            pltpu.VMEM((TILE, SUB), F32),
            pltpu.VMEM((TILE, SUB), F32),
            pltpu.VMEM((TILE, head_dim), F32),
            pltpu.VMEM((TILE, head_dim), F32),
            pltpu.VMEM((TILE, SUB), F32),
            pltpu.VMEM((steps, 2, TILE, head_dim), BF16),
            pltpu.VMEM((steps, 3, TILE, head_dim), BF16),
            pltpu.VMEM((steps, 3, head_dim, TILE), F32),
            pltpu.VMEM((5, block_len, head_dim), BF16),
            pltpu.VMEM((4,) + k.shape, BF16),
            pltpu.VMEM(rel_table.shape, BF16),
            pltpu.VMEM(w_rel.shape, BF16),
            pltpu.VMEM((w_rel.shape[0], 2 * head_dim), BF16),
            pltpu.VMEM((2, head_dim), F32),
            pltpu.VMEM((2, block_tiles, TILE, head_dim), BF16),
            pltpu.VMEM((2, size, 2 * head_dim), F32),
            pltpu.VMEM((2, size, 2 * head_dim), F32),
            pltpu.VMEM((2, 2, size, 2 * head_dim), F32),
            dma((6,)), dma((6,)),
            dma((6,)), dma((5,)), dma((5,)), dma((5,)), dma((5,)), dma((5,)), dma((5,)),
            dma((steps, 3)), dma((steps, 3)), dma((steps,)), dma((steps, 2)), dma((2, 3, block_tiles)), dma((block_tiles, 2)), dma((8,)),
        ],
        out_shape=[seq, seq, seq, seq, d_weights, bias, bias, result, result],
        compiler_params=pltpu.CompilerParams(
            dimension_semantics=("arbitrary",), vmem_limit_bytes=67043328, collective_id=0, has_side_effects=True),
        name="attn_rows",
    )(u_bias, v_bias, k, v, q, d_out, rel_table, w_rel)


def exchange_matrix():
    row = lax.broadcasted_iota(jnp.int32, (SUB, SUB), 0)
    col = lax.broadcasted_iota(jnp.int32, (SUB, SUB), 1)
    return jnp.where(row + col == SUB - 1, 1.0, 0.0).astype(BF16)


def solution(mesh):
    seq_spec = P('cp', 'hp', None)
    head_spec = P('hp', None)
    weight_spec = P(None, 'hp', None)

    def local_fn(q, k, v, u_bias, v_bias, rel_table, w_rel, d_out):
        out, dq, dk, dv, d_w_rel, d_u, d_v, _, _ = run_attn(u_bias, v_bias, k, v, q, d_out, rel_table, w_rel)
        return out, dq, dk, dv, d_u, d_v, jnp.swapaxes(d_w_rel, 0, 1)

    return jax.shard_map(
        local_fn,
        mesh=mesh,
        in_specs=(seq_spec, seq_spec, seq_spec, head_spec, head_spec, P('cp', None), weight_spec, seq_spec),
        out_specs=(seq_spec, seq_spec, seq_spec, seq_spec, head_spec, head_spec, weight_spec),
        check_vma=False,
    )
```

```python
import functools

import jax
import jax.numpy as jnp
from jax import lax
from jax.experimental import pallas as pl
from jax.experimental.pallas import tpu as pltpu
from jax.sharding import PartitionSpec as P

TILE = 512
SUB = 128
NSUB = TILE // SUB
MROWS = 2
PARTS = (pl.ds(0, 2), pl.ds(2, 2), pl.ds(4, 1))
LOG2E = 1.4426950408889634
F32 = jnp.float32
BF16 = jnp.bfloat16


def dot(lhs, rhs):
    return jnp.dot(lhs, rhs, preferred_element_type=F32)


def sub(idx):
    return slice(idx * SUB, (idx + 1) * SUB)


def roll_left(part, flip):
    groups = []
    for start in range(0, SUB, 8):
        rows = jnp.take_along_axis(part[start:start + 8], flip, axis=0)
        rows = pltpu.roll(rows, (SUB - 8 - start) % SUB, 1, stride=1, stride_axis=0)
        groups.append(jnp.take_along_axis(rows, flip, axis=0))
    return jnp.concatenate(groups, axis=0)


def attn_kernel(num_tiles, inv_sqrt, u_ref, v_ref, kin_ref, vin_ref, qin_ref, doin_ref, table_in_ref, w_in_ref,
                o_ref, dq_ref, dk_out_ref, dv_out_ref, dw_out_ref, du_ref, dvb_ref, res_own_ref, res_got_ref,
                full_ref, acc_ref, kt_ref, valt_ref, relt_ref, sc_ref, rot_ref, ds_ref,
                qu_ref, qv_ref, qut_ref, qvt_ref, dot_ref, max_ref, sum_ref, gu_ref, gv_ref, row_ref,
                st_rows_ref, st_grad_ref, part_ref, away_ref, raw_ref, table_ref, w_ref, wide_ref, bias_ref, res_rel_ref,
                core_ref, chip_ref, final_ref, dw_stage_ref, sum_send, sum_recv,
                local_sems, own_send, own_recv, cross_send, cross_recv, fwd_send, fwd_recv,
                part_send, part_recv, rows_send, grad_send, res_sems, load_sems, out_sems):
    step = pl.program_id(0)
    last = pl.num_programs(0) - 1
    dev = lax.axis_index('cp')
    chip, core = lax.div(dev, 2), lax.rem(dev, 2)
    core_peer, chip_peer = dev + 1 - 2 * core, dev + 2 - 4 * chip
    half_steps = num_tiles // 4

    def pair_at(idx):
        first = jnp.where(idx < half_steps, idx, 3 * half_steps - 1 - idx)
        second = jnp.where(idx < half_steps - 1, idx + half_steps, 2 * half_steps - 2 - idx)
        second = jnp.where(idx == last, last, second)
        return jnp.where(chip == 0, first, second)

    def block_at(idx):
        odd = lax.rem(pair_at(idx), 2)
        return 2 * pair_at(idx) + odd + core - 2 * odd * core

    blk = block_at(step)
    scale = inv_sqrt * LOG2E
    block_len = away_ref.shape[1]
    block_tiles = block_len // TILE
    k_ref, val_ref, rel_ref = full_ref.at[0], full_ref.at[1], full_ref.at[2]
    q_ref, do_ref = full_ref.at[3], full_ref.at[4]
    dk_ref, dv_ref, drel_ref = acc_ref.at[0], acc_ref.at[1], acc_ref.at[2]

    def cols(tile):
        return pl.ds(pl.multiple_of(tile * TILE, TILE), TILE)

    def place(arr, block):
        at = 3 - block if arr == 2 else block
        return full_ref.at[arr, pl.ds(pl.multiple_of(at * block_len, block_len), block_len)]

    def to_device(src, dst, send_sem, recv_sem, peer):
        return pltpu.make_async_remote_copy(
            src_ref=src, dst_ref=dst, send_sem=send_sem, recv_sem=recv_sem,
            device_id={'cp': peer}, device_id_type=pl.DeviceIdType.MESH)

    def own_copy(arr):
        return to_device(place(arr, dev), place(arr, dev), own_send.at[arr], own_recv.at[arr], core_peer)

    def cross_copy(arr):
        return to_device(away_ref.at[arr], place(arr, dev), cross_send.at[arr], cross_recv.at[arr], chip_peer)

    def fwd_copy(arr):
        return to_device(place(arr, chip_peer), place(arr, chip_peer), fwd_send.at[arr], fwd_recv.at[arr], core_peer)

    def transpose_half(arr, which):
        dst = (kt_ref, valt_ref, relt_ref)[arr]
        first = (1 - which if arr == 2 else which) * (num_tiles // 2)

        def body(idx, _):
            dst[:, cols(first + idx)] = full_ref[arr, cols(first + idx), :].T
            return 0
        lax.fori_loop(0, num_tiles // 2, body, 0)

    def arrive(arrays):
        for arr in arrays:
            cross_copy(arr).wait_recv()
            fwd_copy(arr).start()
        for arr in arrays:
            fwd_copy(arr).wait_recv()
            if arr < 3:
                transpose_half(arr, 1 - chip)

    def part_copy(slot, arr):
        tile = 2 * slot + 1 - core
        at = num_tiles - 1 - tile if arr == 2 else tile
        return to_device(acc_ref.at[arr, :, cols(at)], part_ref.at[slot, arr],
                         part_send.at[slot, arr], part_recv.at[slot, arr], core_peer)

    def start_parts(slot, arrays):
        for arr in arrays:
            part_copy(slot, arr).start()

    def deliver(tile, stage, part, send_sem, start):
        owner = lax.div(tile, block_tiles)
        local = tile - owner * block_tiles
        if part == 2:
            own_dst, got_dst = res_rel_ref.at[0, pl.ds(local, 1)], res_rel_ref.at[1, pl.ds(local, 1)]
        else:
            own_dst, got_dst = res_own_ref.at[local, PARTS[part]], res_got_ref.at[local, PARTS[part]]

        @pl.when(owner == dev)
        def _():
            if start:
                pltpu.make_async_copy(stage, own_dst, res_sems.at[0, part, local]).start()

        @pl.when(owner == core_peer)
        def _():
            copy = to_device(stage, own_dst, send_sem, res_sems.at[0, part, local], owner)
            copy.start() if start else copy.wait_send()

        @pl.when(lax.div(owner, 2) != chip)
        def _():
            copy = to_device(stage, got_dst, send_sem, res_sems.at[1, part, local], owner)
            copy.start() if start else copy.wait_send()

    def finish_keys(slot):
        tile = 2 * slot + core
        for arr in range(2):
            part_copy(slot, arr).wait_recv()
        d_key = (acc_ref[0, :, cols(tile)] + part_ref[slot, 0]) * inv_sqrt
        st_grad_ref[slot, 0] = d_key.astype(BF16).T
        d_val = acc_ref[1, :, cols(tile)] + part_ref[slot, 1]
        st_grad_ref[slot, 1] = d_val.astype(BF16).T
        deliver(tile, st_grad_ref.at[slot, pl.ds(0, 2)], 1, grad_send.at[slot, 0], True)

    def finish_offsets(slot):
        tile = 2 * slot + core
        part_copy(slot, 2).wait_recv()
        d_off = ((acc_ref[2, :, cols(num_tiles - 1 - tile)] + part_ref[slot, 2]) * inv_sqrt).astype(BF16)
        flip_rows = exchange_matrix()
        for chunk in range(NSUB):
            back = lax.dot_general(flip_rows, d_off[:, sub(chunk)], (((1,), (1,)), ((), ())), preferred_element_type=F32)
            st_grad_ref[slot, 2, sub(NSUB - 1 - chunk)] = back.astype(BF16)
        deliver(tile, st_grad_ref.at[slot, pl.ds(2, 1)], 2, grad_send.at[slot, 1], True)

    top_tile = 2 * pair_at(last) + 1
    top_pair = pair_at(last)

    def finish_all():
        model_dim = table_ref.shape[1]
        half = model_dim // 2
        quarter = half // 2
        size = quarter + 8

        def piece(which, src):
            return rot_ref.at[which, pl.ds(0, size), pl.ds(src * 256, 256)]

        def total_piece(src):
            return rot_ref.at[2, pl.ds(0, size), pl.ds(src * 256, 256)]

        def wait_res(which, part):
            for local in range(block_tiles):
                if part == 2:
                    dst = res_rel_ref.at[which, pl.ds(local, 1)]
                else:
                    dst = (res_own_ref, res_got_ref)[which].at[local, PARTS[part]]
                pltpu.make_async_copy(dst, dst, res_sems.at[which, part, local]).wait()

        def partial(which, src):
            d_rel = jnp.concatenate([res_rel_ref[src, tile] for tile in range(block_tiles)], axis=0)
            for side in range(2):
                at = pl.ds(pl.multiple_of(which * half + side * quarter, 256), quarter)
                piece(which, src)[pl.ds(0, quarter), sub(side)] = lax.dot_general(
                    table_ref[:, at], d_rel, (((0,), (0,)), ((), ())), preferred_element_type=F32)
            bias = bias_ref[...] if src == 0 else jnp.zeros(bias_ref.shape, F32)
            rows = jnp.concatenate([bias, jnp.zeros((6, SUB), F32)], axis=0)
            piece(which, src)[pl.ds(quarter, 8), :] = jnp.concatenate([rows, rows], axis=1)

        def swap(src, dst, send_idx, recv_idx, peer):
            copy = to_device(src, dst, sum_send.at[send_idx], sum_recv.at[recv_idx], peer)
            copy.start()
            return copy

        first, second, third = [], [], []
        for src in range(2):
            wait_res(src, 2)
            partial(1 - core, src)
            first.append(swap(piece(1 - core, src), core_ref.at[src], src, src, core_peer))
            partial(core, src)
            first[src].wait()
            total_piece(src)[...] = piece(core, src)[...] + core_ref[src]
            second.append(swap(total_piece(src), chip_ref.at[1 - src], 2 + src, 3 - src, chip_peer))
        for part in range(2):
            wait_res(0, part)
            wait_res(1, part)
        loads = []
        for tile in range(block_tiles):
            for which, res in enumerate((res_own_ref, res_got_ref)):
                dst = full_ref.at[pl.ds(0, 4), pl.ds((which * block_tiles + tile) * TILE, TILE)]
                loads.append(pltpu.make_async_copy(res.at[tile], dst, load_sems.at[tile, which]))
        for load in loads:
            load.start()
        for tile in range(block_tiles):
            loads[2 * tile].wait()
            loads[2 * tile + 1].wait()
            rows = slice(tile * TILE, (tile + 1) * TILE)
            for arr in range(4):
                own = full_ref[arr, rows]
                got = full_ref[arr, (block_tiles + tile) * TILE:(block_tiles + tile + 1) * TILE]
                raw_ref[arr, rows] = jnp.stack([jnp.where(chip == 0, own, got), jnp.where(chip == 0, got, own)], axis=1)
        stores = [pltpu.make_async_copy(raw_ref.at[arr], dst, local_sems.at[arr])
                  for arr, dst in enumerate((o_ref, dq_ref, dk_out_ref, dv_out_ref))]
        for store in stores:
            store.start()
        stores_rows, stores = stores, []

        def put(which):
            own, got = final_ref.at[which, 0], final_ref.at[which, 1]
            for side in range(2):
                own_part, got_part = own[pl.ds(0, quarter), sub(side)], got[pl.ds(0, quarter), sub(side)]
                at = pl.ds(pl.multiple_of(which * half + side * quarter, 256), quarter)
                stage = dw_stage_ref.at[pl.ds(side * quarter, quarter)]
                stage[...] = jnp.stack([jnp.where(chip == 0, own_part, got_part), jnp.where(chip == 0, got_part, own_part)], axis=1)
                store = pltpu.make_async_copy(stage, dw_out_ref.at[at], out_sems.at[len(stores)])
                store.start()
                stores.append(store)

        for src in (1, 0):
            second[src].wait_send()
            to_device(total_piece(src), chip_ref.at[src], sum_send.at[2 + src], sum_recv.at[2 + src], chip_peer).wait_recv()
            final_ref[core, src] = total_piece(src)[...] + chip_ref[src]
            third.append(swap(final_ref.at[core, src], final_ref.at[core, src], 4 + src, 4 + src, core_peer))
        put(core)
        third[0].wait()
        third[1].wait()
        for store in stores:
            store.wait()
        stores.clear()
        put(1 - core)
        own, got = final_ref[0, 0, quarter:, :SUB], final_ref[0, 1, quarter:, :SUB]
        head0, head1 = jnp.where(chip == 0, own, got), jnp.where(chip == 0, got, own)
        du_ref[...] = jnp.concatenate([head0[0:1], head1[0:1]], axis=0)
        dvb_ref[...] = jnp.concatenate([head0[1:2], head1[1:2]], axis=0)
        for store in stores + stores_rows:
            store.wait()

    def put_heads(arr, start, size, first, second):
        at = 3 - dev if arr == 2 else dev
        own_at = pl.ds(pl.multiple_of(at * block_len + start, SUB), size)
        away_at = pl.ds(pl.multiple_of(start, SUB), size)
        full_ref[arr, own_at] = jnp.where(chip == 0, first, second)
        away_ref[arr, away_at] = jnp.where(chip == 0, second, first)

    def pack_seq(arr, src):
        def body(idx, _):
            heads = jnp.swapaxes(raw_ref[src, cols(idx)], 0, 1)
            put_heads(arr, idx * TILE, TILE, heads[0], heads[1])
            return 0
        lax.fori_loop(0, block_tiles, body, 0)

    def pack_rel():
        weights = jnp.swapaxes(w_ref[...], 0, 1)
        wide_ref[:, :SUB] = weights[0]
        wide_ref[:, SUB:] = weights[1]

        def body(idx, _):
            rel = dot(table_ref[cols(idx), :], wide_ref[...]).astype(BF16)
            flip_rows = exchange_matrix()
            for chunk in range(NSUB):
                back = dot(flip_rows, rel[sub(NSUB - 1 - chunk)]).astype(BF16)
                put_heads(2, (block_tiles - 1 - idx) * TILE + chunk * SUB, SUB, back[:, :SUB], back[:, SUB:])
            return 0
        lax.fori_loop(0, block_tiles, body, 0)

    @pl.when(step == 0)
    def _():
        barrier = pltpu.get_barrier_semaphore()
        for peer in (core_peer, chip_peer, 3 - dev):
            pl.semaphore_signal(barrier, inc=1, device_id={'cp': peer}, device_id_type=pl.DeviceIdType.MESH)
        loads = [pltpu.make_async_copy(src, dst, local_sems.at[idx]) for idx, (src, dst) in enumerate((
            (kin_ref, raw_ref.at[0]), (w_in_ref, w_ref), (table_in_ref, table_ref),
            (vin_ref, raw_ref.at[1]), (qin_ref, raw_ref.at[2]), (doin_ref, raw_ref.at[3])))]
        loads[0].start()

        def clear(tile, _):
            acc_ref[:, :, cols(tile)] = jnp.zeros((3, SUB, TILE), F32)
            return 0

        def ship(arr):
            cross_copy(arr).start()
            own_copy(arr).start()

        loads[0].wait()
        for load in loads[1:]:
            load.start()
        pack_seq(0, 0)
        pl.semaphore_wait(barrier, 3)
        ship(0)
        loads[1].wait()
        loads[2].wait()
        pack_rel()
        ship(2)
        def load_and_ship(arr):
            idx = (1, 3, 4).index(arr)
            loads[3 + idx].wait()
            pack_seq(arr, idx + 1)
            ship(arr)

        @pl.when(chip == 0)
        def _():
            load_and_ship(1)
        load_and_ship(3)

        @pl.when(chip == 1)
        def _():
            load_and_ship(1)
        load_and_ship(4)
        lax.fori_loop(0, num_tiles, clear, 0)
        bias_ref[...] = jnp.zeros_like(bias_ref)
        for arr in (0, 2, 1, 3, 4):
            own_copy(arr).wait_recv()
            if arr < 3:
                transpose_half(arr, chip)

    @pl.when(step == half_steps * (1 - chip))
    def _():
        arrive((0, 2))

    @pl.when(step == half_steps - chip)
    def _():
        arrive((3,))

    rows_at = cols(blk)
    q_wide = q_ref[rows_at, :].astype(F32)
    q_u = (q_wide + u_ref[pl.ds(chip, 1), :]).astype(BF16)
    q_v = (q_wide + v_ref[pl.ds(chip, 1), :]).astype(BF16)
    qu_ref[...] = q_u
    qv_ref[...] = q_v
    qut_ref[...] = q_u.T
    qvt_ref[...] = q_v.T
    max_ref[...] = jnp.full_like(max_ref, -jnp.inf)
    sum_ref[...] = jnp.zeros_like(sum_ref)
    gu_ref[...] = jnp.zeros_like(gu_ref)
    gv_ref[...] = jnp.zeros_like(gv_ref)
    lane = lax.broadcasted_iota(jnp.int32, (SUB, SUB), 1)
    row = lax.broadcasted_iota(jnp.int32, (SUB, SUB), 0)
    upper = lane > row
    flip = 7 - lax.broadcasted_iota(jnp.int32, (8, SUB), 0)
    lower = lane + row < SUB - 1
    first_rel = num_tiles - 1 - blk

    def rotate_rel(tile, slot):
        for half in range(2):
            start = pl.multiple_of(tile * TILE + half * 256, 256)
            for a in range(NSUB):
                if a % MROWS == 0:
                    by_offset = dot(qv_ref[a * SUB:(a + MROWS) * SUB, :], relt_ref[:, pl.ds(start, 256)])
                for c in range(2):
                    part = by_offset[sub(a % MROWS), sub(c)]
                    rot_ref[slot, sub(a), sub(half * 2 + c)] = pltpu.roll(part, 1, 1, stride=1, stride_axis=0)

    rotate_rel(first_rel, 0)
    rotate_rel(jnp.minimum(first_rel + 1, num_tiles - 1), 1)

    def score_tile(tile, diag):
        left = lax.rem(tile, 3)
        right = lax.rem(tile + 1, 3)
        for half in range(2):
            start = pl.multiple_of(tile * TILE + half * 256, 256)
            for a in range(NSUB):
                if a % MROWS == 0:
                    content = dot(qu_ref[a * SUB:(a + MROWS) * SUB, :], kt_ref[:, pl.ds(start, 256)])
                run_max = max_ref[sub(a), :]
                for c2 in range(2):
                    c = half * 2 + c2
                    hi, lo = c - a + NSUB, c - a + NSUB - 1
                    if diag and c > a:
                        score = jnp.full((SUB, SUB), -jnp.inf, F32)
                    else:
                        low_part = rot_ref[left if lo < NSUB else right, sub(a), sub(lo % NSUB)]
                        if diag and c == a:
                            score = jnp.where(upper, -jnp.inf, (content[sub(a % MROWS), sub(c2)] + low_part) * scale)
                        else:
                            high_part = rot_ref[left if hi < NSUB else right, sub(a), sub(hi % NSUB)]
                            score = (content[sub(a % MROWS), sub(c2)] + jnp.where(upper, high_part, low_part)) * scale
                    run_max = jnp.maximum(run_max, score)
                    sc_ref[sub(a), pl.ds(pl.multiple_of(tile * TILE + c * SUB, SUB), SUB)] = score
                max_ref[sub(a), :] = run_max
        if not diag:
            rotate_rel(jnp.minimum(first_rel + tile + 2, num_tiles - 1), lax.rem(tile + 2, 3))

    def score_body(tile, _):
        score_tile(tile, False)
        return 0

    lax.fori_loop(0, blk, score_body, 0)
    score_tile(blk, True)
    max_ref[...] = jnp.broadcast_to(jnp.max(max_ref[...], axis=1, keepdims=True), (TILE, SUB))

    @pl.when(step == half_steps * (1 - chip))
    def _():
        arrive((1,))

    def prob_tile(tile, diag):
        for top in range(0, NSUB, 2):
            rows = slice(top * SUB, (top + 2) * SUB)
            width = top + 2 if diag else NSUB
            prob_rows = []
            for a in range(top, top + 2):
                run_sum = sum_ref[sub(a), :]
                row_max = max_ref[sub(a), :]
                prob_cols = []
                for c in range(width):
                    if diag and c > a:
                        prob_cols.append(jnp.zeros((SUB, SUB), BF16))
                        continue
                    where = pl.ds(pl.multiple_of(tile * TILE + c * SUB, SUB), SUB)
                    prob = jnp.exp2(sc_ref[sub(a), where] - row_max)
                    prob_cols.append(prob.astype(BF16))
                    run_sum = run_sum + prob
                sum_ref[sub(a), :] = run_sum
                prob_rows.append(jnp.concatenate(prob_cols, axis=1))
            keys = pl.ds(pl.multiple_of(tile * TILE, TILE), width * SUB)
            gu_ref[rows, :] += dot(jnp.concatenate(prob_rows, axis=0), val_ref[keys, :])

    def prob_body(tile, _):
        prob_tile(tile, False)
        return 0

    lax.fori_loop(0, blk, prob_body, 0)
    prob_tile(blk, True)

    @pl.when(step == half_steps - chip)
    def _():
        arrive((4,))

    dot_ref[...] = do_ref[rows_at, :].T
    total = jnp.sum(sum_ref[...], axis=1, keepdims=True)
    inv_sum = 1.0 / total
    out = gu_ref[...] * inv_sum
    st_rows_ref[step, 0] = out.astype(BF16)
    delta = jnp.sum(out * do_ref[rows_at, :].astype(F32), axis=1, keepdims=True)
    row_ref[...] = jnp.broadcast_to(delta, (TILE, SUB))
    sum_ref[...] = max_ref[...] + jnp.log2(total)
    gu_ref[...] = jnp.zeros_like(gu_ref)
    ds_ref[1, :, :] = jnp.zeros((TILE, TILE), F32)

    def grad_tile(tile, diag):
        now = lax.rem(tile, 2)
        old = 1 - now
        for half in range(2):
            start = pl.multiple_of(tile * TILE + half * 256, 256)
            win = pl.ds(start, 256)
            d_val = d_key = None
            for top in range(0, NSUB, 2):
                if diag and 2 * half > top:
                    continue
                rows = slice(top * SUB, (top + 2) * SUB)
                do_rows = pl.ds(pl.multiple_of(blk * TILE + top * SUB, SUB), 2 * SUB)
                d_prob = dot(do_ref[do_rows, :], valt_ref[:, win])
                prob_rows, score_rows = [], []
                for a in range(top, top + 2):
                    log_norm = sum_ref[sub(a), :]
                    shift = row_ref[sub(a), :]
                    prob_cols, score_cols = [], []
                    for c2 in range(2):
                        c = half * 2 + c2
                        if diag and c > a:
                            prob_cols.append(jnp.zeros((SUB, SUB), BF16))
                            score_cols.append(jnp.zeros((SUB, SUB), BF16))
                            continue
                        prob = jnp.exp2(sc_ref[sub(a), pl.ds(pl.multiple_of(tile * TILE + c * SUB, SUB), SUB)] - log_norm)
                        d_score = prob * (d_prob[sub(a - top), sub(c2)] - shift)
                        ds_ref[now, sub(a), sub(c)] = roll_left(d_score, flip)
                        prob_cols.append(prob.astype(BF16))
                        score_cols.append(d_score.astype(BF16))
                    prob_rows.append(jnp.concatenate(prob_cols, axis=1))
                    score_rows.append(jnp.concatenate(score_cols, axis=1))
                probs = jnp.concatenate(prob_rows, axis=0)
                scores = jnp.concatenate(score_rows, axis=0)
                more_val, more_key = dot(dot_ref[:, rows], probs), dot(qut_ref[:, rows], scores)
                d_val = more_val if d_val is None else d_val + more_val
                d_key = more_key if d_key is None else d_key + more_key
                gu_ref[rows, :] += dot(scores, k_ref[win, :])
            dv_ref[:, win] += d_val
            dk_ref[:, win] += d_key
        rel_tile = first_rel + tile
        d_off = [None, None]
        for top in range(0, NSUB, 2):
            rows = slice(top * SUB, (top + 2) * SUB)
            wide_rows = []
            for a in range(top, top + 2):
                wide_cols = []
                for y in range(NSUB):
                    c_lo = y + a - NSUB
                    c_hi = c_lo + 1
                    lo_part = ds_ref[now if c_lo >= 0 else old, sub(a), sub(c_lo % NSUB)]
                    hi_part = ds_ref[now if c_hi >= 0 else old, sub(a), sub(c_hi % NSUB)]
                    wide_cols.append(jnp.where(lower, lo_part, hi_part).astype(BF16))
                wide_rows.append(jnp.concatenate(wide_cols, axis=1))
            by_off = jnp.concatenate(wide_rows, axis=0)
            gv_ref[rows, :] += dot(by_off, rel_ref[cols(rel_tile), :])
            for half in range(2):
                more = dot(qvt_ref[:, rows], by_off[:, half * 256:half * 256 + 256])
                d_off[half] = more if d_off[half] is None else d_off[half] + more
        for half in range(2):
            start = pl.multiple_of(rel_tile * TILE + half * 256, 256)
            drel_ref[:, pl.ds(start, 256)] += d_off[half]

    def grad_body(tile, _):
        grad_tile(tile, False)

        @pl.when((step == last) & (lax.rem(tile, 2) == 1) & (tile < top_tile))
        def _():
            key_pair = lax.div(tile, 2)
            off_pair = lax.div(top_tile - tile, 2)
            start_parts(off_pair, (2,))
            start_parts(key_pair, (0, 1))

            @pl.when(key_pair > 0)
            def _():
                finish_offsets(off_pair + 1)
                finish_keys(key_pair - 1)
        return 0

    @pl.when((step > half_steps) & (chip == 0))
    def _():
        finish_offsets(pair_at(step - 1))
        finish_keys(pair_at(step - 1))

    lax.fori_loop(0, blk, grad_body, 0)
    grad_tile(blk, True)
    grad_u = gu_ref[...] * inv_sqrt
    grad_v = gv_ref[...] * inv_sqrt
    st_rows_ref[step, 1] = (grad_u + grad_v).astype(BF16)
    bias_ref[0:1, :] += jnp.sum(grad_u, axis=0, keepdims=True)
    bias_ref[1:2, :] += jnp.sum(grad_v, axis=0, keepdims=True)
    deliver(blk, st_rows_ref.at[step], 0, rows_send.at[step], True)

    @pl.when((step >= half_steps) & (step < last) & (chip == 0))
    def _():
        start_parts(pair_at(step), (2, 0, 1))

    @pl.when(step == last)
    def _():
        start_parts(0, (2,))
        start_parts(top_pair, (0, 1))

        def finish_rest(idx, _):
            finish_offsets(1 - idx)
            finish_keys(top_pair - 1 + idx)
            return 0

        def drain(idx, _):
            for arr in range(3):
                part_copy(idx, arr).wait_send()
            tile = 2 * idx + core
            deliver(tile, st_grad_ref.at[idx, pl.ds(0, 2)], 1, grad_send.at[idx, 0], False)
            deliver(tile, st_grad_ref.at[idx, pl.ds(2, 1)], 2, grad_send.at[idx, 1], False)
            deliver(block_at(idx), st_rows_ref.at[idx], 0, rows_send.at[idx], False)
            return 0

        lax.fori_loop(0, 2, finish_rest, 0)
        for arr in range(5):
            own_copy(arr).wait_send()
            cross_copy(arr).wait_send()
            fwd_copy(arr).wait_send()
        finish_all()
        lax.fori_loop(0, 2 * half_steps, drain, 0)


def run_attn(u_bias, v_bias, k, v, q, d_out, rel_table, w_rel):
    block_len, _, head_dim = k.shape
    seq_len = 4 * block_len
    num_tiles = seq_len // TILE
    steps = num_tiles // 2
    block_tiles = block_len // TILE
    vec = pl.BlockSpec(memory_space=pltpu.VMEM)
    hbm = pl.BlockSpec(memory_space=pl.ANY)
    result = jax.ShapeDtypeStruct((block_tiles, 4, TILE, head_dim), BF16)
    seq = jax.ShapeDtypeStruct(k.shape, BF16)
    bias = jax.ShapeDtypeStruct((2, head_dim), F32)
    d_weights = jax.ShapeDtypeStruct(w_rel.shape, F32)
    size = w_rel.shape[0] // 4 + 8
    dma = pltpu.SemaphoreType.DMA
    return pl.pallas_call(
        functools.partial(attn_kernel, num_tiles, head_dim ** -0.5),
        grid=(steps,),
        in_specs=[vec, vec] + [hbm] * 6,
        out_specs=[hbm] * 5 + [vec, vec, hbm, hbm],
        scratch_shapes=[
            pltpu.VMEM((5, seq_len, head_dim), BF16),
            pltpu.VMEM((3, head_dim, seq_len), F32),
            pltpu.VMEM((head_dim, seq_len), BF16),
            pltpu.VMEM((head_dim, seq_len), BF16),
            pltpu.VMEM((head_dim, seq_len), BF16),
            pltpu.VMEM((TILE, seq_len), F32),
            pltpu.VMEM((3, TILE, TILE), F32),
            pltpu.VMEM((2, TILE, TILE), F32),
            pltpu.VMEM((TILE, head_dim), BF16),
            pltpu.VMEM((TILE, head_dim), BF16),
            pltpu.VMEM((head_dim, TILE), BF16),
            pltpu.VMEM((head_dim, TILE), BF16),
            pltpu.VMEM((head_dim, TILE), BF16),
            pltpu.VMEM((TILE, SUB), F32),
            pltpu.VMEM((TILE, SUB), F32),
            pltpu.VMEM((TILE, head_dim), F32),
            pltpu.VMEM((TILE, head_dim), F32),
            pltpu.VMEM((TILE, SUB), F32),
            pltpu.VMEM((steps, 2, TILE, head_dim), BF16),
            pltpu.VMEM((steps, 3, TILE, head_dim), BF16),
            pltpu.VMEM((steps, 3, head_dim, TILE), F32),
            pltpu.VMEM((5, block_len, head_dim), BF16),
            pltpu.VMEM((4,) + k.shape, BF16),
            pltpu.VMEM(rel_table.shape, BF16),
            pltpu.VMEM(w_rel.shape, BF16),
            pltpu.VMEM((w_rel.shape[0], 2 * head_dim), BF16),
            pltpu.VMEM((2, head_dim), F32),
            pltpu.VMEM((2, block_tiles, TILE, head_dim), BF16),
            pltpu.VMEM((2, size, 2 * head_dim), F32),
            pltpu.VMEM((2, size, 2 * head_dim), F32),
            pltpu.VMEM((2, 2, size, 2 * head_dim), F32),
            pltpu.VMEM((w_rel.shape[0] // 2,) + w_rel.shape[1:], F32),
            dma((6,)), dma((6,)),
            dma((6,)), dma((5,)), dma((5,)), dma((5,)), dma((5,)), dma((5,)), dma((5,)),
            dma((steps, 3)), dma((steps, 3)), dma((steps,)), dma((steps, 2)), dma((2, 3, block_tiles)), dma((block_tiles, 2)), dma((2,)),
        ],
        out_shape=[seq, seq, seq, seq, d_weights, bias, bias, result, result],
        compiler_params=pltpu.CompilerParams(
            dimension_semantics=("arbitrary",), vmem_limit_bytes=67043328, collective_id=0, has_side_effects=True),
        name="attn_rows",
    )(u_bias, v_bias, k, v, q, d_out, rel_table, w_rel)


def exchange_matrix():
    row = lax.broadcasted_iota(jnp.int32, (SUB, SUB), 0)
    col = lax.broadcasted_iota(jnp.int32, (SUB, SUB), 1)
    return jnp.where(row + col == SUB - 1, 1.0, 0.0).astype(BF16)


def solution(mesh):
    seq_spec = P('cp', 'hp', None)
    head_spec = P('hp', None)
    weight_spec = P(None, 'hp', None)

    def local_fn(q, k, v, u_bias, v_bias, rel_table, w_rel, d_out):
        out, dq, dk, dv, d_w_rel, d_u, d_v, _, _ = run_attn(u_bias, v_bias, k, v, q, d_out, rel_table, w_rel)
        return out, dq, dk, dv, d_u, d_v, d_w_rel

    return jax.shard_map(
        local_fn,
        mesh=mesh,
        in_specs=(seq_spec, seq_spec, seq_spec, head_spec, head_spec, P('cp', None), weight_spec, seq_spec),
        out_specs=(seq_spec, seq_spec, seq_spec, seq_spec, head_spec, head_spec, weight_spec),
        check_vma=False,
    )
```

```python
import functools

import jax
import jax.numpy as jnp
from jax import lax
from jax.experimental import pallas as pl
from jax.experimental.pallas import tpu as pltpu
from jax.sharding import PartitionSpec as P

TILE = 512
SUB = 128
NSUB = TILE // SUB
MROWS = 2
PARTS = (pl.ds(0, 2), pl.ds(2, 2), pl.ds(4, 1))
LOG2E = 1.4426950408889634
F32 = jnp.float32
BF16 = jnp.bfloat16


def dot(lhs, rhs):
    return jnp.dot(lhs, rhs, preferred_element_type=F32)


def sub(idx):
    return slice(idx * SUB, (idx + 1) * SUB)


def roll_left(part, flip):
    groups = []
    for start in range(0, SUB, 8):
        rows = jnp.take_along_axis(part[start:start + 8], flip, axis=0)
        rows = pltpu.roll(rows, (SUB - 8 - start) % SUB, 1, stride=1, stride_axis=0)
        groups.append(jnp.take_along_axis(rows, flip, axis=0))
    return jnp.concatenate(groups, axis=0)


def attn_kernel(num_tiles, inv_sqrt, u_ref, v_ref, kin_ref, vin_ref, qin_ref, doin_ref, table_in_ref, w_in_ref,
                o_ref, dq_ref, dk_out_ref, dv_out_ref, dw_out_ref, du_ref, dvb_ref, res_own_ref, res_got_ref,
                full_ref, acc_ref, kt_ref, valt_ref, relt_ref, sc_ref, rot_ref, ds_ref,
                qu_ref, qv_ref, qut_ref, qvt_ref, dot_ref, max_ref, sum_ref, gu_ref, gv_ref, row_ref,
                st_rows_ref, st_grad_ref, part_ref, away_ref, raw_ref, table_ref, w_ref, wide_ref, bias_ref, res_rel_ref,
                core_ref, chip_ref, final_ref, dw_stage_ref, sum_send, sum_recv,
                local_sems, own_send, own_recv, cross_send, cross_recv, fwd_send, fwd_recv,
                part_send, part_recv, rows_send, grad_send, res_sems, load_sems, out_sems):
    step = pl.program_id(0)
    last = pl.num_programs(0) - 1
    dev = lax.axis_index('cp')
    chip, core = lax.div(dev, 2), lax.rem(dev, 2)
    core_peer, chip_peer = dev + 1 - 2 * core, dev + 2 - 4 * chip
    half_steps = num_tiles // 4

    def pair_at(idx):
        first = jnp.where(idx < half_steps, idx, 3 * half_steps - 1 - idx)
        second = jnp.where(idx < half_steps - 1, idx + half_steps, 2 * half_steps - 2 - idx)
        second = jnp.where(idx == last, last, second)
        return jnp.where(chip == 0, first, second)

    def block_at(idx):
        odd = lax.rem(pair_at(idx), 2)
        return 2 * pair_at(idx) + odd + core - 2 * odd * core

    blk = block_at(step)
    scale = inv_sqrt * LOG2E
    block_len = away_ref.shape[1]
    block_tiles = block_len // TILE
    k_ref, val_ref, rel_ref = full_ref.at[0], full_ref.at[1], full_ref.at[2]
    q_ref, do_ref = full_ref.at[3], full_ref.at[4]
    dk_ref, dv_ref, drel_ref = acc_ref.at[0], acc_ref.at[1], acc_ref.at[2]

    def cols(tile):
        return pl.ds(pl.multiple_of(tile * TILE, TILE), TILE)

    def place(arr, block):
        at = 3 - block if arr == 2 else block
        return full_ref.at[arr, pl.ds(pl.multiple_of(at * block_len, block_len), block_len)]

    def to_device(src, dst, send_sem, recv_sem, peer):
        return pltpu.make_async_remote_copy(
            src_ref=src, dst_ref=dst, send_sem=send_sem, recv_sem=recv_sem,
            device_id={'cp': peer}, device_id_type=pl.DeviceIdType.MESH)

    def own_copy(arr):
        return to_device(place(arr, dev), place(arr, dev), own_send.at[arr], own_recv.at[arr], core_peer)

    def cross_copy(arr):
        return to_device(away_ref.at[arr], place(arr, dev), cross_send.at[arr], cross_recv.at[arr], chip_peer)

    def fwd_copy(arr):
        return to_device(place(arr, chip_peer), place(arr, chip_peer), fwd_send.at[arr], fwd_recv.at[arr], core_peer)

    def transpose_half(arr, which):
        dst = (kt_ref, valt_ref, relt_ref)[arr]
        first = (1 - which if arr == 2 else which) * (num_tiles // 2)

        def body(idx, _):
            dst[:, cols(first + idx)] = full_ref[arr, cols(first + idx), :].T
            return 0
        lax.fori_loop(0, num_tiles // 2, body, 0)

    def arrive(arrays):
        for arr in arrays:
            cross_copy(arr).wait_recv()
            fwd_copy(arr).start()
            fwd_copy(arr).wait_recv()
            if arr < 3:
                transpose_half(arr, 1 - chip)

    def part_copy(slot, arr):
        tile = 2 * slot + 1 - core
        at = num_tiles - 1 - tile if arr == 2 else tile
        return to_device(acc_ref.at[arr, :, cols(at)], part_ref.at[slot, arr],
                         part_send.at[slot, arr], part_recv.at[slot, arr], core_peer)

    def start_parts(slot, arrays):
        for arr in arrays:
            part_copy(slot, arr).start()

    def deliver(tile, stage, part, send_sem, start):
        owner = lax.div(tile, block_tiles)
        local = tile - owner * block_tiles
        if part == 2:
            own_dst, got_dst = res_rel_ref.at[0, pl.ds(local, 1)], res_rel_ref.at[1, pl.ds(local, 1)]
        else:
            own_dst, got_dst = res_own_ref.at[local, PARTS[part]], res_got_ref.at[local, PARTS[part]]

        @pl.when(owner == dev)
        def _():
            if start:
                pltpu.make_async_copy(stage, own_dst, res_sems.at[0, part, local]).start()

        @pl.when(owner == core_peer)
        def _():
            copy = to_device(stage, own_dst, send_sem, res_sems.at[0, part, local], owner)
            copy.start() if start else copy.wait_send()

        @pl.when(lax.div(owner, 2) != chip)
        def _():
            copy = to_device(stage, got_dst, send_sem, res_sems.at[1, part, local], owner)
            copy.start() if start else copy.wait_send()

    def finish_keys(slot):
        tile = 2 * slot + core
        for arr in range(2):
            part_copy(slot, arr).wait_recv()
        d_key = (acc_ref[0, :, cols(tile)] + part_ref[slot, 0]) * inv_sqrt
        st_grad_ref[slot, 0] = d_key.astype(BF16).T
        d_val = acc_ref[1, :, cols(tile)] + part_ref[slot, 1]
        st_grad_ref[slot, 1] = d_val.astype(BF16).T
        deliver(tile, st_grad_ref.at[slot, pl.ds(0, 2)], 1, grad_send.at[slot, 0], True)

    def finish_offsets(slot):
        tile = 2 * slot + core
        part_copy(slot, 2).wait_recv()
        d_off = ((acc_ref[2, :, cols(num_tiles - 1 - tile)] + part_ref[slot, 2]) * inv_sqrt).astype(BF16)
        flip_rows = exchange_matrix()
        for chunk in range(NSUB):
            back = lax.dot_general(flip_rows, d_off[:, sub(chunk)], (((1,), (1,)), ((), ())), preferred_element_type=F32)
            st_grad_ref[slot, 2, sub(NSUB - 1 - chunk)] = back.astype(BF16)
        deliver(tile, st_grad_ref.at[slot, pl.ds(2, 1)], 2, grad_send.at[slot, 1], True)

    top_tile = 2 * pair_at(last) + 1
    top_pair = pair_at(last)

    def finish_all():
        model_dim = table_ref.shape[1]
        half = model_dim // 2
        quarter = half // 2
        size = quarter + 8

        def piece(which, src):
            return rot_ref.at[which, pl.ds(0, size), pl.ds(src * 256, 256)]

        def total_piece(src):
            return rot_ref.at[2, pl.ds(0, size), pl.ds(src * 256, 256)]

        def wait_res(which, part):
            for local in range(block_tiles):
                if part == 2:
                    dst = res_rel_ref.at[which, pl.ds(local, 1)]
                else:
                    dst = (res_own_ref, res_got_ref)[which].at[local, PARTS[part]]
                pltpu.make_async_copy(dst, dst, res_sems.at[which, part, local]).wait()

        def partial(which, src):
            d_rel = jnp.concatenate([res_rel_ref[src, tile] for tile in range(block_tiles)], axis=0)
            for side in range(2):
                at = pl.ds(pl.multiple_of(which * half + side * quarter, 256), quarter)
                piece(which, src)[pl.ds(0, quarter), sub(side)] = lax.dot_general(
                    table_ref[:, at], d_rel, (((0,), (0,)), ((), ())), preferred_element_type=F32)
            bias = bias_ref[...] if src == 0 else jnp.zeros(bias_ref.shape, F32)
            rows = jnp.concatenate([bias, jnp.zeros((6, SUB), F32)], axis=0)
            piece(which, src)[pl.ds(quarter, 8), :] = jnp.concatenate([rows, rows], axis=1)

        def swap(src, dst, send_idx, recv_idx, peer):
            copy = to_device(src, dst, sum_send.at[send_idx], sum_recv.at[recv_idx], peer)
            copy.start()
            return copy

        first, second, third = [], [], []
        for src in range(2):
            wait_res(src, 2)
            partial(1 - core, src)
            first.append(swap(piece(1 - core, src), core_ref.at[src], src, src, core_peer))
            partial(core, src)
            first[src].wait()
            total_piece(src)[...] = piece(core, src)[...] + core_ref[src]
            second.append(swap(total_piece(src), chip_ref.at[1 - src], 2 + src, 3 - src, chip_peer))
        for part in range(2):
            wait_res(0, part)
            wait_res(1, part)
        loads = []
        for tile in range(block_tiles):
            for which, res in enumerate((res_own_ref, res_got_ref)):
                dst = full_ref.at[pl.ds(0, 4), pl.ds((which * block_tiles + tile) * TILE, TILE)]
                loads.append(pltpu.make_async_copy(res.at[tile], dst, load_sems.at[tile, which]))
        for load in loads:
            load.start()
        for tile in range(block_tiles):
            loads[2 * tile].wait()
            loads[2 * tile + 1].wait()
            rows = slice(tile * TILE, (tile + 1) * TILE)
            for arr in range(4):
                own = full_ref[arr, rows]
                got = full_ref[arr, (block_tiles + tile) * TILE:(block_tiles + tile + 1) * TILE]
                raw_ref[arr, rows] = jnp.stack([jnp.where(chip == 0, own, got), jnp.where(chip == 0, got, own)], axis=1)
        stores = [pltpu.make_async_copy(raw_ref.at[arr], dst, local_sems.at[arr])
                  for arr, dst in enumerate((o_ref, dq_ref, dk_out_ref, dv_out_ref))]
        for store in stores:
            store.start()
        stores_rows, stores = stores, []

        def put(which):
            own, got = final_ref.at[which, 0], final_ref.at[which, 1]
            for side in range(2):
                own_part, got_part = own[pl.ds(0, quarter), sub(side)], got[pl.ds(0, quarter), sub(side)]
                at = pl.ds(pl.multiple_of(which * half + side * quarter, 256), quarter)
                stage = dw_stage_ref.at[pl.ds(side * quarter, quarter)]
                stage[...] = jnp.stack([jnp.where(chip == 0, own_part, got_part), jnp.where(chip == 0, got_part, own_part)], axis=1)
                store = pltpu.make_async_copy(stage, dw_out_ref.at[at], out_sems.at[len(stores)])
                store.start()
                stores.append(store)

        for src in (1, 0):
            second[src].wait_send()
            to_device(total_piece(src), chip_ref.at[src], sum_send.at[2 + src], sum_recv.at[2 + src], chip_peer).wait_recv()
            final_ref[core, src] = total_piece(src)[...] + chip_ref[src]
            third.append(swap(final_ref.at[core, src], final_ref.at[core, src], 4 + src, 4 + src, core_peer))
        put(core)
        third[0].wait()
        third[1].wait()
        for store in stores:
            store.wait()
        stores.clear()
        put(1 - core)
        own, got = final_ref[0, 0, quarter:, :SUB], final_ref[0, 1, quarter:, :SUB]
        head0, head1 = jnp.where(chip == 0, own, got), jnp.where(chip == 0, got, own)
        du_ref[...] = jnp.concatenate([head0[0:1], head1[0:1]], axis=0)
        dvb_ref[...] = jnp.concatenate([head0[1:2], head1[1:2]], axis=0)
        for store in stores + stores_rows:
            store.wait()

    def put_heads(arr, start, size, first, second):
        at = 3 - dev if arr == 2 else dev
        own_at = pl.ds(pl.multiple_of(at * block_len + start, SUB), size)
        away_at = pl.ds(pl.multiple_of(start, SUB), size)
        full_ref[arr, own_at] = jnp.where(chip == 0, first, second)
        away_ref[arr, away_at] = jnp.where(chip == 0, second, first)

    def pack_seq(arr, src):
        def body(idx, _):
            heads = jnp.swapaxes(raw_ref[src, cols(idx)], 0, 1)
            put_heads(arr, idx * TILE, TILE, heads[0], heads[1])
            return 0
        lax.fori_loop(0, block_tiles, body, 0)

    def pack_rel():
        weights = jnp.swapaxes(w_ref[...], 0, 1)
        wide_ref[:, :SUB] = weights[0]
        wide_ref[:, SUB:] = weights[1]

        def body(idx, _):
            rel = dot(table_ref[cols(idx), :], wide_ref[...]).astype(BF16)
            flip_rows = exchange_matrix()
            for chunk in range(NSUB):
                back = dot(flip_rows, rel[sub(NSUB - 1 - chunk)]).astype(BF16)
                put_heads(2, (block_tiles - 1 - idx) * TILE + chunk * SUB, SUB, back[:, :SUB], back[:, SUB:])
            return 0
        lax.fori_loop(0, block_tiles, body, 0)

    @pl.when(step == 0)
    def _():
        barrier = pltpu.get_barrier_semaphore()
        for peer in (core_peer, chip_peer, 3 - dev):
            pl.semaphore_signal(barrier, inc=1, device_id={'cp': peer}, device_id_type=pl.DeviceIdType.MESH)
        loads = [pltpu.make_async_copy(src, dst, local_sems.at[idx]) for idx, (src, dst) in enumerate((
            (kin_ref, raw_ref.at[0]), (w_in_ref, w_ref), (table_in_ref, table_ref),
            (vin_ref, raw_ref.at[1]), (qin_ref, raw_ref.at[2]), (doin_ref, raw_ref.at[3])))]
        loads[0].start()

        def clear(tile, _):
            acc_ref[:, :, cols(tile)] = jnp.zeros((3, SUB, TILE), F32)
            return 0

        def ship(arr):
            cross_copy(arr).start()
            own_copy(arr).start()

        loads[0].wait()
        for load in loads[1:]:
            load.start()
        pack_seq(0, 0)
        pl.semaphore_wait(barrier, 3)
        ship(0)
        loads[1].wait()
        loads[2].wait()
        pack_rel()
        ship(2)
        def load_and_ship(arr):
            idx = (1, 3, 4).index(arr)
            loads[3 + idx].wait()
            pack_seq(arr, idx + 1)
            ship(arr)

        @pl.when(chip == 0)
        def _():
            load_and_ship(1)
        load_and_ship(3)

        @pl.when(chip == 1)
        def _():
            load_and_ship(1)
        load_and_ship(4)
        lax.fori_loop(0, num_tiles, clear, 0)
        bias_ref[...] = jnp.zeros_like(bias_ref)
        for arr in (0, 2, 1, 3, 4):
            own_copy(arr).wait_recv()
            if arr < 3:
                transpose_half(arr, chip)

    @pl.when(step == half_steps * (1 - chip))
    def _():
        arrive((0, 2))

    @pl.when(step == half_steps - chip)
    def _():
        arrive((3,))

    rows_at = cols(blk)
    q_wide = q_ref[rows_at, :].astype(F32)
    q_u = (q_wide + u_ref[pl.ds(chip, 1), :]).astype(BF16)
    q_v = (q_wide + v_ref[pl.ds(chip, 1), :]).astype(BF16)
    qu_ref[...] = q_u
    qv_ref[...] = q_v
    qut_ref[...] = q_u.T
    qvt_ref[...] = q_v.T
    max_ref[...] = jnp.full_like(max_ref, -jnp.inf)
    sum_ref[...] = jnp.zeros_like(sum_ref)
    gu_ref[...] = jnp.zeros_like(gu_ref)
    gv_ref[...] = jnp.zeros_like(gv_ref)
    lane = lax.broadcasted_iota(jnp.int32, (SUB, SUB), 1)
    row = lax.broadcasted_iota(jnp.int32, (SUB, SUB), 0)
    upper = lane > row
    flip = 7 - lax.broadcasted_iota(jnp.int32, (8, SUB), 0)
    lower = lane + row < SUB - 1
    first_rel = num_tiles - 1 - blk

    def rotate_rel(tile, slot):
        for half in range(2):
            start = pl.multiple_of(tile * TILE + half * 256, 256)
            for a in range(NSUB):
                if a % MROWS == 0:
                    by_offset = dot(qv_ref[a * SUB:(a + MROWS) * SUB, :], relt_ref[:, pl.ds(start, 256)])
                for c in range(2):
                    part = by_offset[sub(a % MROWS), sub(c)]
                    rot_ref[slot, sub(a), sub(half * 2 + c)] = pltpu.roll(part, 1, 1, stride=1, stride_axis=0)

    rotate_rel(first_rel, 0)
    rotate_rel(jnp.minimum(first_rel + 1, num_tiles - 1), 1)

    def score_tile(tile, diag):
        left = lax.rem(tile, 3)
        right = lax.rem(tile + 1, 3)
        for half in range(2):
            start = pl.multiple_of(tile * TILE + half * 256, 256)
            for a in range(NSUB):
                if a % MROWS == 0:
                    content = dot(qu_ref[a * SUB:(a + MROWS) * SUB, :], kt_ref[:, pl.ds(start, 256)])
                run_max = max_ref[sub(a), :]
                for c2 in range(2):
                    c = half * 2 + c2
                    hi, lo = c - a + NSUB, c - a + NSUB - 1
                    if diag and c > a:
                        continue
                    else:
                        low_part = rot_ref[left if lo < NSUB else right, sub(a), sub(lo % NSUB)]
                        if diag and c == a:
                            score = jnp.where(upper, -jnp.inf, (content[sub(a % MROWS), sub(c2)] + low_part) * scale)
                        else:
                            high_part = rot_ref[left if hi < NSUB else right, sub(a), sub(hi % NSUB)]
                            score = (content[sub(a % MROWS), sub(c2)] + jnp.where(upper, high_part, low_part)) * scale
                    run_max = jnp.maximum(run_max, score)
                    sc_ref[sub(a), pl.ds(pl.multiple_of(tile * TILE + c * SUB, SUB), SUB)] = score
                max_ref[sub(a), :] = run_max
        if not diag:
            rotate_rel(jnp.minimum(first_rel + tile + 2, num_tiles - 1), lax.rem(tile + 2, 3))

    def score_body(tile, _):
        score_tile(tile, False)
        return 0

    lax.fori_loop(0, blk, score_body, 0)
    score_tile(blk, True)
    max_ref[...] = jnp.broadcast_to(jnp.max(max_ref[...], axis=1, keepdims=True), (TILE, SUB))

    @pl.when(step == half_steps * (1 - chip))
    def _():
        arrive((1,))

    def prob_tile(tile, diag):
        for top in range(0, NSUB, 2):
            rows = slice(top * SUB, (top + 2) * SUB)
            width = top + 2 if diag else NSUB
            prob_rows = []
            for a in range(top, top + 2):
                run_sum = sum_ref[sub(a), :]
                row_max = max_ref[sub(a), :]
                prob_cols = []
                for c in range(width):
                    if diag and c > a:
                        prob_cols.append(jnp.zeros((SUB, SUB), BF16))
                        continue
                    where = pl.ds(pl.multiple_of(tile * TILE + c * SUB, SUB), SUB)
                    prob = jnp.exp2(sc_ref[sub(a), where] - row_max)
                    prob_cols.append(prob.astype(BF16))
                    run_sum = run_sum + prob
                sum_ref[sub(a), :] = run_sum
                prob_rows.append(jnp.concatenate(prob_cols, axis=1))
            keys = pl.ds(pl.multiple_of(tile * TILE, TILE), width * SUB)
            gu_ref[rows, :] += dot(jnp.concatenate(prob_rows, axis=0), val_ref[keys, :])

    def prob_body(tile, _):
        prob_tile(tile, False)
        return 0

    lax.fori_loop(0, blk, prob_body, 0)
    prob_tile(blk, True)

    @pl.when(step == half_steps - chip)
    def _():
        arrive((4,))

    dot_ref[...] = do_ref[rows_at, :].T
    total = jnp.sum(sum_ref[...], axis=1, keepdims=True)
    inv_sum = 1.0 / total
    out = gu_ref[...] * inv_sum
    st_rows_ref[step, 0] = out.astype(BF16)
    delta = jnp.sum(out * do_ref[rows_at, :].astype(F32), axis=1, keepdims=True)
    row_ref[...] = jnp.broadcast_to(delta, (TILE, SUB))
    sum_ref[...] = max_ref[...] + jnp.log2(total)
    gu_ref[...] = jnp.zeros_like(gu_ref)
    for a in range(NSUB):
        ds_ref[1, sub(a), a * SUB:] = jnp.zeros((SUB, TILE - a * SUB), F32)

    def grad_tile(tile, diag):
        now = lax.rem(tile, 2)
        old = 1 - now
        for half in range(2):
            start = pl.multiple_of(tile * TILE + half * 256, 256)
            win = pl.ds(start, 256)
            d_val = d_key = None
            for top in range(0, NSUB, 2):
                if diag and 2 * half > top:
                    continue
                rows = slice(top * SUB, (top + 2) * SUB)
                do_rows = pl.ds(pl.multiple_of(blk * TILE + top * SUB, SUB), 2 * SUB)
                d_prob = dot(do_ref[do_rows, :], valt_ref[:, win])
                prob_rows, score_rows = [], []
                for a in range(top, top + 2):
                    log_norm = sum_ref[sub(a), :]
                    shift = row_ref[sub(a), :]
                    prob_cols, score_cols = [], []
                    for c2 in range(2):
                        c = half * 2 + c2
                        if diag and c > a:
                            prob_cols.append(jnp.zeros((SUB, SUB), BF16))
                            score_cols.append(jnp.zeros((SUB, SUB), BF16))
                            continue
                        prob = jnp.exp2(sc_ref[sub(a), pl.ds(pl.multiple_of(tile * TILE + c * SUB, SUB), SUB)] - log_norm)
                        d_score = prob * (d_prob[sub(a - top), sub(c2)] - shift)
                        ds_ref[now, sub(a), sub(c)] = roll_left(d_score, flip)
                        prob_cols.append(prob.astype(BF16))
                        score_cols.append(d_score.astype(BF16))
                    prob_rows.append(jnp.concatenate(prob_cols, axis=1))
                    score_rows.append(jnp.concatenate(score_cols, axis=1))
                probs = jnp.concatenate(prob_rows, axis=0)
                scores = jnp.concatenate(score_rows, axis=0)
                more_val, more_key = dot(dot_ref[:, rows], probs), dot(qut_ref[:, rows], scores)
                d_val = more_val if d_val is None else d_val + more_val
                d_key = more_key if d_key is None else d_key + more_key
                gu_ref[rows, :] += dot(scores, k_ref[win, :])
            dv_ref[:, win] += d_val
            dk_ref[:, win] += d_key
        rel_tile = first_rel + tile
        d_off = [None, None]
        for top in range(0, NSUB, 2):
            rows = slice(top * SUB, (top + 2) * SUB)
            wide_rows = []
            for a in range(top, top + 2):
                wide_cols = []
                for y in range(NSUB):
                    c_lo = y + a - NSUB
                    c_hi = c_lo + 1
                    lo_part = ds_ref[now if c_lo >= 0 else old, sub(a), sub(c_lo % NSUB)]
                    hi_part = ds_ref[now if c_hi >= 0 else old, sub(a), sub(c_hi % NSUB)]
                    wide_cols.append(jnp.where(lower, lo_part, hi_part).astype(BF16))
                wide_rows.append(jnp.concatenate(wide_cols, axis=1))
            by_off = jnp.concatenate(wide_rows, axis=0)
            gv_ref[rows, :] += dot(by_off, rel_ref[cols(rel_tile), :])
            for half in range(2):
                more = dot(qvt_ref[:, rows], by_off[:, half * 256:half * 256 + 256])
                d_off[half] = more if d_off[half] is None else d_off[half] + more
        for half in range(2):
            start = pl.multiple_of(rel_tile * TILE + half * 256, 256)
            drel_ref[:, pl.ds(start, 256)] += d_off[half]

    def grad_body(tile, _):
        grad_tile(tile, False)

        @pl.when((step == last) & (lax.rem(tile, 2) == 1) & (tile < top_tile))
        def _():
            start_parts(lax.div(top_tile - tile, 2), (2,))
            start_parts(lax.div(tile, 2), (0, 1))

        @pl.when((step == last) & (lax.rem(tile, 2) == 0) & (tile > 0) & (tile < top_tile - 2))
        def _():
            finish_offsets(lax.div(top_tile - tile + 1, 2))
            finish_keys(lax.div(tile, 2) - 1)
        return 0

    @pl.when((step > half_steps) & (chip == 0))
    def _():
        finish_offsets(pair_at(step - 1))
        finish_keys(pair_at(step - 1))

    lax.fori_loop(0, blk, grad_body, 0)
    grad_tile(blk, True)
    grad_u = gu_ref[...] * inv_sqrt
    grad_v = gv_ref[...] * inv_sqrt
    st_rows_ref[step, 1] = (grad_u + grad_v).astype(BF16)
    bias_ref[0:1, :] += jnp.sum(grad_u, axis=0, keepdims=True)
    bias_ref[1:2, :] += jnp.sum(grad_v, axis=0, keepdims=True)
    deliver(blk, st_rows_ref.at[step], 0, rows_send.at[step], True)

    @pl.when((step >= half_steps) & (step < last) & (chip == 0))
    def _():
        start_parts(pair_at(step), (2, 0, 1))

    @pl.when(step == last)
    def _():
        start_parts(0, (2,))
        start_parts(top_pair, (0, 1))

        def finish_far(idx, _):
            finish_offsets(1 - idx)
            return 0

        def finish_rest(idx, _):
            finish_keys(top_pair - 1 + idx)
            return 0

        def drain(idx, _):
            for arr in range(3):
                part_copy(idx, arr).wait_send()
            tile = 2 * idx + core
            deliver(tile, st_grad_ref.at[idx, pl.ds(0, 2)], 1, grad_send.at[idx, 0], False)
            deliver(tile, st_grad_ref.at[idx, pl.ds(2, 1)], 2, grad_send.at[idx, 1], False)
            deliver(block_at(idx), st_rows_ref.at[idx], 0, rows_send.at[idx], False)
            return 0

        lax.fori_loop(0, 2, finish_far, 0)
        lax.fori_loop(0, 2, finish_rest, 0)
        for arr in range(5):
            own_copy(arr).wait_send()
            cross_copy(arr).wait_send()
            fwd_copy(arr).wait_send()
        finish_all()
        lax.fori_loop(0, 2 * half_steps, drain, 0)


def run_attn(u_bias, v_bias, k, v, q, d_out, rel_table, w_rel):
    block_len, _, head_dim = k.shape
    seq_len = 4 * block_len
    num_tiles = seq_len // TILE
    steps = num_tiles // 2
    block_tiles = block_len // TILE
    vec = pl.BlockSpec(memory_space=pltpu.VMEM)
    hbm = pl.BlockSpec(memory_space=pl.ANY)
    result = jax.ShapeDtypeStruct((block_tiles, 4, TILE, head_dim), BF16)
    seq = jax.ShapeDtypeStruct(k.shape, BF16)
    bias = jax.ShapeDtypeStruct((2, head_dim), F32)
    d_weights = jax.ShapeDtypeStruct(w_rel.shape, F32)
    size = w_rel.shape[0] // 4 + 8
    dma = pltpu.SemaphoreType.DMA
    return pl.pallas_call(
        functools.partial(attn_kernel, num_tiles, head_dim ** -0.5),
        grid=(steps,),
        in_specs=[vec, vec] + [hbm] * 6,
        out_specs=[hbm] * 5 + [vec, vec, hbm, hbm],
        scratch_shapes=[
            pltpu.VMEM((5, seq_len, head_dim), BF16),
            pltpu.VMEM((3, head_dim, seq_len), F32),
            pltpu.VMEM((head_dim, seq_len), BF16),
            pltpu.VMEM((head_dim, seq_len), BF16),
            pltpu.VMEM((head_dim, seq_len), BF16),
            pltpu.VMEM((TILE, seq_len), F32),
            pltpu.VMEM((3, TILE, TILE), F32),
            pltpu.VMEM((2, TILE, TILE), F32),
            pltpu.VMEM((TILE, head_dim), BF16),
            pltpu.VMEM((TILE, head_dim), BF16),
            pltpu.VMEM((head_dim, TILE), BF16),
            pltpu.VMEM((head_dim, TILE), BF16),
            pltpu.VMEM((head_dim, TILE), BF16),
            pltpu.VMEM((TILE, SUB), F32),
            pltpu.VMEM((TILE, SUB), F32),
            pltpu.VMEM((TILE, head_dim), F32),
            pltpu.VMEM((TILE, head_dim), F32),
            pltpu.VMEM((TILE, SUB), F32),
            pltpu.VMEM((steps, 2, TILE, head_dim), BF16),
            pltpu.VMEM((steps, 3, TILE, head_dim), BF16),
            pltpu.VMEM((steps, 3, head_dim, TILE), F32),
            pltpu.VMEM((5, block_len, head_dim), BF16),
            pltpu.VMEM((4,) + k.shape, BF16),
            pltpu.VMEM(rel_table.shape, BF16),
            pltpu.VMEM(w_rel.shape, BF16),
            pltpu.VMEM((w_rel.shape[0], 2 * head_dim), BF16),
            pltpu.VMEM((2, head_dim), F32),
            pltpu.VMEM((2, block_tiles, TILE, head_dim), BF16),
            *[pltpu.VMEM((2, size, 2 * head_dim), F32)] * 2,
            pltpu.VMEM((2, 2, size, 2 * head_dim), F32),
            pltpu.VMEM((w_rel.shape[0] // 2,) + w_rel.shape[1:], F32),
            *[dma((6,))] * 2,
            dma((6,)), *[dma((5,))] * 6,
            *[dma((steps, 3))] * 2, dma((steps,)), dma((steps, 2)), dma((2, 3, block_tiles)), dma((block_tiles, 2)), dma((2,)),
        ],
        out_shape=[seq, seq, seq, seq, d_weights, bias, bias, result, result],
        compiler_params=pltpu.CompilerParams(
            dimension_semantics=("arbitrary",), vmem_limit_bytes=67043328, collective_id=0, has_side_effects=True),
        name="attn_rows",
    )(u_bias, v_bias, k, v, q, d_out, rel_table, w_rel)


def exchange_matrix():
    row = lax.broadcasted_iota(jnp.int32, (SUB, SUB), 0)
    col = lax.broadcasted_iota(jnp.int32, (SUB, SUB), 1)
    return jnp.where(row + col == SUB - 1, 1.0, 0.0).astype(BF16)


def solution(mesh):
    seq_spec = P('cp', 'hp', None)
    head_spec = P('hp', None)
    weight_spec = P(None, 'hp', None)

    def local_fn(q, k, v, u_bias, v_bias, rel_table, w_rel, d_out):
        out, dq, dk, dv, d_w_rel, d_u, d_v, _, _ = run_attn(u_bias, v_bias, k, v, q, d_out, rel_table, w_rel)
        return out, dq, dk, dv, d_u, d_v, d_w_rel

    return jax.shard_map(
        local_fn,
        mesh=mesh,
        in_specs=(seq_spec, seq_spec, seq_spec, head_spec, head_spec, P('cp', None), weight_spec, seq_spec),
        out_specs=(seq_spec, seq_spec, seq_spec, seq_spec, head_spec, head_spec, weight_spec),
        check_vma=False,
    )
```
